256 devices in a mesh: ctx: 128 (over x, y_hi, z, core), head: 2 (over y_lo).
Axes of the slice: x: 4, y: 4 (y_hi: 2, y_lo: 2; y = y_hi * 2 + y_lo), z: 8, core: 2. Of those that a mesh axis runs over, the one named last changes fastest.
Arguments:
- queries: bfloat16 [16384, 2048], P('ctx', 'head'), may hold values from -160 to 160
- rotated_keys: bfloat16 [16384, 512], P('ctx', 'head'), may hold values from -6 to 6
- value_matrix: bfloat16 [16384, 512], P('ctx', 'head'), may hold values from -6 to 6
- doc_lengths: int32 [8], replicated, may hold values from 1 to 12288, 16384 in all
- scored: int32 [512], P('ctx'), may hold values from 0 to 127, as said below
- residual: bfloat16 [512, 4096], P('ctx', 'head'), may hold values from -18 to 18
- norm_gain: float32 [4096], P('head'), may hold values from 0.5 to 1.5
- out_weight: bfloat16 [2048, 4096], P('head'), may hold values from -0.5 to 0.5
- lm_weight: bfloat16 [4096, 128256], P('head', 'ctx'), may hold values from -0.40625 to 0.40625
- token_ids: int32 [512], replicated, may hold values from 0 to 128255
- old_logp: float32 [512], replicated, may hold values from -24 to -9
- advantage: float32 [512], replicated, may hold values from -3 to 3
Outputs:
- attended: bfloat16 [16384, 2048], P('ctx', 'head')
- log_probs: float32 [512], replicated
- token_loss: float32 [512], replicated
The draws below stay inside these ranges and needn't reach their ends.
Inputs may be any that keep to these rules, and one draw needn't show every extreme that they name: `scored`: each aligned block of 4 entries holds distinct increasing offsets. `doc_lengths`: the longest document has exactly three quarters of 16384 positions.
All inputs are finite; a program needn't handle non-finite values.
Results may differ from the reference program's by a relative error of at most 0.0065.
Values may be sent and summed in bfloat16 or wider, within the bound.
A program may use at most 128 MiB of HBM per device.

```python
import math
import jax
import jax.numpy as jnp
import numpy as np
from jax import lax

D = 4096
QUERY_HEADS = 16
KEY_VALUE_HEADS = 4
HEAD_SIZE = 128
V = 128256
TOK_DEV = 128
RESP_DEV = 4
DOCS = 8
PACKED_LENGTH = 16384
RESP = 512


def key_sample(key):
    drawn_sample = jax.random.normal(jax.random.fold_in(key, 12), (PACKED_LENGTH, KEY_VALUE_HEADS * HEAD_SIZE), jnp.float32)
    return jnp.clip(drawn_sample, -6.0, 6.0)


def draw_rotated_keys(key, part):
    sample = key_sample(key)
    return sample.astype(jnp.bfloat16)


def draw_queries(key, part):
    sample = 2.0 * jnp.clip(jax.random.normal(jax.random.fold_in(key, 11), (PACKED_LENGTH, QUERY_HEADS * HEAD_SIZE), jnp.float32), -6.0, 6.0)
    return sample.astype(jnp.bfloat16)


def draw_lm_weight(key, part):
    weight_scale = 3.0 * D ** (-0.5)
    sample = jnp.clip(jax.random.normal(jax.random.fold_in(key, 23), (D, V), jnp.float32), -6.0, 6.0) * weight_scale
    return sample.astype(jnp.bfloat16)


def column_scales():
    steps = jnp.arange(D, dtype=jnp.float32) / max(D - 1, 1)
    return jnp.exp(jnp.log(0.5) + steps * jnp.log(5.9))


def draw_residual(key, part):
    widths = column_scales()[None, :]
    sample = jnp.clip(jax.random.normal(jax.random.fold_in(key, 24), (RESP, D), jnp.float32), -6.0, 6.0) * widths
    return sample.astype(jnp.bfloat16)


def draw_scored(key, part):

    def one_block(block_index):
        picked = jax.random.permutation(jax.random.fold_in(key, block_index), TOK_DEV)[:RESP_DEV]
        return jnp.sort(picked)
    return jax.vmap(one_block)(jnp.arange(RESP // RESP_DEV)).reshape(RESP).astype(jnp.int32)


def with_ends(values, own_key, least, top_value):
    spot = [jax.random.randint(jax.random.fold_in(own_key, axis), (), 0, length) for axis, length in enumerate(values.shape)]
    main_axis = values.shape.index(max(values.shape))
    neighbour = spot[:main_axis] + [(spot[main_axis] + 1) % values.shape[main_axis]] + spot[main_axis + 1:]
    return values.at[tuple(spot)].set(least).at[tuple(neighbour)].set(top_value)


def block_scale(stream_key, shape, split, low, high):
    gain = 1.0
    for dim, blocks in split:
        heights = jax.random.uniform(jax.random.fold_in(jax.random.fold_in(stream_key, 6), dim), (blocks,), jnp.float32, low / len(split), high / len(split))
        gain = gain * jnp.repeat(jnp.exp(heights), shape[dim] // blocks).reshape((-1,) + (1,) * (len(shape) - 1 - dim))
    return gain


def skewed_wide(own_key, extent, number_of, lean):
    weights = [min(1 << octave, number_of + 1 - (1 << octave)) * (1 << 20) // math.isqrt((1 << octave) ** lean) + 1 for octave in range((number_of + 1).bit_length()) if 1 << octave <= number_of]
    width = 1 + sum(weights) // (1 << 30)
    table = np.cumsum(np.array([max(1, weight // width) for weight in weights]))
    lot = jax.random.randint(jax.random.fold_in(own_key, 1), extent, 0, int(table[len(weights) - 1]))
    start = jnp.left_shift(1, jnp.searchsorted(jnp.asarray(table, jnp.int32), lot, side="right").astype(jnp.int32))
    grade = start - 1 + jax.random.randint(jax.random.fold_in(own_key, 4), extent, 0, 1 << 30) % jnp.minimum(start, number_of + 1 - start)
    return jax.random.permutation(jax.random.fold_in(own_key, 2), number_of)[grade].astype(jnp.int32)


def length_profile(number_of, total, bound, skew):
    weights = [(1 << 20) // math.isqrt(grade ** skew) + 1 for grade in range(2, number_of + 1)]
    spare, holding = total - bound - (number_of - 1), [1] * (number_of - 1)
    while spare > 0:
        candidates = [i for i in range(number_of - 1) if holding[i] < bound]
        mass, budget = sum([weights[i] for i in candidates]), spare
        for i in candidates:
            addition = min(bound - holding[i], max(1, budget * weights[i] // mass), spare)
            holding[i] = holding[i] + addition
            spare = spare - addition
    return np.array([bound] + holding)


def ragged_sizes(own_key, count, total, limit, lean):
    if count == 2:
        one = jax.random.randint(own_key, (), max(1, total - limit), min(limit, total - 1) + 1)
        return jnp.stack([one, total - one])
    sizes = jnp.asarray(length_profile(count, total, limit, lean), jnp.int32)
    twos = (count - 1) // 2
    source_of, receiver = sizes[1:1 + 2 * twos:2], sizes[2:2 + 2 * twos:2]
    margin = jnp.minimum(source_of - 1, limit - receiver)
    shifted = jax.random.randint(jax.random.fold_in(own_key, 1), (twos,), 0, 1 << 20) % (margin + 1)
    sizes = sizes.at[1:1 + 2 * twos:2].set(source_of - shifted).at[2:2 + 2 * twos:2].set(receiver + shifted)
    return sizes[jax.random.permutation(jax.random.fold_in(own_key, 2), count)]


def centred(rng, extent, deviation, limit, pieces=(), kind=jnp.bfloat16):
    entries = deviation * jax.random.normal(rng, extent, jnp.float32)
    if pieces:
        entries = entries * block_scale(rng, extent, pieces, -0.22, 0.18)
    return jnp.clip(entries, -limit, limit).astype(kind)


def setup_inputs(seed: int = 0) -> dict:
    keys = jax.random.split(jax.random.key(seed), 13)
    return {
        "queries": draw_queries(jax.random.fold_in(keys[12], 71), 0),
        "rotated_keys": draw_rotated_keys(jax.random.fold_in(keys[12], 71), 0),
        "value_matrix": centred(keys[2], (PACKED_LENGTH, KEY_VALUE_HEADS * HEAD_SIZE), 1.0, 6.0, ((0, 128), (1, 2))),
        "doc_lengths": ragged_sizes(keys[3], DOCS, PACKED_LENGTH, 3 * PACKED_LENGTH // 4, 2).astype(jnp.int32),
        "scored": draw_scored(jax.random.fold_in(keys[12], 71), 0),
        "residual": draw_residual(jax.random.fold_in(keys[12], 71), 0),
        "norm_gain": jnp.clip(1.0 + 0.1 * jax.random.normal(keys[6], (D,), jnp.float32), 0.5, 1.5),
        "out_weight": centred(keys[7], (QUERY_HEADS * HEAD_SIZE, D), (QUERY_HEADS * HEAD_SIZE // 16) ** -0.5, 0.5, ((0, 2),)),
        "lm_weight": draw_lm_weight(jax.random.fold_in(keys[12], 71), 0),
        "token_ids": with_ends(skewed_wide(keys[9], (RESP,), V, 2), jax.random.fold_in(keys[9], 3), 0, V - 1).astype(jnp.int32),
        "old_logp": jnp.clip(jax.random.uniform(keys[10], (RESP,), jnp.float32, -24.0, -9.0), -24.0, -9.0),
        "advantage": centred(keys[11], (RESP,), 0.5, 3.0, (), jnp.float32),
    }


def doc_index(positions, doc_ends):
    return lax.optimization_barrier(jnp.sum((positions[:, None] >= doc_ends[None, :]).astype(jnp.int32), axis=1))

def reference(queries, rotated_keys, value_matrix, doc_lengths, scored, residual, norm_gain, out_weight, lm_weight, token_ids, old_logp, advantage):
    group_count = QUERY_HEADS // KEY_VALUE_HEADS
    doc_ends = jnp.cumsum(doc_lengths).astype(jnp.int32)
    key_pos = jnp.arange(PACKED_LENGTH, dtype=jnp.int32)
    key_doc = doc_index(key_pos, doc_ends)
    key_head_rows = rotated_keys.reshape(PACKED_LENGTH, KEY_VALUE_HEADS, HEAD_SIZE).astype(jnp.float32)
    value_head_rows = value_matrix.reshape(PACKED_LENGTH, KEY_VALUE_HEADS, HEAD_SIZE).astype(jnp.float32)
    query_matrix = min(256, PACKED_LENGTH)

    def one_block(offset):
        block_tile = lax.dynamic_slice_in_dim(queries, offset, query_matrix, 0)
        block_tile = block_tile.reshape(query_matrix, KEY_VALUE_HEADS, group_count, HEAD_SIZE).astype(jnp.float32)
        scores = jnp.einsum('qkgd,rkd->kgqr', block_tile, key_head_rows) * HEAD_SIZE ** (-0.5)
        query_pos = offset + jnp.arange(query_matrix, dtype=jnp.int32)
        allowed = (key_pos[None, :] <= query_pos[:, None]) & (key_doc[None, :] == doc_index(query_pos, doc_ends)[:, None])
        scores = jnp.where(allowed, scores, -1e+30)
        row_top = lax.optimization_barrier(jnp.max(scores, axis=-1, keepdims=True))
        weights = jnp.where(allowed, jnp.exp(scores - row_top), 0.0)
        row_total = lax.optimization_barrier(jnp.sum(weights, axis=-1, keepdims=True))
        probs = lax.optimization_barrier(weights.astype(jnp.bfloat16)).astype(jnp.float32)
        result = jnp.einsum('kgqr,rkd->kgqd', probs, value_head_rows) / row_total
        return jnp.transpose(result, (2, 0, 1, 3)).reshape(query_matrix, QUERY_HEADS * HEAD_SIZE).astype(jnp.bfloat16)
    offsets = jnp.arange(PACKED_LENGTH // query_matrix, dtype=jnp.int32) * query_matrix
    attended = lax.map(one_block, offsets).reshape(PACKED_LENGTH, QUERY_HEADS * HEAD_SIZE)
    positions = jnp.arange(RESP, dtype=jnp.int32) // RESP_DEV * TOK_DEV + scored
    chosen = jnp.take(attended, positions, axis=0)
    hidden = residual.astype(jnp.float32) + jnp.dot(chosen, out_weight, preferred_element_type=jnp.float32)
    mean_square = lax.optimization_barrier(jnp.mean(hidden * hidden, axis=1, keepdims=True))
    normed = (hidden * lax.rsqrt(mean_square + 1e-05) * norm_gain[None, :]).astype(jnp.bfloat16)
    logits = jnp.dot(normed, lm_weight, preferred_element_type=jnp.float32)
    row_top = lax.optimization_barrier(jnp.max(logits, axis=1))
    row_total = lax.optimization_barrier(jnp.sum(jnp.exp(logits - row_top[:, None]), axis=1))
    target = jnp.take_along_axis(logits, token_ids[:, None].astype(jnp.int32), axis=1)[:, 0]
    log_probs = target - row_top - jnp.log(row_total)
    ratio = jnp.exp(jnp.clip(log_probs - old_logp, -4.0, 4.0))
    token_loss = -jnp.minimum(ratio * advantage, jnp.clip(ratio, 0.8, 1.2) * advantage)
    return (attended, log_probs, token_loss)
```

```python
import functools
import math

import jax
import jax.numpy as jnp
from jax import lax
from jax.experimental import pallas as pl
from jax.experimental.pallas import tpu as pltpu
from jax.sharding import Mesh
from jax.sharding import PartitionSpec as P

HEAD_SIZE = 128
CTX = ("x", "yh", "z", "core")
NAMES = ("x", "yh", "z", "core", "head")
NEG = -1e30
SCALE = HEAD_SIZE**-0.5 * math.log2(math.e)
MESH = pl.DeviceIdType.MESH
VMEM = pltpu.VMEM


def remote(src, dst, send_sem, recv_sem, **where):
    return pltpu.make_async_remote_copy(
        src_ref=src,
        dst_ref=dst,
        send_sem=send_sem,
        recv_sem=recv_sem,
        device_id=where,
        device_id_type=MESH,
    )


def greet(peers):
    barrier = pltpu.get_barrier_semaphore()
    for where in peers:
        pl.semaphore_signal(barrier, inc=1, device_id=where, device_id_type=MESH)
    pl.semaphore_wait(barrier, len(peers))


def exchange_kernel(
    sizes,
    kv_ref,
    q_ref,
    kvbuf,
    qbuf,
    first_send,
    first_recv,
    up_send,
    up_recv,
    down_send,
    down_recv,
    q_send,
    q_recv,
):
    xs, zs = sizes
    x, yh, z, kc = (lax.axis_index(n) for n in CTX)
    up, down = (lax.rem(z + 1, zs), lax.rem(z + zs - 1, zs))
    shift = lax.rem(z, xs)
    tx = lax.rem(x + z, xs)
    mine = 2 * yh + kc
    peers = []
    for dx in range(xs):
        for dy in range(2):
            for dk in range(2):
                if dx or dy or dk:
                    peers.append(
                        {
                            "x": lax.rem(x + dx, xs),
                            "yh": lax.rem(yh + dy, 2),
                            "core": lax.rem(kc + dk, 2),
                        }
                    )
    peers.append({"z": up})
    peers.append({"z": down})
    greet(peers)

    def first(dy, dk):
        ty, tk = (lax.rem(yh + dy, 2), lax.rem(kc + dk, 2))
        return remote(
            kv_ref.at[tk],
            kvbuf.at[z, mine],
            first_send.at[2 * dy + dk],
            first_recv.at[mine],
            x=tx,
            yh=ty,
            core=tk,
        )

    def first_here():
        return pltpu.make_async_copy(kv_ref.at[kc], kvbuf.at[z, mine], first_recv.at[mine])

    for dy, dk in ((1, 0), (1, 1), (0, 1)):
        first(dy, dk).start()

    @pl.when(shift == 0)
    def _():
        first_here().start()

    @pl.when(shift != 0)
    def _():
        first(0, 0).start()

    def q_copy(dx, dk):
        ox, tk = (lax.rem(x + dx, xs), lax.rem(kc + dk, 2))
        return remote(
            q_ref.at[tk],
            qbuf.at[x, kc],
            q_send.at[2 * dx + dk],
            q_recv.at[2 * x + kc],
            x=ox,
            core=tk,
        )

    q_here = pltpu.make_async_copy(q_ref.at[kc], qbuf.at[x, kc], q_recv.at[2 * x + kc])
    q_here.start()
    q_order = [
        (dx, dk)
        for dx in [0] + sorted(range(1, xs), key=lambda d: min(d, xs - d))
        for dk in (0, 1)
        if dx or dk
    ]
    for dx, dk in q_order:
        q_copy(dx, dk).start()

    def first_wait(s):
        remote(
            kv_ref.at[0], kvbuf.at[z, s], first_send.at[0], first_recv.at[s], z=up
        ).wait_recv()

    def ring(going_up, slot, t, h):
        send, recv, to = (up_send, up_recv, up) if going_up else (down_send, down_recv, down)
        part = kvbuf.at[slot, pl.ds(2 * h, 2)]
        return remote(part, part, send.at[t, h], recv.at[t, h], z=to)

    def sent(going_up, t, h):
        slot = lax.rem(z - t + zs, zs) if going_up else lax.rem(z + t, zs)
        return ring(going_up, slot, t, h)

    def got(going_up, t, h):
        slot = lax.rem(z - 1 - t + zs, zs) if going_up else lax.rem(z + 1 + t, zs)
        return ring(going_up, slot, t, h)

    full = (zs - 2) // 2
    for t in range(full):
        for h in range(2):
            if t == 0:
                first_wait(2 * h)
                first_wait(2 * h + 1)
            for going_up in (True, False):
                if t > 0:
                    got(going_up, t - 1, h).wait_recv()
                sent(going_up, t, h).start()
    if full == 0:
        for s in range(4):
            first_wait(s)
    for going_up, h in ((True, 0), (False, 1)):
        if full > 0:
            got(going_up, full - 1, h).wait_recv()
        sent(going_up, full, h).start()
    if full > 0:
        got(True, full - 1, 1).wait_recv()
        got(False, full - 1, 0).wait_recv()
    got(True, full, 0).wait_recv()
    got(False, full, 1).wait_recv()

    for t in range(full):
        for h in range(2):
            for going_up in (True, False):
                sent(going_up, t, h).wait_send()
    sent(True, full, 0).wait_send()
    sent(False, full, 1).wait_send()
    for dy, dk in ((1, 0), (1, 1), (0, 1)):
        first(dy, dk).wait_send()

    @pl.when(shift != 0)
    def _():
        first(0, 0).wait_send()

    for dx, dk in q_order:
        q_copy(dx, dk).wait_send()
    for s in range(2 * xs):
        remote(
            q_ref.at[0], qbuf.at[s // 2, s % 2], q_send.at[0], q_recv.at[s], z=up
        ).wait_recv()


def exchange(sizes, kv, q):
    xs, zs = sizes
    tok = q.shape[1]
    full = (zs - 2) // 2
    dma = pltpu.SemaphoreType.DMA
    return pl.pallas_call(
        functools.partial(exchange_kernel, sizes),
        out_shape=(
            jax.ShapeDtypeStruct((zs, 4, *kv.shape[1:]), kv.dtype),
            jax.ShapeDtypeStruct((xs, 2, *q.shape[1:]), q.dtype),
        ),
        in_specs=[pl.BlockSpec(memory_space=VMEM)] * 2,
        out_specs=(pl.BlockSpec(memory_space=VMEM),) * 2,
        scratch_shapes=[
            dma((4,)),
            dma((4,)),
            dma((full + 1, 2)),
            dma((full + 1, 2)),
            dma((full + 1, 2)),
            dma((full + 1, 2)),
            dma((2 * xs,)),
            dma((2 * xs,)),
        ],
        compiler_params=pltpu.CompilerParams(
            collective_id=0, has_side_effects=True, vmem_limit_bytes=24 << 20
        ),
        name="exchange",
    )(kv, q)


def flash_kernel(docs, chunks, meta, q_ref, kv_ref, o_ref, l_ref, acc, top, causal, start, order):
    xq = pl.program_id(0)
    tok = q_ref.shape[2]
    rows = 2 * tok
    heads = q_ref.shape[3] // HEAD_SIZE
    first = meta[xq]
    lanes = lax.broadcasted_iota(jnp.int32, (rows, 128), 1)
    positions = first + lax.broadcasted_iota(jnp.int32, (rows, 128), 0)
    begins = jnp.zeros((rows, 128), jnp.int32)
    low = jnp.int32(0)
    for d in range(docs):
        doc_start = meta[8 + d]
        begins = jnp.where(positions >= doc_start, jnp.maximum(begins, doc_start), begins)
        low = jnp.where(first >= doc_start, jnp.maximum(low, doc_start), low)
    causal[...] = positions - lanes
    start[...] = begins - lanes
    acc[...] = jnp.zeros_like(acc)
    top[...] = jnp.full_like(top, NEG)

    def pick(i, n):
        base = meta[32 + i]
        order[n] = i
        return n + jnp.where((base < first + rows) & (base + rows > low), 1, 0)

    active = lax.fori_loop(0, chunks, pick, jnp.int32(0))

    def step(pair, carry):
        one = order[2 * pair]
        whole = 2 * pair + 1 < active
        two = jnp.where(whole, order[2 * pair + 1], one)
        bases = (meta[32 + one], jnp.where(whole, meta[32 + two], 1 << 28))
        keys, values, biases = [], [], []
        for chunk, base in zip((one, two), bases):
            zz, yy = (chunk // 2, lax.rem(chunk, 2))
            for k in range(2):
                keys.append(kv_ref[zz, 2 * yy + k, 0])
                values.append(kv_ref[zz, 2 * yy + k, 1])
                at = base + k * tok
                ok = (causal[...] >= at) & (start[...] <= at)
                biases.append(jnp.where(ok, 0.0, NEG))
        key = jnp.concatenate(keys, axis=0)
        value = jnp.concatenate(values, axis=0)
        value = jnp.concatenate([value, jnp.ones_like(value)], axis=1)
        bias = jnp.concatenate(biases, axis=1)
        for h in range(heads):
            cols = slice(h * HEAD_SIZE, (h + 1) * HEAD_SIZE)
            q = q_ref[0, :, :, cols].reshape(rows, HEAD_SIZE)
            s = lax.dot_general(
                q, key, (((1,), (1,)), ((), ())), preferred_element_type=jnp.float32
            )
            s = s * SCALE + bias
            old = top[h]
            new = jnp.maximum(old, jnp.max(s, axis=1, keepdims=True))
            w = jnp.exp2(s - new[:, :1]).astype(jnp.bfloat16)
            update = jnp.dot(w, value, preferred_element_type=jnp.float32)
            shrink = jnp.exp2(old - new)
            top[h] = new
            acc[h] = acc[h] * jnp.concatenate([shrink, shrink], axis=1) + update
        return carry

    lax.fori_loop(0, (active + 1) // 2, step, 0)

    lane = lax.broadcasted_iota(jnp.int32, (rows, 128), 1)
    packed = jnp.full((rows, 128), NEG, jnp.float32)
    for h in range(heads):
        total = jnp.maximum(acc[h, :, HEAD_SIZE:], 1e-30)
        out = acc[h, :, :HEAD_SIZE] / total
        o_ref[0, :, :, h * HEAD_SIZE : (h + 1) * HEAD_SIZE] = out.astype(jnp.bfloat16).reshape(
            2, tok, HEAD_SIZE
        )
        packed = jnp.where(lane == h, top[h] + jnp.log2(total), packed)
    for k in range(2):
        l_ref[0, k] = jnp.transpose(packed[k * tok : (k + 1) * tok])[:8]


def flash(docs, meta, q, kv):
    xs, _, tok, width = q.shape
    chunks = kv.shape[0] * 2
    heads = width // HEAD_SIZE
    keys = kv.shape[0] * 4 * tok
    rows = 2 * tok
    return pl.pallas_call(
        functools.partial(flash_kernel, docs, chunks),
        out_shape=(
            jax.ShapeDtypeStruct(q.shape, jnp.bfloat16),
            jax.ShapeDtypeStruct((xs, 2, 8, 128), jnp.float32),
        ),
        grid=(xs,),
        in_specs=[
            pl.BlockSpec(memory_space=pltpu.SMEM),
            pl.BlockSpec((1, 2, tok, width), lambda i: (i, 0, 0, 0)),
            pl.BlockSpec(memory_space=VMEM),
        ],
        out_specs=(
            pl.BlockSpec((1, 2, tok, width), lambda i: (i, 0, 0, 0)),
            pl.BlockSpec((1, 2, 8, 128), lambda i: (i, 0, 0, 0)),
        ),
        scratch_shapes=[
            VMEM((heads, rows, 2 * HEAD_SIZE), jnp.float32),
            VMEM((heads, rows, 128), jnp.float32),
            VMEM((rows, 128), jnp.int32),
            VMEM((rows, 128), jnp.int32),
            pltpu.SMEM((chunks + 2,), jnp.int32),
        ],
        compiler_params=pltpu.CompilerParams(vmem_limit_bytes=32 << 20),
        cost_estimate=pl.CostEstimate(
            flops=4 * heads * xs * rows * keys * HEAD_SIZE // 3,
            bytes_accessed=4 << 20,
            transcendentals=heads * xs * rows * keys // 3,
        ),
        name="flash",
    )(meta, q, kv)


def rows_kernel(
    sizes,
    width_full,
    o_ref,
    l_ref,
    res_ref,
    scored_ref,
    gain_ref,
    ow_ref,
    att_ref,
    g_ref,
    obuf,
    lbuf,
    rbuf,
    cbuf,
    wbuf,
    psend,
    pbuf,
    sqbuf,
    ubuf,
    w_sem,
    o_send,
    o_recv,
    l_send,
    l_recv,
    r_send,
    r_recv,
    c_send,
    c_recv,
    p_sem,
    s_send,
    s_recv,
    u_sem,
    y_sem,
    z_send,
    z_recv,
    x_send,
    x_recv,
    k_send,
    k_recv,
):
    xs, zs = sizes
    x, yh, z, kc = (lax.axis_index(n) for n in CTX)
    hd = lax.axis_index("head")
    oy, ok, oh = (lax.rem(yh + 1, 2), lax.rem(kc + 1, 2), lax.rem(hd + 1, 2))
    row_slot = 2 * yh + kc
    quarter = 2 * kc + yh
    half = width_full // 2
    wide = half // 4

    peers = []
    for dx in range(xs):
        for dk in range(2):
            if dx or dk:
                peers.append({"x": lax.rem(x + dx, xs), "core": lax.rem(kc + dk, 2)})
    peers += [{"yh": oy}, {"yh": oy, "core": ok}]
    for where in ({}, {"core": ok}, {"yh": oy}, {"yh": oy, "core": ok}):
        peers.append({"head": oh, **where})
    for dz in range(1, zs):
        peers.append({"z": lax.rem(z + dz, zs)})

    weights = []
    for j, side in enumerate((hd, oh)):
        col = pl.multiple_of(side * half + quarter * wide, 128)
        weights.append(
            pltpu.make_async_copy(ow_ref.at[:, pl.ds(col, wide)], wbuf.at[j], w_sem.at[j])
        )
        weights[-1].start()
    greet(peers)

    o_order = [
        (dx, dk)
        for dx in sorted(range(1, xs), key=lambda d: -min(d, xs - d)) + [0]
        for dk in (0, 1)
        if dx or dk
    ]

    def o_copies(dx, dk):
        tx, tk = (lax.rem(x + dx, xs), lax.rem(kc + dk, 2))
        where = {"x": tx, "core": tk}
        s, mine = (2 * dx + dk, 2 * x + kc)
        return (
            remote(l_ref.at[tx, tk], lbuf.at[x, kc], l_send.at[s], l_recv.at[mine], **where),
            remote(o_ref.at[tx, tk], obuf.at[x, kc], o_send.at[s], o_recv.at[mine], **where),
        )

    for dx, dk in o_order:
        for copy in o_copies(dx, dk):
            copy.start()
    pltpu.make_async_copy(o_ref.at[x, kc], obuf.at[x, kc], o_recv.at[2 * x + kc]).start()
    pltpu.make_async_copy(l_ref.at[x, kc], lbuf.at[x, kc], l_recv.at[2 * x + kc]).start()

    def r_copy(dy, dk):
        ty, tk = (lax.rem(yh + dy, 2), lax.rem(kc + dk, 2))
        return remote(
            res_ref.at[2 * tk + ty],
            rbuf.at[row_slot],
            r_send.at[2 * dy + dk],
            r_recv.at[row_slot],
            yh=ty,
            core=tk,
        )

    near = ((0, 1), (1, 0), (1, 1))
    for dy, dk in near:
        r_copy(dy, dk).start()
    pltpu.make_async_copy(res_ref.at[quarter], rbuf.at[row_slot], r_recv.at[row_slot]).start()

    for s in range(2 * xs):
        at = (s // 2, s % 2)
        remote(l_ref.at[0, 0], lbuf.at[at], l_send.at[0], l_recv.at[s], head=oh).wait_recv()
        remote(o_ref.at[0, 0], obuf.at[at], o_send.at[0], o_recv.at[s], head=oh).wait_recv()

    for k in range(2):
        parts = [lbuf[j, k] for j in range(xs)]
        highest = functools.reduce(jnp.maximum, parts)
        parts = [jnp.exp2(part - highest) for part in parts]
        total = functools.reduce(jnp.add, parts)
        parts = [part / total for part in parts]
        padding = [jnp.zeros((128 - 8 * xs, 128), jnp.float32)]
        shares = jnp.transpose(jnp.concatenate(parts + padding, axis=0))
        heads = o_ref.shape[3] // HEAD_SIZE
        for h in range(heads):
            cols = slice(h * HEAD_SIZE, (h + 1) * HEAD_SIZE)
            merged = sum(
                shares[:, 8 * j + h : 8 * j + h + 1] * obuf[j, k, :, cols].astype(jnp.float32)
                for j in range(xs)
            )
            out = (k * heads + h) * HEAD_SIZE
            att_ref[:, out : out + HEAD_SIZE] = merged.astype(jnp.bfloat16)

    tok = att_ref.shape[0]
    hot = scored_ref[...] == lax.broadcasted_iota(jnp.int32, (16, tok), 1)
    hot = jnp.where(hot, 1.0, 0.0).astype(jnp.bfloat16)
    cbuf[row_slot] = jnp.dot(hot, att_ref[...], preferred_element_type=jnp.float32).astype(
        jnp.bfloat16
    )

    def c_copy(dy, dk):
        return remote(
            cbuf.at[row_slot],
            cbuf.at[row_slot],
            c_send.at[2 * dy + dk],
            c_recv.at[2 * dy + dk],
            yh=lax.rem(yh + dy, 2),
            core=lax.rem(kc + dk, 2),
        )

    for dy, dk in near:
        c_copy(dy, dk).start()
    for dy, dk in near:
        c_copy(dy, dk).wait_recv()
    for copy in weights:
        copy.wait()
    chosen = (cbuf[0] + cbuf[1]) + (cbuf[2] + cbuf[3])
    psend[...] = jnp.dot(chosen, wbuf[1], preferred_element_type=jnp.float32).astype(jnp.bfloat16)
    p_copy = remote(psend, pbuf, p_sem.at[0], p_sem.at[1], head=oh)
    p_copy.start()
    hidden = jnp.dot(chosen, wbuf[0], preferred_element_type=jnp.float32)
    for s in range(4):
        remote(res_ref.at[0], rbuf.at[s], r_send.at[0], r_recv.at[s], head=oh).wait_recv()
    residual = (rbuf[0] + rbuf[1]) + (rbuf[2] + rbuf[3])
    p_copy.wait_recv()
    hidden = residual.astype(jnp.float32) + (hidden + pbuf[...].astype(jnp.float32))

    own = 4 * hd + row_slot
    sqbuf[own] = jnp.broadcast_to(jnp.sum(hidden * hidden, axis=1, keepdims=True), (16, 128))

    def s_copy(d):
        dh, dy, dk = (d // 4, d // 2 % 2, d % 2)
        return remote(
            sqbuf.at[own],
            sqbuf.at[own],
            s_send.at[d],
            s_recv.at[d],
            head=lax.rem(hd + dh, 2),
            yh=lax.rem(yh + dy, 2),
            core=lax.rem(kc + dk, 2),
        )

    for d in range(1, 8):
        s_copy(d).start()
    for d in range(1, 8):
        s_copy(d).wait_recv()
    squares = functools.reduce(jnp.add, [sqbuf[s] for s in range(8)])
    scale = lax.rsqrt(squares / width_full + 1e-05)[:, :1]
    ubuf[...] = (hidden * scale * gain_ref[quarter]).astype(jnp.bfloat16)

    mine = pl.ds(pl.multiple_of(quarter * wide, 128), wide)
    both = pl.ds(pl.multiple_of(kc * 2 * wide, 128), 2 * wide)
    others = pl.ds(pl.multiple_of(ok * 2 * wide, 128), 2 * wide)
    here = pltpu.make_async_copy(ubuf, g_ref.at[x, z, :, mine], u_sem)
    here.start()
    y_copy = remote(ubuf, g_ref.at[x, z, :, mine], y_sem.at[0], y_sem.at[1], yh=oy)
    y_copy.start()
    here.wait()
    y_copy.wait_recv()

    def block(bx, bz):
        return g_ref.at[bx, bz, :, both]

    def z_copy(dz):
        to = lax.rem(z + dz, zs)
        return remote(block(x, z), block(x, z), z_send.at[dz], z_recv.at[dz], z=to)

    def x_copy(dx, dz):
        bz = lax.rem(z + zs - dz, zs)
        to = lax.rem(x + dx, xs)
        return remote(block(x, bz), block(x, bz), x_send.at[dx, dz], x_recv.at[dx, dz], x=to)

    def k_copy(dx):
        plane = g_ref.at[lax.rem(x + xs - dx, xs), :, :, both]
        return remote(plane, plane, k_send.at[dx], k_recv.at[dx], core=ok)

    z_order = sorted(range(1, zs), key=lambda d: min(d, zs - d))
    x_order = sorted(range(1, xs), key=lambda d: min(d, xs - d))
    for dz in reversed(z_order):
        z_copy(dz).start()
    for dz in [0] + z_order:
        if dz:
            z_copy(dz).wait_recv()
        for dx in x_order:
            x_copy(dx, dz).start()
    k_copy(0).start()
    for dx in x_order:
        for dz in [0] + z_order:
            x_copy(dx, dz).wait_recv()
        k_copy(dx).start()
    for dx in range(xs):
        k_copy(dx).wait_recv()

    for dx, dk in o_order:
        for copy in o_copies(dx, dk):
            copy.wait_send()
    for dy, dk in near:
        r_copy(dy, dk).wait_send()
        c_copy(dy, dk).wait_send()
    p_copy.wait_send()
    for d in range(1, 8):
        s_copy(d).wait_send()
    y_copy.wait_send()
    for dz in z_order:
        z_copy(dz).wait_send()
    for dx in x_order:
        for dz in range(zs):
            x_copy(dx, dz).wait_send()
    for dx in range(xs):
        k_copy(dx).wait_send()


def gathered_rows(sizes, o, l, res, scored, gain, out_weight):
    xs, zs = sizes
    tok = o.shape[2]
    width_full = out_weight.shape[1]
    depth = out_weight.shape[0]
    half = width_full // 2
    wide = half // 4
    dma = pltpu.SemaphoreType.DMA
    bf16 = jnp.bfloat16
    return pl.pallas_call(
        functools.partial(rows_kernel, sizes, width_full),
        out_shape=(
            jax.ShapeDtypeStruct((tok, depth), bf16),
            jax.ShapeDtypeStruct((xs, zs, 16, half), bf16),
        ),
        in_specs=[pl.BlockSpec(memory_space=VMEM)] * 5 + [pl.BlockSpec(memory_space=pl.ANY)],
        out_specs=(pl.BlockSpec(memory_space=VMEM),) * 2,
        scratch_shapes=[
            VMEM(o.shape, bf16),
            VMEM(l.shape, jnp.float32),
            VMEM((4, 16, wide), bf16),
            VMEM((4, 16, depth), bf16),
            VMEM((2, depth, wide), bf16),
            VMEM((16, wide), bf16),
            VMEM((16, wide), bf16),
            VMEM((8, 16, 128), jnp.float32),
            VMEM((16, wide), bf16),
            dma((2,)),
            dma((2 * xs,)),
            dma((2 * xs,)),
            dma((2 * xs,)),
            dma((2 * xs,)),
            dma((4,)),
            dma((4,)),
            dma((4,)),
            dma((4,)),
            dma((2,)),
            dma((8,)),
            dma((8,)),
            dma,
            dma((2,)),
            dma((zs,)),
            dma((zs,)),
            dma((xs, zs)),
            dma((xs, zs)),
            dma((xs,)),
            dma((xs,)),
        ],
        compiler_params=pltpu.CompilerParams(
            collective_id=1, has_side_effects=True, vmem_limit_bytes=32 << 20
        ),
        name="gathered_rows",
    )(o, l, res, scored, gain, out_weight)


def stats_kernel(
    sizes,
    logits_ref,
    ids_ref,
    out_ref,
    lbuf,
    kbuf,
    ybuf,
    xbuf,
    zbuf,
    e_sem,
    k_sem,
    y_sem,
    x_send,
    x_recv,
    z_send,
    z_recv,
    h_sem,
):
    xs, zs = sizes
    x, yh, z, kc = (lax.axis_index(n) for n in CTX)
    hd = lax.axis_index("head")
    oy, ok, oh = (lax.rem(yh + 1, 2), lax.rem(kc + 1, 2), lax.rem(hd + 1, 2))
    peers = [{"head": oh}, {"core": ok}, {"yh": oy}]
    for dx in range(1, xs):
        peers.append({"x": lax.rem(x + dx, xs)})
    for dz in range(1, zs):
        peers.append({"z": lax.rem(z + dz, zs)})
    greet(peers)

    e_copy = remote(logits_ref.at[oh], lbuf, e_sem.at[0], e_sem.at[1], head=oh)
    e_copy.start()
    e_copy.wait_recv()

    rows, width = lbuf.shape
    tile = min(128, rows)
    for at in range(0, rows, tile):
        span = slice(at, at + tile)
        logits = logits_ref[hd, span].astype(jnp.float32) + lbuf[span].astype(jnp.float32)
        highest = jnp.max(logits, axis=1, keepdims=True)
        total = jnp.sum(jnp.exp(logits - highest), axis=1, keepdims=True)
        match = ids_ref[span] == lax.broadcasted_iota(jnp.int32, (tile, width), 1)
        target = jnp.sum(jnp.where(match, logits, 0.0), axis=1, keepdims=True)
        lane = lax.broadcasted_iota(jnp.int32, (tile, 128), 1)
        packed = jnp.where(lane == 0, highest, jnp.where(lane == 1, total, target))
        kbuf[kc, :, at : at + tile] = jnp.transpose(packed)[:8]

    def merge(buf, count):
        tops = [buf[i, 0:1] for i in range(count)]
        top = functools.reduce(jnp.maximum, tops)
        total = functools.reduce(
            jnp.add, [buf[i, 1:2] * jnp.exp(tops[i] - top) for i in range(count)]
        )
        target = functools.reduce(jnp.add, [buf[i, 2:3] for i in range(count)])
        return jnp.concatenate([top, total] + [target] * 6, axis=0)

    k_copy = remote(kbuf.at[kc], kbuf.at[kc], k_sem.at[0], k_sem.at[1], core=ok)
    k_copy.start()
    k_copy.wait_recv()
    ybuf[yh] = merge(kbuf, 2)
    y_copy = remote(ybuf.at[yh], ybuf.at[yh], y_sem.at[0], y_sem.at[1], yh=oy)
    y_copy.start()
    y_copy.wait_recv()
    xbuf[x] = merge(ybuf, 2)

    def x_copy(d):
        to = lax.rem(x + d, xs)
        return remote(xbuf.at[x], xbuf.at[x], x_send.at[d], x_recv.at[d], x=to)

    for d in range(1, xs):
        x_copy(d).start()
    for d in range(1, xs):
        x_copy(d).wait_recv()
    zbuf[z] = merge(xbuf, xs)

    def z_copy(d):
        to = lax.rem(z + d, zs)
        return remote(zbuf.at[z], zbuf.at[z], z_send.at[d], z_recv.at[d], z=to)

    for d in range(1, zs):
        z_copy(d).start()
    for d in range(1, zs):
        z_copy(d).wait_recv()
    final = merge(zbuf, zs)
    out_ref[hd] = jnp.broadcast_to(final[2:3] - final[0:1] - jnp.log(final[1:2]), final.shape)
    h_copy = remote(out_ref.at[hd], out_ref.at[hd], h_sem.at[0], h_sem.at[1], head=oh)
    h_copy.start()
    h_copy.wait_recv()

    e_copy.wait_send()
    k_copy.wait_send()
    y_copy.wait_send()
    for d in range(1, xs):
        x_copy(d).wait_send()
    for d in range(1, zs):
        z_copy(d).wait_send()
    h_copy.wait_send()


def row_stats(sizes, logits, ids):
    xs, zs = sizes
    _, rows, width = logits.shape
    dma = pltpu.SemaphoreType.DMA
    f32 = jnp.float32
    return pl.pallas_call(
        functools.partial(stats_kernel, sizes),
        out_shape=jax.ShapeDtypeStruct((2, 8, rows), f32),
        in_specs=[pl.BlockSpec(memory_space=VMEM)] * 2,
        out_specs=pl.BlockSpec(memory_space=VMEM),
        scratch_shapes=[
            VMEM((rows, width), jnp.bfloat16),
            VMEM((2, 8, rows), f32),
            VMEM((2, 8, rows), f32),
            VMEM((xs, 8, rows), f32),
            VMEM((zs, 8, rows), f32),
            dma((2,)),
            dma((2,)),
            dma((2,)),
            dma((xs,)),
            dma((xs,)),
            dma((zs,)),
            dma((zs,)),
            dma((2,)),
        ],
        compiler_params=pltpu.CompilerParams(
            collective_id=2, has_side_effects=True, vmem_limit_bytes=24 << 20
        ),
        name="row_stats",
    )(logits, ids)


def per_device(
    sizes,
    queries,
    rotated_keys,
    value_matrix,
    doc_lengths,
    scored,
    residual,
    norm_gain,
    out_weight,
    lm_weight,
    token_ids,
    old_logp,
    advantage,
):
    xs, zs = sizes
    tok = queries.shape[0]
    x, yh, z, kc = (lax.axis_index(n) for n in CTX)
    hd = lax.axis_index("head")
    docs = doc_lengths.shape[0]
    plane = 4 * zs * tok

    kv = jnp.stack([rotated_keys, value_matrix]).reshape(2, tok, 2, HEAD_SIZE)
    kv = jnp.transpose(kv, (2, 0, 1, 3))
    q = jnp.transpose(queries.reshape(tok, 2, -1), (1, 0, 2))
    kvs, qs = exchange(sizes, kv, q)

    block = yh * zs + z
    doc_starts = jnp.cumsum(doc_lengths) - doc_lengths
    q_first = jnp.arange(8, dtype=jnp.int32) * plane + block * 2 * tok
    zz = jnp.arange(zs, dtype=jnp.int32)[:, None]
    yy = jnp.arange(2, dtype=jnp.int32)[None, :]
    source_x = (x - zz + 2 * xs * zs) % xs
    bases = source_x * plane + (yy * zs + zz) * 2 * tok
    meta = jnp.concatenate(
        [q_first, jnp.pad(doc_starts.astype(jnp.int32), (0, 24 - docs)), bases.reshape(-1)]
    )
    o, l = flash(docs, meta, qs, kvs)

    row_slot = 2 * yh + kc
    resp = scored.shape[0]
    mine = (jnp.arange(4, dtype=jnp.int32) == row_slot)[:, None]
    scored16 = jnp.where(mine, scored[None, :], -1).reshape(4 * resp, 1)
    half = residual.shape[1]
    res = jnp.where(mine[:, :, None], residual[None], 0).astype(jnp.bfloat16)
    res = jnp.transpose(res.reshape(4 * resp, 4, half // 4), (1, 0, 2))
    gain = norm_gain.reshape(4, 1, half // 4)
    attended, rows = gathered_rows(sizes, o, l, res, scored16, gain, out_weight)

    count = xs * zs * 4 * resp
    logits = jnp.dot(
        rows.reshape(count, half), lm_weight, preferred_element_type=jnp.float32
    ).astype(jnp.bfloat16)
    vocab = lm_weight.shape[1]
    start = (((x * 2 + yh) * zs + z) * 2 + kc) * vocab
    ids = token_ids.reshape(xs, 2, zs, 2, resp).transpose(0, 2, 1, 3, 4).reshape(2, count // 2)
    ids = lax.dynamic_index_in_dim(ids, hd, 0, keepdims=False)[:, None] - start
    found = row_stats(sizes, logits.reshape(2, count // 2, vocab), ids)
    log_probs = found[:, 0].reshape(xs, zs, 2, 2, resp).transpose(0, 2, 1, 3, 4).reshape(count)
    ratio = jnp.exp(jnp.clip(log_probs - old_logp, -4.0, 4.0))
    token_loss = -jnp.minimum(ratio * advantage, jnp.clip(ratio, 0.8, 1.2) * advantage)
    return (attended, log_probs, token_loss)


def solution(mesh, shape=(4, 2, 8, 2)):
    finer = Mesh(mesh.devices.reshape(*shape, mesh.shape["head"]), NAMES)
    placed = (
        P(CTX, "head"),
        P(CTX, "head"),
        P(CTX, "head"),
        P(),
        P(CTX),
        P(CTX, "head"),
        P("head"),
        P("head", None),
        P("head", CTX),
        P(),
        P(),
        P(),
    )
    return jax.shard_map(
        functools.partial(per_device, (shape[0], shape[2])),
        mesh=finer,
        in_specs=placed,
        out_specs=(P(CTX, "head"), P(), P()),
        check_vma=False,
    )
```

```python
import functools
import math

import jax
import jax.numpy as jnp
from jax import lax
from jax.experimental import pallas as pl
from jax.experimental.pallas import tpu as pltpu
from jax.sharding import Mesh
from jax.sharding import PartitionSpec as P

HEAD_SIZE = 128
CTX = ("x", "yh", "z", "core")
NAMES = ("x", "yh", "z", "core", "head")
NEG = -1e30
SCALE = HEAD_SIZE**-0.5 * math.log2(math.e)
MESH = pl.DeviceIdType.MESH
VMEM = pltpu.VMEM


def remote(src, dst, send_sem, recv_sem, **where):
    return pltpu.make_async_remote_copy(
        src_ref=src,
        dst_ref=dst,
        send_sem=send_sem,
        recv_sem=recv_sem,
        device_id=where,
        device_id_type=MESH,
    )


def greet(peers):
    barrier = pltpu.get_barrier_semaphore()
    for where in peers:
        pl.semaphore_signal(barrier, inc=1, device_id=where, device_id_type=MESH)
    pl.semaphore_wait(barrier, len(peers))


def exchange_kernel(
    sizes,
    k_ref,
    v_ref,
    q_ref,
    hot_ref,
    kvbuf,
    qbuf,
    hotbuf,
    first_send,
    first_recv,
    up_send,
    up_recv,
    down_send,
    down_recv,
    q_send,
    q_recv,
    h_send,
    h_recv,
):
    xs, zs = sizes
    x, yh, z, kc = (lax.axis_index(n) for n in CTX)
    up, down = (lax.rem(z + 1, zs), lax.rem(z + zs - 1, zs))
    shift = lax.rem(z, xs)
    tx = lax.rem(x + z, xs)
    mine = 2 * yh + kc
    group = q_ref.shape[1] // 2
    peers = []
    for dx in range(xs):
        for dy in range(2):
            for dk in range(2):
                if dx or dy or dk:
                    peers.append(
                        {
                            "x": lax.rem(x + dx, xs),
                            "yh": lax.rem(yh + dy, 2),
                            "core": lax.rem(kc + dk, 2),
                        }
                    )
    peers.append({"z": up})
    peers.append({"z": down})
    greet(peers)

    def columns(ref, head, width):
        return ref.at[:, pl.ds(pl.multiple_of(head * width, 128), width)]

    def first(dy, dk):
        ty, tk = (lax.rem(yh + dy, 2), lax.rem(kc + dk, 2))
        return [
            remote(
                columns(ref, tk, HEAD_SIZE),
                kvbuf.at[z, mine, i],
                first_send.at[2 * dy + dk, i],
                first_recv.at[mine, i],
                x=tx,
                yh=ty,
                core=tk,
            )
            for i, ref in enumerate((k_ref, v_ref))
        ]

    def first_here():
        return [
            pltpu.make_async_copy(
                columns(ref, kc, HEAD_SIZE), kvbuf.at[z, mine, i], first_recv.at[mine, i]
            )
            for i, ref in enumerate((k_ref, v_ref))
        ]

    for dy, dk in ((1, 0), (1, 1), (0, 1)):
        for copy in first(dy, dk):
            copy.start()

    @pl.when(shift == 0)
    def _():
        for copy in first_here():
            copy.start()

    @pl.when(shift != 0)
    def _():
        for copy in first(0, 0):
            copy.start()

    def q_copies(dx, dk):
        ox, tk = (lax.rem(x + dx, xs), lax.rem(kc + dk, 2))
        s, own = (2 * dx + dk, 2 * x + kc)
        where = {"x": ox, "core": tk}
        q_part = columns(q_ref, tk, group)
        return (
            remote(hot_ref, hotbuf.at[x, kc], h_send.at[s], h_recv.at[own], **where),
            remote(q_part, qbuf.at[x, kc], q_send.at[s], q_recv.at[own], **where),
        )

    pltpu.make_async_copy(
        columns(q_ref, kc, group), qbuf.at[x, kc], q_recv.at[2 * x + kc]
    ).start()
    pltpu.make_async_copy(hot_ref, hotbuf.at[x, kc], h_recv.at[2 * x + kc]).start()
    q_order = [
        (dx, dk)
        for dx in [0] + sorted(range(1, xs), key=lambda d: min(d, xs - d))
        for dk in (0, 1)
        if dx or dk
    ]
    for dx, dk in q_order:
        for copy in q_copies(dx, dk):
            copy.start()

    def first_wait(s):
        for i in range(2):
            part = kvbuf.at[z, s, i]
            remote(part, part, first_send.at[0, i], first_recv.at[s, i], z=up).wait_recv()

    def ring(going_up, slot, t, h):
        send, recv, to = (up_send, up_recv, up) if going_up else (down_send, down_recv, down)
        part = kvbuf.at[slot, pl.ds(2 * h, 2)]
        return remote(part, part, send.at[t, h], recv.at[t, h], z=to)

    def sent(going_up, t, h):
        slot = lax.rem(z - t + zs, zs) if going_up else lax.rem(z + t, zs)
        return ring(going_up, slot, t, h)

    def got(going_up, t, h):
        slot = lax.rem(z - 1 - t + zs, zs) if going_up else lax.rem(z + 1 + t, zs)
        return ring(going_up, slot, t, h)

    full = (zs - 2) // 2
    for t in range(full):
        for h in range(2):
            if t == 0:
                first_wait(2 * h)
                first_wait(2 * h + 1)
            for going_up in (True, False):
                if t > 0:
                    got(going_up, t - 1, h).wait_recv()
                sent(going_up, t, h).start()
    if full == 0:
        for s in range(4):
            first_wait(s)
    for going_up, h in ((True, 0), (False, 1)):
        if full > 0:
            got(going_up, full - 1, h).wait_recv()
        sent(going_up, full, h).start()
    if full > 0:
        got(True, full - 1, 1).wait_recv()
        got(False, full - 1, 0).wait_recv()
    got(True, full, 0).wait_recv()
    got(False, full, 1).wait_recv()

    for t in range(full):
        for h in range(2):
            for going_up in (True, False):
                sent(going_up, t, h).wait_send()
    sent(True, full, 0).wait_send()
    sent(False, full, 1).wait_send()
    for dy, dk in ((1, 0), (1, 1), (0, 1)):
        for copy in first(dy, dk):
            copy.wait_send()

    @pl.when(shift != 0)
    def _():
        for copy in first(0, 0):
            copy.wait_send()

    for dx, dk in q_order:
        for copy in q_copies(dx, dk):
            copy.wait_send()
    for s in range(2 * xs):
        part = qbuf.at[s // 2, s % 2]
        remote(part, part, q_send.at[0], q_recv.at[s], z=up).wait_recv()
        part = hotbuf.at[s // 2, s % 2]
        remote(part, part, h_send.at[0], h_recv.at[s], z=up).wait_recv()


def exchange(sizes, k, v, q, hot):
    xs, zs = sizes
    tok = q.shape[0]
    full = (zs - 2) // 2
    dma = pltpu.SemaphoreType.DMA
    return pl.pallas_call(
        functools.partial(exchange_kernel, sizes),
        out_shape=(
            jax.ShapeDtypeStruct((zs, 4, 2, tok, HEAD_SIZE), k.dtype),
            jax.ShapeDtypeStruct((xs, 2, tok, q.shape[1] // 2), q.dtype),
            jax.ShapeDtypeStruct((xs, 2, *hot.shape), hot.dtype),
        ),
        in_specs=[pl.BlockSpec(memory_space=VMEM)] * 4,
        out_specs=(pl.BlockSpec(memory_space=VMEM),) * 3,
        scratch_shapes=[
            dma((4, 2)),
            dma((4, 2)),
            dma((full + 1, 2)),
            dma((full + 1, 2)),
            dma((full + 1, 2)),
            dma((full + 1, 2)),
            dma((2 * xs,)),
            dma((2 * xs,)),
            dma((2 * xs,)),
            dma((2 * xs,)),
        ],
        compiler_params=pltpu.CompilerParams(
            collective_id=0, has_side_effects=True, vmem_limit_bytes=24 << 20
        ),
        name="exchange",
    )(k, v, q, hot)


def flash_kernel(
    sizes,
    docs,
    lengths,
    q_ref,
    kv_ref,
    hot_ref,
    o_ref,
    l_ref,
    co_ref,
    cl_ref,
    acc,
    top,
    causal,
    start,
    order,
    where,
):
    xs, zs = sizes
    chunks = 2 * zs
    xq = pl.program_id(0)
    x, yh, z, _ = (lax.axis_index(n) for n in CTX)
    tok = q_ref.shape[2]
    rows = 2 * tok
    plane = chunks * rows
    heads = q_ref.shape[3] // HEAD_SIZE
    first = xq * plane + (yh * zs + z) * rows
    lanes = lax.broadcasted_iota(jnp.int32, (rows, 128), 1)
    positions = first + lax.broadcasted_iota(jnp.int32, (rows, 128), 0)
    begins = jnp.zeros((rows, 128), jnp.int32)
    low = jnp.int32(0)
    doc_start = jnp.int32(0)
    for d in range(docs):
        begins = jnp.where(positions >= doc_start, doc_start, begins)
        low = jnp.where(first >= doc_start, doc_start, low)
        doc_start = doc_start + lengths[d]
    causal[...] = positions - lanes
    start[...] = begins - lanes
    acc[...] = jnp.zeros_like(acc)
    top[...] = jnp.full_like(top, NEG)

    active = jnp.int32(0)
    for i in range(chunks):
        zz, yy = (i // 2, i % 2)
        base = lax.rem(x + 2 * xs * zs - zz, xs) * plane + (yy * zs + zz) * rows
        order[active] = i
        where[active] = base
        active = active + jnp.where((base < first + rows) & (base + rows > low), 1, 0)

    def step(pair, carry):
        one = order[2 * pair]
        whole = 2 * pair + 1 < active
        two = jnp.where(whole, order[2 * pair + 1], one)
        bases = (where[2 * pair], jnp.where(whole, where[2 * pair + 1], 1 << 28))
        keys, values, biases = [], [], []
        for chunk, base in zip((one, two), bases):
            zz, yy = (chunk // 2, lax.rem(chunk, 2))
            for k in range(2):
                keys.append(kv_ref[zz, 2 * yy + k, 0])
                values.append(kv_ref[zz, 2 * yy + k, 1])
                at = base + k * tok
                ok = (causal[...] >= at) & (start[...] <= at)
                biases.append(jnp.where(ok, 0.0, NEG))
        key = jnp.concatenate(keys, axis=0)
        value = jnp.concatenate(values, axis=0)
        value = jnp.concatenate([value, jnp.ones_like(value)], axis=1)
        bias = jnp.concatenate(biases, axis=1)
        for h in range(heads):
            cols = slice(h * HEAD_SIZE, (h + 1) * HEAD_SIZE)
            q = q_ref[0, :, :, cols].reshape(rows, HEAD_SIZE)
            s = lax.dot_general(
                q, key, (((1,), (1,)), ((), ())), preferred_element_type=jnp.float32
            )
            s = s * SCALE + bias
            old = top[h]
            new = jnp.maximum(old, jnp.max(s, axis=1, keepdims=True))
            w = jnp.exp2(s - new[:, :1]).astype(jnp.bfloat16)
            update = jnp.dot(w, value, preferred_element_type=jnp.float32)
            shrink = jnp.exp2(old - new)
            top[h] = new
            acc[h] = acc[h] * jnp.concatenate([shrink, shrink], axis=1) + update
        return carry

    lax.fori_loop(0, (active + 1) // 2, step, 0)

    packed = jnp.zeros((rows, 128), jnp.float32)
    for h in range(heads):
        total = jnp.maximum(acc[h, :, HEAD_SIZE:], 1e-30)
        out = acc[h, :, :HEAD_SIZE] / total
        o_ref[0, :, :, h * HEAD_SIZE : (h + 1) * HEAD_SIZE] = out.astype(jnp.bfloat16).reshape(
            2, tok, HEAD_SIZE
        )
        packed = jnp.where(lanes == h, top[h] + jnp.log2(total), packed)
    chosen, levels = 0.0, 0.0
    for k in range(2):
        level = packed[k * tok : (k + 1) * tok]
        l_ref[0, k] = jnp.transpose(level)[:8]
        hot = hot_ref[0, k]
        chosen = chosen + jnp.dot(hot, o_ref[0, k], preferred_element_type=jnp.float32)
        levels = levels + jnp.dot(
            hot.astype(jnp.float32),
            level,
            preferred_element_type=jnp.float32,
            precision=lax.Precision.HIGHEST,
        )
    co_ref[0] = chosen.astype(jnp.bfloat16)
    cl_ref[0] = levels


def flash(sizes, lengths, q, kv, hot):
    xs, _, tok, width = q.shape
    heads = width // HEAD_SIZE
    keys = kv.shape[0] * 4 * tok
    rows = 2 * tok
    picks = hot.shape[2]

    def whole(*shape):
        return pl.BlockSpec((1, *shape), lambda i: (i,) + (0,) * len(shape))

    return pl.pallas_call(
        functools.partial(flash_kernel, sizes, lengths.shape[0]),
        out_shape=(
            jax.ShapeDtypeStruct(q.shape, jnp.bfloat16),
            jax.ShapeDtypeStruct((xs, 2, 8, 128), jnp.float32),
            jax.ShapeDtypeStruct((xs, picks, width), jnp.bfloat16),
            jax.ShapeDtypeStruct((xs, picks, 128), jnp.float32),
        ),
        grid=(xs,),
        in_specs=[
            pl.BlockSpec(memory_space=pltpu.SMEM),
            whole(2, tok, width),
            pl.BlockSpec(memory_space=VMEM),
            whole(2, picks, 128),
        ],
        out_specs=(
            whole(2, tok, width),
            whole(2, 8, 128),
            whole(picks, width),
            whole(picks, 128),
        ),
        scratch_shapes=[
            VMEM((heads, rows, 2 * HEAD_SIZE), jnp.float32),
            VMEM((heads, rows, 128), jnp.float32),
            VMEM((rows, 128), jnp.int32),
            VMEM((rows, 128), jnp.int32),
            pltpu.SMEM((2 * sizes[1] + 2,), jnp.int32),
            pltpu.SMEM((2 * sizes[1] + 2,), jnp.int32),
        ],
        compiler_params=pltpu.CompilerParams(vmem_limit_bytes=32 << 20),
        cost_estimate=pl.CostEstimate(
            flops=4 * heads * xs * rows * keys * HEAD_SIZE // 3,
            bytes_accessed=4 << 20,
            transcendentals=heads * xs * rows * keys // 3,
        ),
        name="flash",
    )(lengths, q, kv, hot)


def shares_of(levels):
    highest = functools.reduce(jnp.maximum, levels)
    parts = [jnp.exp2(level - highest) for level in levels]
    total = functools.reduce(jnp.add, parts)
    return [part / total for part in parts]


def tail_kernel(
    sizes,
    width_full,
    o_ref,
    l_ref,
    co_ref,
    cl_ref,
    res_ref,
    gain_ref,
    ids_ref,
    ow_ref,
    lm_ref,
    att_ref,
    out_ref,
    obuf,
    lbuf,
    cobuf,
    clbuf,
    rbuf,
    wbuf,
    lmbuf,
    psend,
    pbuf,
    sqbuf,
    ubuf,
    g_ref,
    logits,
    arrived,
    kbuf,
    ybuf,
    xbuf,
    zbuf,
    w_sem,
    o_send,
    o_recv,
    l_send,
    l_recv,
    c_send,
    c_recv,
    r_send,
    r_recv,
    p_sem,
    s_send,
    s_recv,
    u_sem,
    y_sem,
    z_send,
    z_recv,
    x_send,
    x_recv,
    k_send,
    k_recv,
    e_send,
    e_recv,
    mk_sem,
    my_sem,
    mx_send,
    mx_recv,
    mz_send,
    mz_recv,
    mh_sem,
):
    xs, zs = sizes
    x, yh, z, kc = (lax.axis_index(n) for n in CTX)
    hd = lax.axis_index("head")
    oy, ok, oh = (lax.rem(yh + 1, 2), lax.rem(kc + 1, 2), lax.rem(hd + 1, 2))
    row_slot = 2 * yh + kc
    quarter = 2 * kc + yh
    half = width_full // 2
    wide = half // 4
    heads = o_ref.shape[3] // HEAD_SIZE
    z_order = sorted(range(1, zs), key=lambda d: min(d, zs - d))
    x_order = sorted(range(1, xs), key=lambda d: min(d, xs - d))
    near = ((0, 1), (1, 0), (1, 1))

    weights = []
    for j, side in enumerate((hd, oh)):
        col = pl.multiple_of(side * half + quarter * wide, 128)
        weights.append(
            pltpu.make_async_copy(ow_ref.at[:, pl.ds(col, wide)], wbuf.at[j], w_sem.at[j])
        )
        weights[-1].start()
    embedding = pltpu.make_async_copy(lm_ref, lmbuf, w_sem.at[2])
    embedding.start()

    peers = []
    for dx in range(xs):
        for dy in range(2):
            for dk in range(2):
                if dx or dy or dk:
                    peers.append(
                        {
                            "x": lax.rem(x + dx, xs),
                            "yh": lax.rem(yh + dy, 2),
                            "core": lax.rem(kc + dk, 2),
                        }
                    )
    for where in ({}, {"core": ok}, {"yh": oy}, {"yh": oy, "core": ok}):
        peers.append({"head": oh, **where})
    for dz in range(1, zs):
        peers.append({"z": lax.rem(z + dz, zs)})
    greet(peers)

    def c_copies(dx, dy, dk):
        where = {
            "x": lax.rem(x + dx, xs),
            "yh": lax.rem(yh + dy, 2),
            "core": lax.rem(kc + dk, 2),
        }
        at = where["x"]
        own = (x, yh, kc)
        return (
            remote(
                cl_ref.at[at],
                clbuf.at[own],
                c_send.at[0, 4 * dx + 2 * dy + dk],
                c_recv.at[0, 4 * x + row_slot],
                **where,
            ),
            remote(
                co_ref.at[at],
                cobuf.at[own],
                c_send.at[1, 4 * dx + 2 * dy + dk],
                c_recv.at[1, 4 * x + row_slot],
                **where,
            ),
        )

    c_order = [
        (dx, dy, dk)
        for dx in list(reversed(x_order)) + [0]
        for dy in (1, 0)
        for dk in (0, 1)
        if dx or dy or dk
    ]
    for each in c_order:
        for copy in c_copies(*each):
            copy.start()
    pltpu.make_async_copy(
        cl_ref.at[x], clbuf.at[x, yh, kc], c_recv.at[0, 4 * x + row_slot]
    ).start()
    pltpu.make_async_copy(
        co_ref.at[x], cobuf.at[x, yh, kc], c_recv.at[1, 4 * x + row_slot]
    ).start()

    def r_copy(dy, dk):
        ty, tk = (lax.rem(yh + dy, 2), lax.rem(kc + dk, 2))
        return remote(
            res_ref.at[2 * tk + ty],
            rbuf.at[row_slot],
            r_send.at[2 * dy + dk],
            r_recv.at[row_slot],
            yh=ty,
            core=tk,
        )

    for dy, dk in near:
        r_copy(dy, dk).start()
    pltpu.make_async_copy(res_ref.at[quarter], rbuf.at[row_slot], r_recv.at[row_slot]).start()

    def o_copies(dx, dk):
        tx, tk = (lax.rem(x + dx, xs), lax.rem(kc + dk, 2))
        where = {"x": tx, "core": tk}
        s, mine = (2 * dx + dk, 2 * x + kc)
        return (
            remote(l_ref.at[tx, tk], lbuf.at[x, kc], l_send.at[s], l_recv.at[mine], **where),
            remote(o_ref.at[tx, tk], obuf.at[x, kc], o_send.at[s], o_recv.at[mine], **where),
        )

    o_order = [
        (dx, dk) for dx in list(reversed(x_order)) + [0] for dk in (0, 1) if dx or dk
    ]
    for dx, dk in o_order:
        for copy in o_copies(dx, dk):
            copy.start()
    pltpu.make_async_copy(o_ref.at[x, kc], obuf.at[x, kc], o_recv.at[2 * x + kc]).start()
    pltpu.make_async_copy(l_ref.at[x, kc], lbuf.at[x, kc], l_recv.at[2 * x + kc]).start()

    for s in range(4 * xs):
        at = (s // 4, s // 2 % 2, s % 2)
        for i, buf in enumerate((clbuf, cobuf)):
            part = buf.at[at]
            remote(part, part, c_send.at[i, 0], c_recv.at[i, s], head=oh).wait_recv()
    pieces = []
    for k in range(2):
        shares = shares_of([clbuf[j, 0, k] + clbuf[j, 1, k] for j in range(xs)])
        values = [(cobuf[j, 0, k] + cobuf[j, 1, k]).astype(jnp.float32) for j in range(xs)]
        for h in range(heads):
            cols = slice(h * HEAD_SIZE, (h + 1) * HEAD_SIZE)
            merged = sum(shares[j][:, h : h + 1] * values[j][:, cols] for j in range(xs))
            pieces.append(merged.astype(jnp.bfloat16))
    chosen = jnp.concatenate(pieces, axis=1)

    for copy in weights:
        copy.wait()
    psend[...] = jnp.dot(chosen, wbuf[1], preferred_element_type=jnp.float32).astype(jnp.bfloat16)
    p_copy = remote(psend, pbuf, p_sem.at[0], p_sem.at[1], head=oh)
    p_copy.start()
    hidden = jnp.dot(chosen, wbuf[0], preferred_element_type=jnp.float32)
    for s in range(4):
        part = rbuf.at[s]
        remote(part, part, r_send.at[0], r_recv.at[s], head=oh).wait_recv()
    residual = (rbuf[0] + rbuf[1]) + (rbuf[2] + rbuf[3])
    p_copy.wait_recv()
    hidden = residual.astype(jnp.float32) + (hidden + pbuf[...].astype(jnp.float32))

    own = 4 * hd + row_slot
    sqbuf[own] = jnp.broadcast_to(jnp.sum(hidden * hidden, axis=1, keepdims=True), (16, 128))

    def s_copy(d):
        dh, dy, dk = (d // 4, d // 2 % 2, d % 2)
        return remote(
            sqbuf.at[own],
            sqbuf.at[own],
            s_send.at[d],
            s_recv.at[d],
            head=lax.rem(hd + dh, 2),
            yh=lax.rem(yh + dy, 2),
            core=lax.rem(kc + dk, 2),
        )

    for d in range(1, 8):
        s_copy(d).start()
    for d in range(1, 8):
        s_copy(d).wait_recv()
    squares = functools.reduce(jnp.add, [sqbuf[s] for s in range(8)])
    scale = lax.rsqrt(squares / width_full + 1e-05)[:, :1]
    ubuf[...] = (hidden * scale * gain_ref[quarter]).astype(jnp.bfloat16)

    mine = pl.ds(pl.multiple_of(quarter * wide, 128), wide)
    both = pl.ds(pl.multiple_of(kc * 2 * wide, 128), 2 * wide)
    here = pltpu.make_async_copy(ubuf, g_ref.at[x, z, :, mine], u_sem)
    here.start()
    y_copy = remote(ubuf, g_ref.at[x, z, :, mine], y_sem.at[0], y_sem.at[1], yh=oy)
    y_copy.start()
    here.wait()
    y_copy.wait_recv()

    def block(bx, bz):
        return g_ref.at[bx, bz, :, both]

    def z_copy(dz):
        to = lax.rem(z + dz, zs)
        return remote(block(x, z), block(x, z), z_send.at[dz], z_recv.at[dz], z=to)

    def x_copy(dx, dz):
        bz = lax.rem(z + zs - dz, zs)
        to = lax.rem(x + dx, xs)
        return remote(block(x, bz), block(x, bz), x_send.at[dx, dz], x_recv.at[dx, dz], x=to)

    def plane_of(dx):
        return lax.rem(x + xs - dx, xs)

    def k_copy(dx):
        plane = g_ref.at[plane_of(dx), :, :, both]
        return remote(plane, plane, k_send.at[dx], k_recv.at[dx], core=ok)

    def e_copy(dx):
        at = plane_of(dx)
        return remote(
            logits.at[at, oh], arrived.at[at], e_send.at[dx], e_recv.at[dx], head=oh
        )

    def project(dx):
        at = plane_of(dx)
        k_copy(dx).wait_recv()
        rows = g_ref[at].reshape(zs * 16, half)
        out = jnp.dot(rows, lmbuf[...], preferred_element_type=jnp.float32)
        logits[at] = out.astype(jnp.bfloat16).reshape(logits.shape[1:])
        e_copy(dx).start()

    def reduce_plane(dx):
        at = plane_of(dx)
        e_copy(dx).wait_recv()
        both_halves = logits[at, hd].astype(jnp.float32) + arrived[at].astype(jnp.float32)
        rows, width = both_halves.shape
        highest = jnp.max(both_halves, axis=1, keepdims=True)
        total = jnp.sum(jnp.exp(both_halves - highest), axis=1, keepdims=True)
        match = ids_ref[at] == lax.broadcasted_iota(jnp.int32, (rows, width), 1)
        target = jnp.sum(jnp.where(match, both_halves, 0.0), axis=1, keepdims=True)
        lane = lax.broadcasted_iota(jnp.int32, (rows, 128), 1)
        packed = jnp.where(lane == 0, highest, jnp.where(lane == 1, total, target))
        kbuf[kc, at] = jnp.transpose(packed)[:8]

    for dz in reversed(z_order):
        z_copy(dz).start()
    for dz in [0] + z_order:
        if dz:
            z_copy(dz).wait_recv()
        for dx in x_order:
            x_copy(dx, dz).start()
    k_copy(0).start()

    for s in range(2 * xs):
        at = (s // 2, s % 2)
        for buf, send, recv in ((lbuf, l_send, l_recv), (obuf, o_send, o_recv)):
            part = buf.at[at]
            remote(part, part, send.at[0], recv.at[s], head=oh).wait_recv()
    for k in range(2):
        parts = shares_of([lbuf[j, k] for j in range(xs)])
        parts.append(jnp.zeros((128 - 8 * xs, 128), jnp.float32))
        shares = jnp.transpose(jnp.concatenate(parts, axis=0))
        for h in range(heads):
            cols = slice(h * HEAD_SIZE, (h + 1) * HEAD_SIZE)
            merged = sum(
                shares[:, 8 * j + h : 8 * j + h + 1] * obuf[j, k, :, cols].astype(jnp.float32)
                for j in range(xs)
            )
            at = (k * heads + h) * HEAD_SIZE
            att_ref[:, at : at + HEAD_SIZE] = merged.astype(jnp.bfloat16)

    embedding.wait()
    project(0)
    last = 0
    for dx in x_order:
        for dz in [0] + z_order:
            x_copy(dx, dz).wait_recv()
        k_copy(dx).start()
        reduce_plane(last)
        project(dx)
        last = dx
    reduce_plane(last)

    def merge(buf, count):
        tops = [buf[i, :, 0:1] for i in range(count)]
        top = functools.reduce(jnp.maximum, tops)
        total = functools.reduce(
            jnp.add, [buf[i, :, 1:2] * jnp.exp(tops[i] - top) for i in range(count)]
        )
        target = functools.reduce(jnp.add, [buf[i, :, 2:3] for i in range(count)])
        return jnp.concatenate([top, total] + [target] * 6, axis=1)

    mk_copy = remote(kbuf.at[kc], kbuf.at[kc], mk_sem.at[0], mk_sem.at[1], core=ok)
    mk_copy.start()
    mk_copy.wait_recv()
    ybuf[yh] = merge(kbuf, 2)
    my_copy = remote(ybuf.at[yh], ybuf.at[yh], my_sem.at[0], my_sem.at[1], yh=oy)
    my_copy.start()
    my_copy.wait_recv()
    xbuf[x] = merge(ybuf, 2)

    def mx_copy(d):
        to = lax.rem(x + d, xs)
        return remote(xbuf.at[x], xbuf.at[x], mx_send.at[d], mx_recv.at[d], x=to)

    for d in range(1, xs):
        mx_copy(d).start()
    for d in range(1, xs):
        mx_copy(d).wait_recv()
    zbuf[z] = merge(xbuf, xs)

    def mz_copy(d):
        to = lax.rem(z + d, zs)
        return remote(zbuf.at[z], zbuf.at[z], mz_send.at[d], mz_recv.at[d], z=to)

    for d in range(1, zs):
        mz_copy(d).start()
    for d in range(1, zs):
        mz_copy(d).wait_recv()
    final = merge(zbuf, zs)
    final = final[:, 2:3] - final[:, 0:1] - jnp.log(final[:, 1:2])
    out_ref[hd] = jnp.broadcast_to(final, out_ref.shape[1:])
    mh_copy = remote(out_ref.at[hd], out_ref.at[hd], mh_sem.at[0], mh_sem.at[1], head=oh)
    mh_copy.start()
    mh_copy.wait_recv()

    for each in c_order:
        for copy in c_copies(*each):
            copy.wait_send()
    for dy, dk in near:
        r_copy(dy, dk).wait_send()
    for dx, dk in o_order:
        for copy in o_copies(dx, dk):
            copy.wait_send()
    p_copy.wait_send()
    for d in range(1, 8):
        s_copy(d).wait_send()
    y_copy.wait_send()
    for dz in z_order:
        z_copy(dz).wait_send()
    for dx in x_order:
        for dz in range(zs):
            x_copy(dx, dz).wait_send()
    for dx in range(xs):
        k_copy(dx).wait_send()
        e_copy(dx).wait_send()
    mk_copy.wait_send()
    my_copy.wait_send()
    for d in range(1, xs):
        mx_copy(d).wait_send()
    for d in range(1, zs):
        mz_copy(d).wait_send()
    mh_copy.wait_send()


def tail(sizes, o, l, co, cl, res, gain, ids, out_weight, lm_weight):
    xs, zs = sizes
    tok = o.shape[2]
    depth, width_full = out_weight.shape
    half, vocab = lm_weight.shape
    wide = half // 4
    side = zs * 8
    dma = pltpu.SemaphoreType.DMA
    bf16, f32 = (jnp.bfloat16, jnp.float32)
    hbm = pl.BlockSpec(memory_space=pltpu.HBM)
    return pl.pallas_call(
        functools.partial(tail_kernel, sizes, width_full),
        out_shape=(
            jax.ShapeDtypeStruct((tok, depth), bf16),
            jax.ShapeDtypeStruct((2, xs, 8, side), f32),
        ),
        in_specs=[pl.BlockSpec(memory_space=VMEM)] * 7 + [hbm] * 2,
        out_specs=(pl.BlockSpec(memory_space=VMEM),) * 2,
        scratch_shapes=[
            VMEM(o.shape, bf16),
            VMEM(l.shape, f32),
            VMEM((xs, 2, 2, *co.shape[1:]), bf16),
            VMEM((xs, 2, 2, *cl.shape[1:]), f32),
            VMEM((4, 16, wide), bf16),
            VMEM((2, depth, wide), bf16),
            VMEM((half, vocab), bf16),
            VMEM((16, wide), bf16),
            VMEM((16, wide), bf16),
            VMEM((8, 16, 128), f32),
            VMEM((16, wide), bf16),
            VMEM((xs, zs, 16, half), bf16),
            VMEM((xs, 2, side, vocab), bf16),
            VMEM((xs, side, vocab), bf16),
            VMEM((2, xs, 8, side), f32),
            VMEM((2, xs, 8, side), f32),
            VMEM((xs, xs, 8, side), f32),
            VMEM((zs, xs, 8, side), f32),
            dma((3,)),
            dma((2 * xs,)),
            dma((2 * xs,)),
            dma((2 * xs,)),
            dma((2 * xs,)),
            dma((2, 4 * xs)),
            dma((2, 4 * xs)),
            dma((4,)),
            dma((4,)),
            dma((2,)),
            dma((8,)),
            dma((8,)),
            dma,
            dma((2,)),
            dma((zs,)),
            dma((zs,)),
            dma((xs, zs)),
            dma((xs, zs)),
            dma((xs,)),
            dma((xs,)),
            dma((xs,)),
            dma((xs,)),
            dma((2,)),
            dma((2,)),
            dma((xs,)),
            dma((xs,)),
            dma((zs,)),
            dma((zs,)),
            dma((2,)),
        ],
        compiler_params=pltpu.CompilerParams(
            collective_id=1, has_side_effects=True, vmem_limit_bytes=48 << 20
        ),
        name="tail",
    )(o, l, co, cl, res, gain, ids, out_weight, lm_weight)


def per_device(
    sizes,
    queries,
    rotated_keys,
    value_matrix,
    doc_lengths,
    scored,
    residual,
    norm_gain,
    out_weight,
    lm_weight,
    token_ids,
    old_logp,
    advantage,
):
    xs, zs = sizes
    tok = queries.shape[0]
    x, yh, z, kc = (lax.axis_index(n) for n in CTX)
    hd = lax.axis_index("head")
    resp = scored.shape[0]
    half = residual.shape[1]
    mine = (jnp.arange(4, dtype=jnp.int32) == 2 * yh + kc)[:, None]
    spots = jnp.where(mine, scored[None, :], -1).reshape(4 * resp, 1)
    hot = (spots == jnp.arange(tok, dtype=jnp.int32)[None, :]).astype(jnp.bfloat16)
    kvs, qs, hots = exchange(sizes, rotated_keys, value_matrix, queries, hot)
    o, l, co, cl = flash(sizes, doc_lengths, qs, kvs, hots)

    res = jnp.where(mine[:, :, None], residual[None], 0).astype(jnp.bfloat16)
    res = jnp.transpose(res.reshape(4 * resp, 4, half // 4), (1, 0, 2))
    gain = norm_gain.reshape(4, 1, half // 4)
    vocab = lm_weight.shape[1]
    start = (((x * 2 + yh) * zs + z) * 2 + kc) * vocab
    ids = token_ids.reshape(xs, 2, 2, zs // 2, 2, resp).transpose(2, 0, 3, 1, 4, 5)
    ids = lax.dynamic_index_in_dim(ids.reshape(2, xs, -1, 1), hd, 0, keepdims=False) - start
    attended, found = tail(sizes, o, l, co, cl, res, gain, ids, out_weight, lm_weight)
    found = found[:, :, 0].reshape(2, xs, zs // 2, 2, 2, resp)
    log_probs = found.transpose(1, 3, 0, 2, 4, 5).reshape(-1)
    ratio = jnp.exp(jnp.clip(log_probs - old_logp, -4.0, 4.0))
    token_loss = -jnp.minimum(ratio * advantage, jnp.clip(ratio, 0.8, 1.2) * advantage)
    return (attended, log_probs, token_loss)


def solution(mesh, shape=(4, 2, 8, 2)):
    finer = Mesh(mesh.devices.reshape(*shape, mesh.shape["head"]), NAMES)
    placed = (
        P(CTX, "head"),
        P(CTX, "head"),
        P(CTX, "head"),
        P(),
        P(CTX),
        P(CTX, "head"),
        P("head"),
        P("head", None),
        P("head", CTX),
        P(),
        P(),
        P(),
    )
    return jax.shard_map(
        functools.partial(per_device, (shape[0], shape[2])),
        mesh=finer,
        in_specs=placed,
        out_specs=(P(CTX, "head"), P(), P()),
        check_vma=False,
    )
```

```python
import functools
import math

import jax
import jax.numpy as jnp
from jax import lax
from jax.experimental import pallas as pl
from jax.experimental.pallas import tpu as pltpu
from jax.sharding import Mesh
from jax.sharding import PartitionSpec as P

HEAD_SIZE = 128
CTX = ("x", "yh", "z", "core")
NAMES = ("x", "yh", "z", "core", "head")
NEG = -1e30
SCALE = HEAD_SIZE**-0.5 * math.log2(math.e)
MESH = pl.DeviceIdType.MESH
VMEM = pltpu.VMEM


def remote(src, dst, send_sem, recv_sem, **where):
    return pltpu.make_async_remote_copy(
        src_ref=src,
        dst_ref=dst,
        send_sem=send_sem,
        recv_sem=recv_sem,
        device_id=where,
        device_id_type=MESH,
    )


def greet(peers):
    barrier = pltpu.get_barrier_semaphore()
    for where in peers:
        pl.semaphore_signal(barrier, inc=1, device_id=where, device_id_type=MESH)
    pl.semaphore_wait(barrier, len(peers))


def exchange_kernel(
    sizes,
    k_ref,
    v_ref,
    q_ref,
    hot_ref,
    res_ref,
    kvbuf,
    qbuf,
    hotbuf,
    resbuf,
    first_send,
    first_recv,
    up_send,
    up_recv,
    down_send,
    down_recv,
    q_send,
    q_recv,
    h_send,
    h_recv,
    r_send,
    r_recv,
):
    xs, zs = sizes
    x, yh, z, kc = (lax.axis_index(n) for n in CTX)
    up, down = (lax.rem(z + 1, zs), lax.rem(z + zs - 1, zs))
    shift = lax.rem(z, xs)
    tx = lax.rem(x + z, xs)
    mine = 2 * yh + kc
    group = q_ref.shape[1] // 2
    peers = []
    for dx in range(xs):
        for dy in range(2):
            for dk in range(2):
                if dx or dy or dk:
                    peers.append(
                        {
                            "x": lax.rem(x + dx, xs),
                            "yh": lax.rem(yh + dy, 2),
                            "core": lax.rem(kc + dk, 2),
                        }
                    )
    peers.append({"z": up})
    peers.append({"z": down})
    greet(peers)

    def columns(ref, head, width):
        return ref.at[:, pl.ds(pl.multiple_of(head * width, 128), width)]

    def first(dy, dk):
        ty, tk = (lax.rem(yh + dy, 2), lax.rem(kc + dk, 2))
        return [
            remote(
                columns(ref, tk, HEAD_SIZE),
                kvbuf.at[z, mine, i],
                first_send.at[2 * dy + dk, i],
                first_recv.at[mine, i],
                x=tx,
                yh=ty,
                core=tk,
            )
            for i, ref in enumerate((k_ref, v_ref))
        ]

    def first_here():
        return [
            pltpu.make_async_copy(
                columns(ref, kc, HEAD_SIZE), kvbuf.at[z, mine, i], first_recv.at[mine, i]
            )
            for i, ref in enumerate((k_ref, v_ref))
        ]

    for dy, dk in ((1, 0), (1, 1), (0, 1)):
        for copy in first(dy, dk):
            copy.start()

    @pl.when(shift == 0)
    def _():
        for copy in first_here():
            copy.start()

    @pl.when(shift != 0)
    def _():
        for copy in first(0, 0):
            copy.start()

    def q_copies(dx, dk):
        ox, tk = (lax.rem(x + dx, xs), lax.rem(kc + dk, 2))
        s, own = (2 * dx + dk, 2 * x + kc)
        where = {"x": ox, "core": tk}
        q_part = columns(q_ref, tk, group)
        return (
            remote(hot_ref, hotbuf.at[x, kc], h_send.at[s], h_recv.at[own], **where),
            remote(q_part, qbuf.at[x, kc], q_send.at[s], q_recv.at[own], **where),
        )

    pltpu.make_async_copy(
        columns(q_ref, kc, group), qbuf.at[x, kc], q_recv.at[2 * x + kc]
    ).start()
    pltpu.make_async_copy(hot_ref, hotbuf.at[x, kc], h_recv.at[2 * x + kc]).start()
    q_order = [
        (dx, dk)
        for dx in [0] + sorted(range(1, xs), key=lambda d: min(d, xs - d))
        for dk in (0, 1)
        if dx or dk
    ]
    for dx, dk in q_order:
        for copy in q_copies(dx, dk):
            copy.start()

    near = ((0, 1), (1, 0), (1, 1))

    def r_copy(dy, dk):
        ty, tk = (lax.rem(yh + dy, 2), lax.rem(kc + dk, 2))
        return remote(
            res_ref.at[tk],
            resbuf.at[mine],
            r_send.at[2 * dy + dk],
            r_recv.at[mine],
            yh=ty,
            core=tk,
        )

    for dy, dk in near:
        r_copy(dy, dk).start()
    pltpu.make_async_copy(res_ref.at[kc], resbuf.at[mine], r_recv.at[mine]).start()

    def first_wait(s):
        for i in range(2):
            part = kvbuf.at[z, s, i]
            remote(part, part, first_send.at[0, i], first_recv.at[s, i], z=up).wait_recv()

    def ring(going_up, slot, t, h):
        send, recv, to = (up_send, up_recv, up) if going_up else (down_send, down_recv, down)
        part = kvbuf.at[slot, pl.ds(2 * h, 2)]
        return remote(part, part, send.at[t, h], recv.at[t, h], z=to)

    def sent(going_up, t, h):
        slot = lax.rem(z - t + zs, zs) if going_up else lax.rem(z + t, zs)
        return ring(going_up, slot, t, h)

    def got(going_up, t, h):
        slot = lax.rem(z - 1 - t + zs, zs) if going_up else lax.rem(z + 1 + t, zs)
        return ring(going_up, slot, t, h)

    full = (zs - 2) // 2
    for t in range(full):
        for h in range(2):
            if t == 0:
                first_wait(2 * h)
                first_wait(2 * h + 1)
            for going_up in (True, False):
                if t > 0:
                    got(going_up, t - 1, h).wait_recv()
                sent(going_up, t, h).start()
    if full == 0:
        for s in range(4):
            first_wait(s)
    for going_up, h in ((True, 0), (False, 1)):
        if full > 0:
            got(going_up, full - 1, h).wait_recv()
        sent(going_up, full, h).start()
    if full > 0:
        got(True, full - 1, 1).wait_recv()
        got(False, full - 1, 0).wait_recv()
    got(True, full, 0).wait_recv()
    got(False, full, 1).wait_recv()

    for t in range(full):
        for h in range(2):
            for going_up in (True, False):
                sent(going_up, t, h).wait_send()
    sent(True, full, 0).wait_send()
    sent(False, full, 1).wait_send()
    for dy, dk in ((1, 0), (1, 1), (0, 1)):
        for copy in first(dy, dk):
            copy.wait_send()

    @pl.when(shift != 0)
    def _():
        for copy in first(0, 0):
            copy.wait_send()

    for dy, dk in near:
        r_copy(dy, dk).wait_send()
    for s in range(4):
        part = resbuf.at[s]
        remote(part, part, r_send.at[0], r_recv.at[s], z=up).wait_recv()
    for dx, dk in q_order:
        for copy in q_copies(dx, dk):
            copy.wait_send()
    for s in range(2 * xs):
        part = qbuf.at[s // 2, s % 2]
        remote(part, part, q_send.at[0], q_recv.at[s], z=up).wait_recv()
        part = hotbuf.at[s // 2, s % 2]
        remote(part, part, h_send.at[0], h_recv.at[s], z=up).wait_recv()


def exchange(sizes, k, v, q, hot, res):
    xs, zs = sizes
    tok = q.shape[0]
    full = (zs - 2) // 2
    dma = pltpu.SemaphoreType.DMA
    return pl.pallas_call(
        functools.partial(exchange_kernel, sizes),
        out_shape=(
            jax.ShapeDtypeStruct((zs, 4, 2, tok, HEAD_SIZE), k.dtype),
            jax.ShapeDtypeStruct((xs, 2, tok, q.shape[1] // 2), q.dtype),
            jax.ShapeDtypeStruct((xs, 2, *hot.shape), hot.dtype),
            jax.ShapeDtypeStruct((4, *res.shape[1:]), res.dtype),
        ),
        in_specs=[pl.BlockSpec(memory_space=VMEM)] * 5,
        out_specs=(pl.BlockSpec(memory_space=VMEM),) * 4,
        scratch_shapes=[
            dma((4, 2)),
            dma((4, 2)),
            dma((full + 1, 2)),
            dma((full + 1, 2)),
            dma((full + 1, 2)),
            dma((full + 1, 2)),
            dma((2 * xs,)),
            dma((2 * xs,)),
            dma((2 * xs,)),
            dma((2 * xs,)),
            dma((4,)),
            dma((4,)),
        ],
        compiler_params=pltpu.CompilerParams(
            collective_id=0, has_side_effects=True, vmem_limit_bytes=24 << 20
        ),
        name="exchange",
    )(k, v, q, hot, res)


def flash_kernel(
    sizes,
    docs,
    lengths,
    q_ref,
    kv_ref,
    hot_ref,
    o_ref,
    l_ref,
    co_ref,
    cl_ref,
    acc,
    top,
    causal,
    start,
    order,
    where,
):
    xs, zs = sizes
    chunks = 2 * zs
    xq = pl.program_id(0)
    x, yh, z, _ = (lax.axis_index(n) for n in CTX)
    tok = q_ref.shape[2]
    rows = 2 * tok
    plane = chunks * rows
    heads = q_ref.shape[3] // HEAD_SIZE
    first = xq * plane + (yh * zs + z) * rows
    lanes = lax.broadcasted_iota(jnp.int32, (rows, 128), 1)
    positions = first + lax.broadcasted_iota(jnp.int32, (rows, 128), 0)
    begins = jnp.zeros((rows, 128), jnp.int32)
    low = jnp.int32(0)
    doc_start = jnp.int32(0)
    for d in range(docs):
        begins = jnp.where(positions >= doc_start, doc_start, begins)
        low = jnp.where(first >= doc_start, doc_start, low)
        doc_start = doc_start + lengths[d]
    causal[...] = positions - lanes
    start[...] = begins - lanes
    acc[...] = jnp.zeros_like(acc)
    top[...] = jnp.full_like(top, NEG)

    active = jnp.int32(0)
    for i in range(chunks):
        zz, yy = (i // 2, i % 2)
        base = lax.rem(x + 2 * xs * zs - zz, xs) * plane + (yy * zs + zz) * rows
        order[active] = i
        where[active] = base
        active = active + jnp.where((base < first + rows) & (base + rows > low), 1, 0)

    def step(pair, carry):
        one = order[2 * pair]
        whole = 2 * pair + 1 < active
        two = jnp.where(whole, order[2 * pair + 1], one)
        bases = (where[2 * pair], jnp.where(whole, where[2 * pair + 1], 1 << 28))
        keys, values, biases = [], [], []
        for chunk, base in zip((one, two), bases):
            zz, yy = (chunk // 2, lax.rem(chunk, 2))
            for k in range(2):
                keys.append(kv_ref[zz, 2 * yy + k, 0])
                values.append(kv_ref[zz, 2 * yy + k, 1])
                at = base + k * tok
                ok = (causal[...] >= at) & (start[...] <= at)
                biases.append(jnp.where(ok, 0.0, NEG))
        key = jnp.concatenate(keys, axis=0)
        value = jnp.concatenate(values, axis=0)
        value = jnp.concatenate([value, jnp.ones_like(value)], axis=1)
        bias = jnp.concatenate(biases, axis=1)
        for h in range(heads):
            cols = slice(h * HEAD_SIZE, (h + 1) * HEAD_SIZE)
            q = q_ref[0, :, :, cols].reshape(rows, HEAD_SIZE)
            s = lax.dot_general(
                q, key, (((1,), (1,)), ((), ())), preferred_element_type=jnp.float32
            )
            s = s * SCALE + bias
            old = top[h]
            new = jnp.maximum(old, jnp.max(s, axis=1, keepdims=True))
            w = jnp.exp2(s - new[:, :1]).astype(jnp.bfloat16)
            update = jnp.dot(w, value, preferred_element_type=jnp.float32)
            shrink = jnp.exp2(old - new)
            top[h] = new
            acc[h] = acc[h] * jnp.concatenate([shrink, shrink], axis=1) + update
        return carry

    lax.fori_loop(0, (active + 1) // 2, step, 0)

    packed = jnp.zeros((rows, 128), jnp.float32)
    for h in range(heads):
        total = jnp.maximum(acc[h, :, HEAD_SIZE:], 1e-30)
        out = acc[h, :, :HEAD_SIZE] / total
        o_ref[0, :, :, h * HEAD_SIZE : (h + 1) * HEAD_SIZE] = out.astype(jnp.bfloat16).reshape(
            2, tok, HEAD_SIZE
        )
        packed = jnp.where(lanes == h, top[h] + jnp.log2(total), packed)
    chosen, levels = 0.0, 0.0
    for k in range(2):
        level = packed[k * tok : (k + 1) * tok]
        l_ref[0, k] = jnp.transpose(level)[:8]
        hot = hot_ref[0, k]
        chosen = chosen + jnp.dot(hot, o_ref[0, k], preferred_element_type=jnp.float32)
        levels = levels + jnp.dot(
            hot.astype(jnp.float32),
            level,
            preferred_element_type=jnp.float32,
            precision=lax.Precision.HIGHEST,
        )
    co_ref[0] = chosen.astype(jnp.bfloat16)
    cl_ref[0] = levels


def flash(sizes, lengths, q, kv, hot):
    xs, _, tok, width = q.shape
    heads = width // HEAD_SIZE
    keys = kv.shape[0] * 4 * tok
    rows = 2 * tok
    picks = hot.shape[2]

    def whole(*shape):
        return pl.BlockSpec((1, *shape), lambda i: (i,) + (0,) * len(shape))

    return pl.pallas_call(
        functools.partial(flash_kernel, sizes, lengths.shape[0]),
        out_shape=(
            jax.ShapeDtypeStruct(q.shape, jnp.bfloat16),
            jax.ShapeDtypeStruct((xs, 2, 8, 128), jnp.float32),
            jax.ShapeDtypeStruct((xs, picks, width), jnp.bfloat16),
            jax.ShapeDtypeStruct((xs, picks, 128), jnp.float32),
        ),
        grid=(xs,),
        in_specs=[
            pl.BlockSpec(memory_space=pltpu.SMEM),
            whole(2, tok, width),
            pl.BlockSpec(memory_space=VMEM),
            whole(2, picks, 128),
        ],
        out_specs=(
            whole(2, tok, width),
            whole(2, 8, 128),
            whole(picks, width),
            whole(picks, 128),
        ),
        scratch_shapes=[
            VMEM((heads, rows, 2 * HEAD_SIZE), jnp.float32),
            VMEM((heads, rows, 128), jnp.float32),
            VMEM((rows, 128), jnp.int32),
            VMEM((rows, 128), jnp.int32),
            pltpu.SMEM((2 * sizes[1] + 2,), jnp.int32),
            pltpu.SMEM((2 * sizes[1] + 2,), jnp.int32),
        ],
        compiler_params=pltpu.CompilerParams(vmem_limit_bytes=32 << 20),
        cost_estimate=pl.CostEstimate(
            flops=4 * heads * xs * rows * keys * HEAD_SIZE // 3,
            bytes_accessed=4 << 20,
            transcendentals=heads * xs * rows * keys // 3,
        ),
        name="flash",
    )(lengths, q, kv, hot)


def shares_of(levels):
    highest = functools.reduce(jnp.maximum, levels)
    parts = [jnp.exp2(level - highest) for level in levels]
    total = functools.reduce(jnp.add, parts)
    return [part / total for part in parts]


def tail_kernel(
    sizes,
    width_full,
    o_ref,
    l_ref,
    co_ref,
    cl_ref,
    res_ref,
    gain_ref,
    ids_ref,
    ow_ref,
    lm_ref,
    att_ref,
    out_ref,
    obuf,
    lbuf,
    cobuf,
    clbuf,
    wbuf,
    lmbuf,
    psend,
    pbuf,
    sqbuf,
    ubuf,
    g_ref,
    logits,
    arrived,
    sbuf,
    fbuf,
    w_sem,
    o_send,
    o_recv,
    l_send,
    l_recv,
    c_send,
    c_recv,
    p_sem,
    s_send,
    s_recv,
    u_sem,
    z_send,
    z_recv,
    x_send,
    x_recv,
    k_send,
    k_recv,
    e_send,
    e_recv,
    m_send,
    m_recv,
    f_send,
    f_recv,
):
    xs, zs = sizes
    x, yh, z, kc = (lax.axis_index(n) for n in CTX)
    hd = lax.axis_index("head")
    ok, oh = (lax.rem(kc + 1, 2), lax.rem(hd + 1, 2))
    row_slot = 2 * yh + kc
    half = width_full // 2
    wide = half // 2
    heads = o_ref.shape[3] // HEAD_SIZE
    z_order = sorted(range(1, zs), key=lambda d: min(d, zs - d))
    x_order = sorted(range(1, xs), key=lambda d: min(d, xs - d))

    weights = []
    for j, side in enumerate((hd, oh)):
        col = pl.multiple_of(side * half + kc * wide, 128)
        weights.append(
            pltpu.make_async_copy(ow_ref.at[:, pl.ds(col, wide)], wbuf.at[j], w_sem.at[j])
        )
        weights[-1].start()
    embedding = pltpu.make_async_copy(lm_ref, lmbuf, w_sem.at[2])
    embedding.start()

    peers = []
    for dx in range(xs):
        for dy in range(2):
            for dk in range(2):
                if dx or dy or dk:
                    peers.append(
                        {
                            "x": lax.rem(x + dx, xs),
                            "yh": lax.rem(yh + dy, 2),
                            "core": lax.rem(kc + dk, 2),
                        }
                    )
    for where in ({}, {"core": ok}):
        peers.append({"head": oh, **where})
    for dz in range(1, zs):
        peers.append({"z": lax.rem(z + dz, zs)})
        peers.append({"z": lax.rem(z + dz, zs), "head": oh})
    greet(peers)

    def c_copies(dx, dy, dk):
        where = {
            "x": lax.rem(x + dx, xs),
            "yh": lax.rem(yh + dy, 2),
            "core": lax.rem(kc + dk, 2),
        }
        at = where["x"]
        own = (x, yh, kc)
        return (
            remote(
                cl_ref.at[at],
                clbuf.at[own],
                c_send.at[0, 4 * dx + 2 * dy + dk],
                c_recv.at[0, 4 * x + row_slot],
                **where,
            ),
            remote(
                co_ref.at[at],
                cobuf.at[own],
                c_send.at[1, 4 * dx + 2 * dy + dk],
                c_recv.at[1, 4 * x + row_slot],
                **where,
            ),
        )

    c_order = [
        (dx, dy, dk)
        for dx in list(reversed(x_order)) + [0]
        for dy in (1, 0)
        for dk in (0, 1)
        if dx or dy or dk
    ]
    for each in c_order:
        for copy in c_copies(*each):
            copy.start()
    pltpu.make_async_copy(
        cl_ref.at[x], clbuf.at[x, yh, kc], c_recv.at[0, 4 * x + row_slot]
    ).start()
    pltpu.make_async_copy(
        co_ref.at[x], cobuf.at[x, yh, kc], c_recv.at[1, 4 * x + row_slot]
    ).start()

    def o_copies(dx, dk):
        tx, tk = (lax.rem(x + dx, xs), lax.rem(kc + dk, 2))
        where = {"x": tx, "core": tk}
        s, mine = (2 * dx + dk, 2 * x + kc)
        return (
            remote(l_ref.at[tx, tk], lbuf.at[x, kc], l_send.at[s], l_recv.at[mine], **where),
            remote(o_ref.at[tx, tk], obuf.at[x, kc], o_send.at[s], o_recv.at[mine], **where),
        )

    o_order = [
        (dx, dk) for dx in list(reversed(x_order)) + [0] for dk in (0, 1) if dx or dk
    ]
    for dx, dk in o_order:
        for copy in o_copies(dx, dk):
            copy.start()
    pltpu.make_async_copy(o_ref.at[x, kc], obuf.at[x, kc], o_recv.at[2 * x + kc]).start()
    pltpu.make_async_copy(l_ref.at[x, kc], lbuf.at[x, kc], l_recv.at[2 * x + kc]).start()

    for s in range(4 * xs):
        at = (s // 4, s // 2 % 2, s % 2)
        for i, buf in enumerate((clbuf, cobuf)):
            part = buf.at[at]
            remote(part, part, c_send.at[i, 0], c_recv.at[i, s], head=oh).wait_recv()
    pieces = []
    for k in range(2):
        shares = shares_of(
            [jnp.concatenate([clbuf[j, 0, k], clbuf[j, 1, k]], axis=0) for j in range(xs)]
        )
        values = [
            jnp.concatenate([cobuf[j, yy, k].astype(jnp.float32) for yy in range(2)], axis=0)
            for j in range(xs)
        ]
        for h in range(heads):
            cols = slice(h * HEAD_SIZE, (h + 1) * HEAD_SIZE)
            merged = sum(shares[j][:, h : h + 1] * values[j][:, cols] for j in range(xs))
            pieces.append(merged.astype(jnp.bfloat16))
    chosen = jnp.concatenate(pieces, axis=1)

    for copy in weights:
        copy.wait()
    psend[...] = jnp.dot(chosen, wbuf[1], preferred_element_type=jnp.float32).astype(jnp.bfloat16)
    p_copy = remote(psend, pbuf, p_sem.at[0], p_sem.at[1], head=oh)
    p_copy.start()
    hidden = jnp.dot(chosen, wbuf[0], preferred_element_type=jnp.float32)
    residual = (res_ref[0] + res_ref[1]) + (res_ref[2] + res_ref[3])
    p_copy.wait_recv()
    hidden = residual.astype(jnp.float32) + (hidden + pbuf[...].astype(jnp.float32))

    own = 2 * hd + kc
    sqbuf[own] = jnp.broadcast_to(jnp.sum(hidden * hidden, axis=1, keepdims=True), (16, 128))

    def s_copy(d):
        return remote(
            sqbuf.at[own],
            sqbuf.at[own],
            s_send.at[d],
            s_recv.at[d],
            head=lax.rem(hd + d // 2, 2),
            core=lax.rem(kc + d % 2, 2),
        )

    for d in range(1, 4):
        s_copy(d).start()
    for d in range(1, 4):
        s_copy(d).wait_recv()
    squares = (sqbuf[0] + sqbuf[1]) + (sqbuf[2] + sqbuf[3])
    scale = lax.rsqrt(squares / width_full + 1e-05)[:, :1]
    ubuf[...] = (hidden * scale * gain_ref[kc]).astype(jnp.bfloat16)
    both = pl.ds(pl.multiple_of(kc * wide, 128), wide)

    def block(bx, bz):
        return g_ref.at[bx, bz, :, both]

    def z_copy(dz):
        to = lax.rem(z + dz, zs)
        return remote(ubuf, block(x, z), z_send.at[dz], z_recv.at[dz], z=to)

    def x_copy(dx, dz):
        bz = lax.rem(z + zs - dz, zs)
        to = lax.rem(x + dx, xs)
        return remote(block(x, bz), block(x, bz), x_send.at[dx, dz], x_recv.at[dx, dz], x=to)

    def relay(dz):
        bz = lax.rem(z + zs - dz, zs)
        step = 1 if 2 * dz < zs - 2 else xs - 1
        part = block(lax.rem(x + xs - step, xs), bz)
        to = lax.rem(x + step, xs)
        return remote(part, part, x_send.at[2, dz], x_recv.at[2, dz], x=to)

    def plane_of(dx):
        return lax.rem(x + xs - dx, xs)

    def k_copy(dx):
        plane = g_ref.at[plane_of(dx), :, :, both]
        return remote(plane, plane, k_send.at[dx], k_recv.at[dx], core=ok)

    def e_copy(dx):
        at = plane_of(dx)
        return remote(
            logits.at[at, oh], arrived.at[at], e_send.at[dx], e_recv.at[dx], head=oh
        )

    def project(dx):
        at = plane_of(dx)
        k_copy(dx).wait_recv()
        rows = g_ref[at].reshape(zs * 16, half)
        out = lax.dot_general(
            rows, lmbuf[...], (((1,), (1,)), ((), ())), preferred_element_type=jnp.float32
        )
        logits[at] = out.astype(jnp.bfloat16).reshape(logits.shape[1:])
        e_copy(dx).start()

    def reduce_plane(dx, packed):
        at = plane_of(dx)
        e_copy(dx).wait_recv()
        both_halves = logits[at, hd].astype(jnp.float32) + arrived[at].astype(jnp.float32)
        rows, width = both_halves.shape
        highest = jnp.max(both_halves, axis=1, keepdims=True)
        total = jnp.sum(jnp.exp(both_halves - highest), axis=1, keepdims=True)
        match = ids_ref[at] == lax.broadcasted_iota(jnp.int32, (rows, width), 1)
        target = jnp.sum(jnp.where(match, both_halves, 0.0), axis=1, keepdims=True)
        lane = lax.broadcasted_iota(jnp.int32, (rows, 128), 1)
        for i, column in enumerate((highest, total, target)):
            packed = jnp.where(lane == at + 8 * i, column, packed)
        return packed

    for dz in reversed(z_order):
        z_copy(dz).start()
    here = pltpu.make_async_copy(ubuf, block(x, z), u_sem)
    here.start()
    here.wait()
    z_seq = [0] + z_order
    sides = [1, xs - 1] if xs > 2 else [1]
    for dz in z_seq:
        if dz:
            z_copy(dz).wait_recv()
        for dx in sides:
            x_copy(dx, dz).start()
    k_copy(0).start()
    for dz in z_seq:
        for dx in sides:
            x_copy(dx, dz).wait_recv()
        if xs > 2:
            relay(dz).start()
    for dx in sides:
        k_copy(dx).start()

    for s in range(2 * xs):
        at = (s // 2, s % 2)
        for buf, send, recv in ((lbuf, l_send, l_recv), (obuf, o_send, o_recv)):
            part = buf.at[at]
            remote(part, part, send.at[0], recv.at[s], head=oh).wait_recv()
    for k in range(2):
        parts = shares_of([lbuf[j, k] for j in range(xs)])
        parts.append(jnp.zeros((128 - 8 * xs, 128), jnp.float32))
        shares = jnp.transpose(jnp.concatenate(parts, axis=0))
        for h in range(heads):
            cols = slice(h * HEAD_SIZE, (h + 1) * HEAD_SIZE)
            merged = sum(
                shares[:, 8 * j + h : 8 * j + h + 1] * obuf[j, k, :, cols].astype(jnp.float32)
                for j in range(xs)
            )
            at = (k * heads + h) * HEAD_SIZE
            att_ref[:, at : at + HEAD_SIZE] = merged.astype(jnp.bfloat16)

    embedding.wait()
    packed = jnp.zeros((zs * 8, 128), jnp.float32)
    project(0)
    last = 0
    for dx in sides:
        project(dx)
        packed = reduce_plane(last, packed)
        last = dx
    if xs > 2:
        for dz in z_seq:
            relay(dz).wait_recv()
        k_copy(2).start()
        packed = reduce_plane(last, packed)
        last = 2
        project(2)
    packed = reduce_plane(last, packed)
    packed = jnp.transpose(packed)
    mine = 4 * x + row_slot
    for i in range(3):
        sbuf[mine, i] = packed[8 * i : 8 * i + 8]

    def merged(parts):
        tops = [part[0] for part in parts]
        top = functools.reduce(jnp.maximum, tops)
        total = functools.reduce(
            jnp.add, [part[1] * jnp.exp(part[0] - top) for part in parts]
        )
        target = functools.reduce(jnp.add, [part[2] for part in parts])
        return (top, total, target)

    def m_copy(dx, dy, dk):
        s = 4 * dx + 2 * dy + dk
        return remote(
            sbuf.at[mine],
            sbuf.at[mine],
            m_send.at[s],
            m_recv.at[s],
            x=lax.rem(x + dx, xs),
            yh=lax.rem(yh + dy, 2),
            core=lax.rem(kc + dk, 2),
        )

    for each in c_order:
        m_copy(*each).start()
    for each in c_order:
        m_copy(*each).wait_recv()
    for i, value in enumerate(merged([sbuf[s] for s in range(4 * xs)])):
        fbuf[hd, z, i] = value

    def f_copy(dh, dz):
        part = fbuf.at[hd, z]
        s = zs * dh + dz
        where = {"head": lax.rem(hd + dh, 2), "z": lax.rem(z + dz, zs)}
        return remote(part, part, f_send.at[s], f_recv.at[s], **where)

    f_order = [(dh, dz) for dz in reversed([0] + z_order) for dh in (0, 1) if dh or dz]
    for each in f_order:
        f_copy(*each).start()
    for each in f_order:
        f_copy(*each).wait_recv()
    for h in range(2):
        top, total, target = merged([fbuf[h, zz] for zz in range(zs)])
        out_ref[h] = target - top - jnp.log(total)

    for each in c_order:
        for copy in c_copies(*each):
            copy.wait_send()
    for dx, dk in o_order:
        for copy in o_copies(dx, dk):
            copy.wait_send()
    p_copy.wait_send()
    for d in range(1, 4):
        s_copy(d).wait_send()
    for dz in z_order:
        z_copy(dz).wait_send()
    for dz in range(zs):
        for dx in sides:
            x_copy(dx, dz).wait_send()
        if xs > 2:
            relay(dz).wait_send()
    for dx in range(xs):
        k_copy(dx).wait_send()
        e_copy(dx).wait_send()
    for each in c_order:
        m_copy(*each).wait_send()
    for each in f_order:
        f_copy(*each).wait_send()


def tail(sizes, o, l, co, cl, res, gain, ids, out_weight, lm_weight):
    xs, zs = sizes
    tok = o.shape[2]
    depth, width_full = out_weight.shape
    vocab, half = lm_weight.shape
    wide = half // 2
    side = zs * 8
    dma = pltpu.SemaphoreType.DMA
    bf16, f32 = (jnp.bfloat16, jnp.float32)
    hbm = pl.BlockSpec(memory_space=pltpu.HBM)
    return pl.pallas_call(
        functools.partial(tail_kernel, sizes, width_full),
        out_shape=(
            jax.ShapeDtypeStruct((tok, depth), bf16),
            jax.ShapeDtypeStruct((2, 8, side), f32),
        ),
        in_specs=[pl.BlockSpec(memory_space=VMEM)] * 7 + [hbm] * 2,
        out_specs=(pl.BlockSpec(memory_space=VMEM),) * 2,
        scratch_shapes=[
            VMEM(o.shape, bf16),
            VMEM(l.shape, f32),
            VMEM((xs, 2, 2, *co.shape[1:]), bf16),
            VMEM((xs, 2, 2, *cl.shape[1:]), f32),
            VMEM((2, depth, wide), bf16),
            VMEM((vocab, half), bf16),
            VMEM((16, wide), bf16),
            VMEM((16, wide), bf16),
            VMEM((4, 16, 128), f32),
            VMEM((16, wide), bf16),
            VMEM((xs, zs, 16, half), bf16),
            VMEM((xs, 2, side, vocab), bf16),
            VMEM((xs, side, vocab), bf16),
            VMEM((4 * xs, 3, 8, side), f32),
            VMEM((2, zs, 3, 8, side), f32),
            dma((3,)),
            dma((2 * xs,)),
            dma((2 * xs,)),
            dma((2 * xs,)),
            dma((2 * xs,)),
            dma((2, 4 * xs)),
            dma((2, 4 * xs)),
            dma((2,)),
            dma((4,)),
            dma((4,)),
            dma,
            dma((zs,)),
            dma((zs,)),
            dma((xs, zs)),
            dma((xs, zs)),
            dma((xs,)),
            dma((xs,)),
            dma((xs,)),
            dma((xs,)),
            dma((4 * xs,)),
            dma((4 * xs,)),
            dma((2 * zs,)),
            dma((2 * zs,)),
        ],
        compiler_params=pltpu.CompilerParams(
            collective_id=1, has_side_effects=True, vmem_limit_bytes=61 << 20
        ),
        name="tail",
    )(o, l, co, cl, res, gain, ids, out_weight, lm_weight)


def per_device(
    sizes,
    queries,
    rotated_keys,
    value_matrix,
    doc_lengths,
    scored,
    residual,
    norm_gain,
    out_weight,
    lm_weight,
    token_ids,
    old_logp,
    advantage,
):
    xs, zs = sizes
    tok = queries.shape[0]
    x, yh, z, kc = (lax.axis_index(n) for n in CTX)
    hd = lax.axis_index("head")
    resp = scored.shape[0]
    half = residual.shape[1]
    mine = (jnp.arange(4, dtype=jnp.int32) == 2 * yh + kc)[:, None]
    near = (jnp.arange(2, dtype=jnp.int32) == kc)[:, None]
    spots = jnp.where(near, scored[None, :], -1).reshape(2 * resp, 1)
    hot = (spots == jnp.arange(tok, dtype=jnp.int32)[None, :]).astype(jnp.bfloat16)
    res = jnp.where(mine[:, :, None], residual[None], 0).astype(jnp.bfloat16)
    res = jnp.transpose(res.reshape(4 * resp, 2, half // 2), (1, 0, 2))
    kvs, qs, hots, res = exchange(sizes, rotated_keys, value_matrix, queries, hot, res)
    o, l, co, cl = flash(sizes, doc_lengths, qs, kvs, hots)

    gain = norm_gain.reshape(2, 1, half // 2)
    vocab = lm_weight.shape[1]
    start = (((x * 2 + yh) * zs + z) * 2 + kc) * vocab
    ids = token_ids.reshape(xs, 2, 2, zs // 2, 2, resp).transpose(2, 0, 3, 1, 4, 5)
    ids = lax.dynamic_index_in_dim(ids.reshape(2, xs, -1, 1), hd, 0, keepdims=False) - start
    attended, found = tail(sizes, o, l, co, cl, res, gain, ids, out_weight, lm_weight.T)
    found = found[:, :xs].reshape(2, xs, zs // 2, 2, 2, resp)
    log_probs = found.transpose(1, 3, 0, 2, 4, 5).reshape(-1)
    ratio = jnp.exp(jnp.clip(log_probs - old_logp, -4.0, 4.0))
    token_loss = -jnp.minimum(ratio * advantage, jnp.clip(ratio, 0.8, 1.2) * advantage)
    return (attended, log_probs, token_loss)


def solution(mesh, shape=(4, 2, 8, 2)):
    finer = Mesh(mesh.devices.reshape(*shape, mesh.shape["head"]), NAMES)
    placed = (
        P(CTX, "head"),
        P(CTX, "head"),
        P(CTX, "head"),
        P(),
        P(CTX),
        P(CTX, "head"),
        P("head"),
        P("head", None),
        P("head", CTX),
        P(),
        P(),
        P(),
    )
    return jax.shard_map(
        functools.partial(per_device, (shape[0], shape[2])),
        mesh=finer,
        in_specs=placed,
        out_specs=(P(CTX, "head"), P(), P()),
        check_vma=False,
    )
```

```python
import functools
import math

import jax
import jax.numpy as jnp
from jax import lax
from jax.experimental import pallas as pl
from jax.experimental.pallas import tpu as pltpu
from jax.sharding import Mesh
from jax.sharding import PartitionSpec as P

HEAD_SIZE = 128
CTX = ("x", "yh", "z", "core")
NAMES = ("x", "yh", "z", "core", "head")
NEG = -1e30
SCALE = HEAD_SIZE**-0.5 * math.log2(math.e)
MESH = pl.DeviceIdType.MESH
VMEM = pltpu.VMEM


def remote(src, dst, send_sem, recv_sem, **where):
    return pltpu.make_async_remote_copy(
        src_ref=src,
        dst_ref=dst,
        send_sem=send_sem,
        recv_sem=recv_sem,
        device_id=where,
        device_id_type=MESH,
    )


def greet(peers):
    barrier = pltpu.get_barrier_semaphore()
    for where in peers:
        pl.semaphore_signal(barrier, inc=1, device_id=where, device_id_type=MESH)
    pl.semaphore_wait(barrier, len(peers))


def exchange_kernel(
    sizes,
    k_ref,
    v_ref,
    q_ref,
    hot_ref,
    res_ref,
    kvbuf,
    qbuf,
    hotbuf,
    resbuf,
    first_send,
    first_recv,
    up_send,
    up_recv,
    down_send,
    down_recv,
    q_send,
    q_recv,
    h_send,
    h_recv,
    r_send,
    r_recv,
    y_sem,
):
    xs, zs = sizes
    x, yh, z, kc = (lax.axis_index(n) for n in CTX)
    up, down = (lax.rem(z + 1, zs), lax.rem(z + zs - 1, zs))
    shift = lax.rem(z, xs)
    tx = lax.rem(x + z, xs)
    mine = 2 * yh + kc
    group = q_ref.shape[1] // 2
    peers = []
    for dx in range(xs):
        for dy in range(2):
            for dk in range(2):
                if dx or dy or dk:
                    peers.append(
                        {
                            "x": lax.rem(x + dx, xs),
                            "yh": lax.rem(yh + dy, 2),
                            "core": lax.rem(kc + dk, 2),
                        }
                    )
    peers.append({"z": up})
    peers.append({"z": down})
    greet(peers)

    def columns(ref, head, width):
        return ref.at[:, pl.ds(pl.multiple_of(head * width, 128), width)]

    def first(dk):
        tk = lax.rem(kc + dk, 2)
        return [
            remote(
                columns(ref, tk, HEAD_SIZE),
                kvbuf.at[z, mine, i],
                first_send.at[dk, i],
                first_recv.at[kc, i],
                x=tx,
                core=tk,
            )
            for i, ref in enumerate((k_ref, v_ref))
        ]

    def first_here():
        return [
            pltpu.make_async_copy(
                columns(ref, kc, HEAD_SIZE), kvbuf.at[z, mine, i], first_recv.at[kc, i]
            )
            for i, ref in enumerate((k_ref, v_ref))
        ]

    for copy in first(1):
        copy.start()

    @pl.when(shift == 0)
    def _():
        for copy in first_here():
            copy.start()

    @pl.when(shift != 0)
    def _():
        for copy in first(0):
            copy.start()

    def q_copies(dx, dk):
        ox, tk = (lax.rem(x + dx, xs), lax.rem(kc + dk, 2))
        s, own = (2 * dx + dk, 2 * x + kc)
        where = {"x": ox, "core": tk}
        q_part = columns(q_ref, tk, group)
        return (
            remote(hot_ref, hotbuf.at[x, kc], h_send.at[s], h_recv.at[own], **where),
            remote(q_part, qbuf.at[x, kc], q_send.at[s], q_recv.at[own], **where),
        )

    pltpu.make_async_copy(
        columns(q_ref, kc, group), qbuf.at[x, kc], q_recv.at[2 * x + kc]
    ).start()
    pltpu.make_async_copy(hot_ref, hotbuf.at[x, kc], h_recv.at[2 * x + kc]).start()
    q_order = [
        (dx, dk)
        for dx in [0] + sorted(range(1, xs), key=lambda d: min(d, xs - d))
        for dk in (0, 1)
        if dx or dk
    ]
    for dx, dk in q_order:
        for copy in q_copies(dx, dk):
            copy.start()

    near = ((0, 1), (1, 0), (1, 1))

    def r_copy(dy, dk):
        ty, tk = (lax.rem(yh + dy, 2), lax.rem(kc + dk, 2))
        return remote(
            res_ref.at[tk],
            resbuf.at[mine],
            r_send.at[2 * dy + dk],
            r_recv.at[mine],
            yh=ty,
            core=tk,
        )

    for dy, dk in near:
        r_copy(dy, dk).start()
    pltpu.make_async_copy(res_ref.at[kc], resbuf.at[mine], r_recv.at[mine]).start()

    def first_wait(k):
        for i in range(2):
            part = kvbuf.at[z, 2 * yh + k, i]
            remote(part, part, first_send.at[0, i], first_recv.at[k, i], z=up).wait_recv()

    def across(side):
        part = kvbuf.at[z, pl.ds(2 * side, 2)]
        return remote(part, part, y_sem.at[0], y_sem.at[1], yh=lax.rem(yh + 1, 2))

    for k in range(2):
        first_wait(k)
    across(yh).start()

    def ring(going_up, slot, t, h):
        send, recv, to = (up_send, up_recv, up) if going_up else (down_send, down_recv, down)
        part = kvbuf.at[slot, pl.ds(2 * lax.rem(yh + h, 2), 2)]
        return remote(part, part, send.at[t, h], recv.at[t, h], z=to)

    def sent(going_up, t, h):
        slot = lax.rem(z - t + zs, zs) if going_up else lax.rem(z + t, zs)
        return ring(going_up, slot, t, h)

    def got(going_up, t, h):
        slot = lax.rem(z - 1 - t + zs, zs) if going_up else lax.rem(z + 1 + t, zs)
        return ring(going_up, slot, t, h)

    full = (zs - 2) // 2
    for t in range(full):
        for h in range(2):
            if t == 0 and h == 1:
                across(1 - yh).wait_recv()
            for going_up in (True, False):
                if t > 0:
                    got(going_up, t - 1, h).wait_recv()
                sent(going_up, t, h).start()
    if full == 0:
        across(1 - yh).wait_recv()
    for going_up, h in ((True, 0), (False, 1)):
        if full > 0:
            got(going_up, full - 1, h).wait_recv()
        sent(going_up, full, h).start()
    if full > 0:
        got(True, full - 1, 1).wait_recv()
        got(False, full - 1, 0).wait_recv()
    got(True, full, 0).wait_recv()
    got(False, full, 1).wait_recv()

    for t in range(full):
        for h in range(2):
            for going_up in (True, False):
                sent(going_up, t, h).wait_send()
    sent(True, full, 0).wait_send()
    sent(False, full, 1).wait_send()
    for copy in first(1):
        copy.wait_send()
    across(yh).wait_send()

    @pl.when(shift != 0)
    def _():
        for copy in first(0):
            copy.wait_send()

    for dy, dk in near:
        r_copy(dy, dk).wait_send()
    for s in range(4):
        part = resbuf.at[s]
        remote(part, part, r_send.at[0], r_recv.at[s], z=up).wait_recv()
    for dx, dk in q_order:
        for copy in q_copies(dx, dk):
            copy.wait_send()
    for s in range(2 * xs):
        part = qbuf.at[s // 2, s % 2]
        remote(part, part, q_send.at[0], q_recv.at[s], z=up).wait_recv()
        part = hotbuf.at[s // 2, s % 2]
        remote(part, part, h_send.at[0], h_recv.at[s], z=up).wait_recv()


def exchange(sizes, k, v, q, hot, res):
    xs, zs = sizes
    tok = q.shape[0]
    full = (zs - 2) // 2
    dma = pltpu.SemaphoreType.DMA
    return pl.pallas_call(
        functools.partial(exchange_kernel, sizes),
        out_shape=(
            jax.ShapeDtypeStruct((zs, 4, 2, tok, HEAD_SIZE), k.dtype),
            jax.ShapeDtypeStruct((xs, 2, tok, q.shape[1] // 2), q.dtype),
            jax.ShapeDtypeStruct((xs, 2, *hot.shape), hot.dtype),
            jax.ShapeDtypeStruct((4, *res.shape[1:]), res.dtype),
        ),
        in_specs=[pl.BlockSpec(memory_space=VMEM)] * 5,
        out_specs=(pl.BlockSpec(memory_space=VMEM),) * 4,
        scratch_shapes=[
            dma((2, 2)),
            dma((2, 2)),
            dma((full + 1, 2)),
            dma((full + 1, 2)),
            dma((full + 1, 2)),
            dma((full + 1, 2)),
            dma((2 * xs,)),
            dma((2 * xs,)),
            dma((2 * xs,)),
            dma((2 * xs,)),
            dma((4,)),
            dma((4,)),
            dma((2,)),
        ],
        compiler_params=pltpu.CompilerParams(
            collective_id=0, has_side_effects=True, vmem_limit_bytes=24 << 20
        ),
        name="exchange",
    )(k, v, q, hot, res)


def flash_kernel(
    sizes,
    docs,
    lengths,
    q_ref,
    kv_ref,
    hot_ref,
    o_ref,
    l_ref,
    co_ref,
    cl_ref,
    acc,
    top,
    causal,
    start,
    order,
    where,
):
    xs, zs = sizes
    chunks = 2 * zs
    xq = pl.program_id(0)
    x, yh, z, _ = (lax.axis_index(n) for n in CTX)
    tok = q_ref.shape[2]
    rows = 2 * tok
    plane = chunks * rows
    heads = q_ref.shape[3] // HEAD_SIZE
    first = xq * plane + (yh * zs + z) * rows
    lanes = lax.broadcasted_iota(jnp.int32, (rows, 128), 1)
    positions = first + lax.broadcasted_iota(jnp.int32, (rows, 128), 0)
    begins = jnp.zeros((rows, 128), jnp.int32)
    low = jnp.int32(0)
    doc_start = jnp.int32(0)
    for d in range(docs):
        begins = jnp.where(positions >= doc_start, doc_start, begins)
        low = jnp.where(first >= doc_start, doc_start, low)
        doc_start = doc_start + lengths[d]
    causal[...] = positions - lanes
    start[...] = begins - lanes
    acc[...] = jnp.zeros_like(acc)
    top[...] = jnp.full_like(top, NEG)

    active = jnp.int32(0)
    for i in range(chunks):
        zz, yy = (i // 2, i % 2)
        base = lax.rem(x + 2 * xs * zs - zz, xs) * plane + (yy * zs + zz) * rows
        order[active] = i
        where[active] = base
        active = active + jnp.where((base < first + rows) & (base + rows > low), 1, 0)

    def step(pair, carry):
        one = order[2 * pair]
        whole = 2 * pair + 1 < active
        two = jnp.where(whole, order[2 * pair + 1], one)
        bases = (where[2 * pair], jnp.where(whole, where[2 * pair + 1], 1 << 28))
        keys, values, biases = [], [], []
        for chunk, base in zip((one, two), bases):
            zz, yy = (chunk // 2, lax.rem(chunk, 2))
            for k in range(2):
                keys.append(kv_ref[zz, 2 * yy + k, 0])
                values.append(kv_ref[zz, 2 * yy + k, 1])
                at = base + k * tok
                ok = (causal[...] >= at) & (start[...] <= at)
                biases.append(jnp.where(ok, 0.0, NEG))
        key = jnp.concatenate(keys, axis=0)
        value = jnp.concatenate(values, axis=0)
        value = jnp.concatenate([value, jnp.ones_like(value)], axis=1)
        bias = jnp.concatenate(biases, axis=1)
        for h in range(heads):
            cols = slice(h * HEAD_SIZE, (h + 1) * HEAD_SIZE)
            q = q_ref[0, :, :, cols].reshape(rows, HEAD_SIZE)
            s = lax.dot_general(
                q, key, (((1,), (1,)), ((), ())), preferred_element_type=jnp.float32
            )
            s = s * SCALE + bias
            old = top[h]
            new = jnp.maximum(old, jnp.max(s, axis=1, keepdims=True))
            w = jnp.exp2(s - new[:, :1]).astype(jnp.bfloat16)
            update = jnp.dot(w, value, preferred_element_type=jnp.float32)
            shrink = jnp.exp2(old - new)
            top[h] = new
            acc[h] = acc[h] * jnp.concatenate([shrink, shrink], axis=1) + update
        return carry

    lax.fori_loop(0, (active + 1) // 2, step, 0)

    packed = jnp.zeros((rows, 128), jnp.float32)
    for h in range(heads):
        total = jnp.maximum(acc[h, :, HEAD_SIZE:], 1e-30)
        out = acc[h, :, :HEAD_SIZE] / total
        o_ref[0, :, :, h * HEAD_SIZE : (h + 1) * HEAD_SIZE] = out.astype(jnp.bfloat16).reshape(
            2, tok, HEAD_SIZE
        )
        packed = jnp.where(lanes == h, top[h] + jnp.log2(total), packed)
    chosen, levels = 0.0, 0.0
    for k in range(2):
        level = packed[k * tok : (k + 1) * tok]
        l_ref[0, k] = jnp.transpose(level)[:8]
        hot = hot_ref[0, k]
        chosen = chosen + jnp.dot(hot, o_ref[0, k], preferred_element_type=jnp.float32)
        levels = levels + jnp.dot(
            hot.astype(jnp.float32),
            level,
            preferred_element_type=jnp.float32,
            precision=lax.Precision.HIGHEST,
        )
    co_ref[0] = chosen.astype(jnp.bfloat16)
    cl_ref[0] = levels


def flash(sizes, lengths, q, kv, hot):
    xs, _, tok, width = q.shape
    heads = width // HEAD_SIZE
    keys = kv.shape[0] * 4 * tok
    rows = 2 * tok
    picks = hot.shape[2]

    def whole(*shape):
        return pl.BlockSpec((1, *shape), lambda i: (i,) + (0,) * len(shape))

    return pl.pallas_call(
        functools.partial(flash_kernel, sizes, lengths.shape[0]),
        out_shape=(
            jax.ShapeDtypeStruct(q.shape, jnp.bfloat16),
            jax.ShapeDtypeStruct((xs, 2, 8, 128), jnp.float32),
            jax.ShapeDtypeStruct((xs, picks, width), jnp.bfloat16),
            jax.ShapeDtypeStruct((xs, picks, 128), jnp.float32),
        ),
        grid=(xs,),
        in_specs=[
            pl.BlockSpec(memory_space=pltpu.SMEM),
            whole(2, tok, width),
            pl.BlockSpec(memory_space=VMEM),
            whole(2, picks, 128),
        ],
        out_specs=(
            whole(2, tok, width),
            whole(2, 8, 128),
            whole(picks, width),
            whole(picks, 128),
        ),
        scratch_shapes=[
            VMEM((heads, rows, 2 * HEAD_SIZE), jnp.float32),
            VMEM((heads, rows, 128), jnp.float32),
            VMEM((rows, 128), jnp.int32),
            VMEM((rows, 128), jnp.int32),
            pltpu.SMEM((2 * sizes[1] + 2,), jnp.int32),
            pltpu.SMEM((2 * sizes[1] + 2,), jnp.int32),
        ],
        compiler_params=pltpu.CompilerParams(vmem_limit_bytes=32 << 20),
        cost_estimate=pl.CostEstimate(
            flops=4 * heads * xs * rows * keys * HEAD_SIZE // 3,
            bytes_accessed=4 << 20,
            transcendentals=heads * xs * rows * keys // 3,
        ),
        name="flash",
    )(lengths, q, kv, hot)


def shares_of(levels):
    highest = functools.reduce(jnp.maximum, levels)
    parts = [jnp.exp2(level - highest) for level in levels]
    total = functools.reduce(jnp.add, parts)
    return [part / total for part in parts]


def tail_kernel(
    sizes,
    width_full,
    o_ref,
    l_ref,
    co_ref,
    cl_ref,
    res_ref,
    gain_ref,
    ids_ref,
    ow_ref,
    lm_ref,
    att_ref,
    out_ref,
    obuf,
    lbuf,
    cobuf,
    clbuf,
    wbuf,
    lmbuf,
    psend,
    pbuf,
    sqbuf,
    ubuf,
    g_ref,
    logits,
    arrived,
    sbuf,
    fbuf,
    w_sem,
    o_send,
    o_recv,
    l_send,
    l_recv,
    c_send,
    c_recv,
    p_sem,
    s_send,
    s_recv,
    u_sem,
    z_send,
    z_recv,
    x_send,
    x_recv,
    k_send,
    k_recv,
    e_send,
    e_recv,
    m_send,
    m_recv,
    f_send,
    f_recv,
):
    xs, zs = sizes
    x, yh, z, kc = (lax.axis_index(n) for n in CTX)
    hd = lax.axis_index("head")
    ok, oh = (lax.rem(kc + 1, 2), lax.rem(hd + 1, 2))
    row_slot = 2 * yh + kc
    half = width_full // 2
    wide = half // 2
    heads = o_ref.shape[3] // HEAD_SIZE
    z_order = sorted(range(1, zs), key=lambda d: min(d, zs - d))
    x_order = sorted(range(1, xs), key=lambda d: min(d, xs - d))

    weights = []
    for j, side in enumerate((hd, oh)):
        col = pl.multiple_of(side * half + kc * wide, 128)
        weights.append(
            pltpu.make_async_copy(ow_ref.at[:, pl.ds(col, wide)], wbuf.at[j], w_sem.at[j])
        )
        weights[-1].start()
    embedding = pltpu.make_async_copy(lm_ref, lmbuf, w_sem.at[2])
    embedding.start()

    peers = []
    for dx in range(xs):
        for dy in range(2):
            for dk in range(2):
                if dx or dy or dk:
                    peers.append(
                        {
                            "x": lax.rem(x + dx, xs),
                            "yh": lax.rem(yh + dy, 2),
                            "core": lax.rem(kc + dk, 2),
                        }
                    )
    for where in ({}, {"core": ok}):
        peers.append({"head": oh, **where})
    for dz in range(1, zs):
        peers.append({"z": lax.rem(z + dz, zs)})
        peers.append({"z": lax.rem(z + dz, zs), "head": oh})
    greet(peers)

    def c_copies(dx, dy, dk):
        where = {
            "x": lax.rem(x + dx, xs),
            "yh": lax.rem(yh + dy, 2),
            "core": lax.rem(kc + dk, 2),
        }
        at = where["x"]
        own = (x, yh, kc)
        return (
            remote(
                cl_ref.at[at],
                clbuf.at[own],
                c_send.at[0, 4 * dx + 2 * dy + dk],
                c_recv.at[0, 4 * x + row_slot],
                **where,
            ),
            remote(
                co_ref.at[at],
                cobuf.at[own],
                c_send.at[1, 4 * dx + 2 * dy + dk],
                c_recv.at[1, 4 * x + row_slot],
                **where,
            ),
        )

    c_order = [
        (dx, dy, dk)
        for dx in list(reversed(x_order)) + [0]
        for dy in (1, 0)
        for dk in (0, 1)
        if dx or dy or dk
    ]
    for each in c_order:
        for copy in c_copies(*each):
            copy.start()
    pltpu.make_async_copy(
        cl_ref.at[x], clbuf.at[x, yh, kc], c_recv.at[0, 4 * x + row_slot]
    ).start()
    pltpu.make_async_copy(
        co_ref.at[x], cobuf.at[x, yh, kc], c_recv.at[1, 4 * x + row_slot]
    ).start()

    def o_copies(dx, dk):
        tx, tk = (lax.rem(x + dx, xs), lax.rem(kc + dk, 2))
        where = {"x": tx, "core": tk}
        s, mine = (2 * dx + dk, 2 * x + kc)
        return (
            remote(l_ref.at[tx, tk], lbuf.at[x, kc], l_send.at[s], l_recv.at[mine], **where),
            remote(o_ref.at[tx, tk], obuf.at[x, kc], o_send.at[s], o_recv.at[mine], **where),
        )

    o_order = [
        (dx, dk) for dx in list(reversed(x_order)) + [0] for dk in (0, 1) if dx or dk
    ]
    for dx, dk in o_order:
        for copy in o_copies(dx, dk):
            copy.start()
    pltpu.make_async_copy(o_ref.at[x, kc], obuf.at[x, kc], o_recv.at[2 * x + kc]).start()
    pltpu.make_async_copy(l_ref.at[x, kc], lbuf.at[x, kc], l_recv.at[2 * x + kc]).start()

    for s in range(4 * xs):
        at = (s // 4, s // 2 % 2, s % 2)
        for i, buf in enumerate((clbuf, cobuf)):
            part = buf.at[at]
            remote(part, part, c_send.at[i, 0], c_recv.at[i, s], head=oh).wait_recv()
    pieces = []
    for k in range(2):
        shares = shares_of(
            [jnp.concatenate([clbuf[j, 0, k], clbuf[j, 1, k]], axis=0) for j in range(xs)]
        )
        values = [
            jnp.concatenate([cobuf[j, yy, k].astype(jnp.float32) for yy in range(2)], axis=0)
            for j in range(xs)
        ]
        for h in range(heads):
            cols = slice(h * HEAD_SIZE, (h + 1) * HEAD_SIZE)
            merged = sum(shares[j][:, h : h + 1] * values[j][:, cols] for j in range(xs))
            pieces.append(merged.astype(jnp.bfloat16))
    chosen = jnp.concatenate(pieces, axis=1)

    for copy in weights:
        copy.wait()
    psend[...] = jnp.dot(chosen, wbuf[1], preferred_element_type=jnp.float32).astype(jnp.bfloat16)
    p_copy = remote(psend, pbuf, p_sem.at[0], p_sem.at[1], head=oh)
    p_copy.start()
    hidden = jnp.dot(chosen, wbuf[0], preferred_element_type=jnp.float32)
    residual = (res_ref[0] + res_ref[1]) + (res_ref[2] + res_ref[3])
    p_copy.wait_recv()
    hidden = residual.astype(jnp.float32) + (hidden + pbuf[...].astype(jnp.float32))

    own = 2 * hd + kc
    sqbuf[own] = jnp.broadcast_to(jnp.sum(hidden * hidden, axis=1, keepdims=True), (16, 128))

    def s_copy(d):
        return remote(
            sqbuf.at[own],
            sqbuf.at[own],
            s_send.at[d],
            s_recv.at[d],
            head=lax.rem(hd + d // 2, 2),
            core=lax.rem(kc + d % 2, 2),
        )

    for d in range(1, 4):
        s_copy(d).start()
    for d in range(1, 4):
        s_copy(d).wait_recv()
    squares = (sqbuf[0] + sqbuf[1]) + (sqbuf[2] + sqbuf[3])
    scale = lax.rsqrt(squares / width_full + 1e-05)[:, :1]
    ubuf[...] = (hidden * scale * gain_ref[kc]).astype(jnp.bfloat16)
    both = pl.ds(pl.multiple_of(kc * wide, 128), wide)

    def block(bx, bz):
        return g_ref.at[bx, bz, :, both]

    def z_copy(dz):
        to = lax.rem(z + dz, zs)
        return remote(ubuf, block(x, z), z_send.at[dz], z_recv.at[dz], z=to)

    def x_copy(dx, dz):
        bz = lax.rem(z + zs - dz, zs)
        to = lax.rem(x + dx, xs)
        return remote(block(x, bz), block(x, bz), x_send.at[dx, dz], x_recv.at[dx, dz], x=to)

    def relay(dz):
        bz = lax.rem(z + zs - dz, zs)
        step = 1 if 2 * dz < zs - 2 else xs - 1
        part = block(lax.rem(x + xs - step, xs), bz)
        to = lax.rem(x + step, xs)
        return remote(part, part, x_send.at[2, dz], x_recv.at[2, dz], x=to)

    def plane_of(dx):
        return lax.rem(x + xs - dx, xs)

    def k_copy(dx):
        plane = g_ref.at[plane_of(dx), :, :, both]
        return remote(plane, plane, k_send.at[dx], k_recv.at[dx], core=ok)

    def e_copy(dx):
        at = plane_of(dx)
        return remote(
            logits.at[at, oh], arrived.at[at], e_send.at[dx], e_recv.at[dx], head=oh
        )

    def project(dx):
        at = plane_of(dx)
        k_copy(dx).wait_recv()
        rows = g_ref[at].reshape(zs * 16, half)
        out = lax.dot_general(
            rows, lmbuf[...], (((1,), (1,)), ((), ())), preferred_element_type=jnp.float32
        )
        logits[at] = out.astype(jnp.bfloat16).reshape(logits.shape[1:])
        e_copy(dx).start()

    def reduce_plane(dx, packed):
        at = plane_of(dx)
        e_copy(dx).wait_recv()
        both_halves = logits[at, hd].astype(jnp.float32) + arrived[at].astype(jnp.float32)
        rows, width = both_halves.shape
        highest = jnp.max(both_halves, axis=1, keepdims=True)
        total = jnp.sum(jnp.exp(both_halves - highest), axis=1, keepdims=True)
        match = ids_ref[at] == lax.broadcasted_iota(jnp.int32, (rows, width), 1)
        target = jnp.sum(jnp.where(match, both_halves, 0.0), axis=1, keepdims=True)
        lane = lax.broadcasted_iota(jnp.int32, packed.shape, 1)
        row = lax.broadcasted_iota(jnp.int32, packed.shape, 0)
        low = lax.rem(at, 2) * rows
        here = (row >= low) & (row < low + rows)
        for i, column in enumerate((highest, total, target)):
            column = jnp.concatenate([column, column], axis=0)
            packed = jnp.where(here & (lane == at // 2 + 2 * i), column, packed)
        return packed

    for dz in reversed(z_order):
        z_copy(dz).start()
    here = pltpu.make_async_copy(ubuf, block(x, z), u_sem)
    here.start()
    here.wait()
    z_seq = [0] + z_order
    sides = [1, xs - 1] if xs > 2 else [1]
    for dz in z_seq:
        if dz:
            z_copy(dz).wait_recv()
        for dx in sides:
            x_copy(dx, dz).start()
    k_copy(0).start()
    embedding.wait()
    project(0)
    for dz in z_seq:
        for dx in sides:
            x_copy(dx, dz).wait_recv()
        if xs > 2:
            relay(dz).start()
    for dx in sides:
        k_copy(dx).start()
    for dx in sides:
        project(dx)

    for s in range(2 * xs):
        at = (s // 2, s % 2)
        for buf, send, recv in ((lbuf, l_send, l_recv), (obuf, o_send, o_recv)):
            part = buf.at[at]
            remote(part, part, send.at[0], recv.at[s], head=oh).wait_recv()
    for k in range(2):
        parts = shares_of([lbuf[j, k] for j in range(xs)])
        parts.append(jnp.zeros((128 - 8 * xs, 128), jnp.float32))
        shares = jnp.transpose(jnp.concatenate(parts, axis=0))
        for h in range(heads):
            cols = slice(h * HEAD_SIZE, (h + 1) * HEAD_SIZE)
            merged = sum(
                shares[:, 8 * j + h : 8 * j + h + 1] * obuf[j, k, :, cols].astype(jnp.float32)
                for j in range(xs)
            )
            at = (k * heads + h) * HEAD_SIZE
            att_ref[:, at : at + HEAD_SIZE] = merged.astype(jnp.bfloat16)

    packed = jnp.zeros((zs * 16, 128), jnp.float32)
    packed = reduce_plane(0, packed)
    if xs > 2:
        for dz in z_seq:
            relay(dz).wait_recv()
        k_copy(2).start()
        packed = reduce_plane(1, packed)
        project(2)
        packed = reduce_plane(xs - 1, packed)
        packed = reduce_plane(2, packed)
    else:
        packed = reduce_plane(1, packed)
    mine = 4 * x + row_slot
    sbuf[mine] = jnp.transpose(packed)[:8]

    def merged(parts):
        tops = [part[0:2] for part in parts]
        top = functools.reduce(jnp.maximum, tops)
        total = functools.reduce(
            jnp.add, [part[2:4] * jnp.exp(part[0:2] - top) for part in parts]
        )
        target = functools.reduce(jnp.add, [part[4:6] for part in parts])
        return (top, total, target)

    def m_copy(dx, dy, dk):
        s = 4 * dx + 2 * dy + dk
        return remote(
            sbuf.at[mine],
            sbuf.at[mine],
            m_send.at[s],
            m_recv.at[s],
            x=lax.rem(x + dx, xs),
            yh=lax.rem(yh + dy, 2),
            core=lax.rem(kc + dk, 2),
        )

    for each in c_order:
        m_copy(*each).start()
    for each in c_order:
        m_copy(*each).wait_recv()
    top, total, target = merged([sbuf[s] for s in range(4 * xs)])
    fbuf[hd, z] = jnp.concatenate([top, total, target, target], axis=0)

    def f_copy(dh, dz):
        part = fbuf.at[hd, z]
        s = zs * dh + dz
        where = {"head": lax.rem(hd + dh, 2), "z": lax.rem(z + dz, zs)}
        return remote(part, part, f_send.at[s], f_recv.at[s], **where)

    f_order = [(dh, dz) for dz in reversed([0] + z_order) for dh in (0, 1) if dh or dz]
    for each in f_order:
        f_copy(*each).start()
    for each in f_order:
        f_copy(*each).wait_recv()
    for h in range(2):
        top, total, target = merged([fbuf[h, zz] for zz in range(zs)])
        found = target - top - jnp.log(total)
        out_ref[h] = jnp.concatenate([found] * 4, axis=0)

    for each in c_order:
        for copy in c_copies(*each):
            copy.wait_send()
    for dx, dk in o_order:
        for copy in o_copies(dx, dk):
            copy.wait_send()
    p_copy.wait_send()
    for d in range(1, 4):
        s_copy(d).wait_send()
    for dz in z_order:
        z_copy(dz).wait_send()
    for dz in range(zs):
        for dx in sides:
            x_copy(dx, dz).wait_send()
        if xs > 2:
            relay(dz).wait_send()
    for dx in range(xs):
        k_copy(dx).wait_send()
        e_copy(dx).wait_send()
    for each in c_order:
        m_copy(*each).wait_send()
    for each in f_order:
        f_copy(*each).wait_send()


def tail(sizes, o, l, co, cl, res, gain, ids, out_weight, lm_weight):
    xs, zs = sizes
    tok = o.shape[2]
    depth, width_full = out_weight.shape
    vocab, half = lm_weight.shape
    wide = half // 2
    side = zs * 8
    dma = pltpu.SemaphoreType.DMA
    bf16, f32 = (jnp.bfloat16, jnp.float32)
    hbm = pl.BlockSpec(memory_space=pltpu.HBM)
    return pl.pallas_call(
        functools.partial(tail_kernel, sizes, width_full),
        out_shape=(
            jax.ShapeDtypeStruct((tok, depth), bf16),
            jax.ShapeDtypeStruct((2, 8, 2 * side), f32),
        ),
        in_specs=[pl.BlockSpec(memory_space=VMEM)] * 7 + [hbm] * 2,
        out_specs=(pl.BlockSpec(memory_space=VMEM),) * 2,
        scratch_shapes=[
            VMEM(o.shape, bf16),
            VMEM(l.shape, f32),
            VMEM((xs, 2, 2, *co.shape[1:]), bf16),
            VMEM((xs, 2, 2, *cl.shape[1:]), f32),
            VMEM((2, depth, wide), bf16),
            VMEM((vocab, half), bf16),
            VMEM((16, wide), bf16),
            VMEM((16, wide), bf16),
            VMEM((4, 16, 128), f32),
            VMEM((16, wide), bf16),
            VMEM((xs, zs, 16, half), bf16),
            VMEM((xs, 2, side, vocab), bf16),
            VMEM((xs, side, vocab), bf16),
            VMEM((4 * xs, 8, 2 * side), f32),
            VMEM((2, zs, 8, 2 * side), f32),
            dma((3,)),
            dma((2 * xs,)),
            dma((2 * xs,)),
            dma((2 * xs,)),
            dma((2 * xs,)),
            dma((2, 4 * xs)),
            dma((2, 4 * xs)),
            dma((2,)),
            dma((4,)),
            dma((4,)),
            dma,
            dma((zs,)),
            dma((zs,)),
            dma((xs, zs)),
            dma((xs, zs)),
            dma((xs,)),
            dma((xs,)),
            dma((xs,)),
            dma((xs,)),
            dma((4 * xs,)),
            dma((4 * xs,)),
            dma((2 * zs,)),
            dma((2 * zs,)),
        ],
        compiler_params=pltpu.CompilerParams(
            collective_id=1, has_side_effects=True, vmem_limit_bytes=50 << 20
        ),
        name="tail",
    )(o, l, co, cl, res, gain, ids, out_weight, lm_weight)


def per_device(
    sizes,
    queries,
    rotated_keys,
    value_matrix,
    doc_lengths,
    scored,
    residual,
    norm_gain,
    out_weight,
    lm_weight,
    token_ids,
    old_logp,
    advantage,
):
    xs, zs = sizes
    tok = queries.shape[0]
    x, yh, z, kc = (lax.axis_index(n) for n in CTX)
    hd = lax.axis_index("head")
    resp = scored.shape[0]
    half = residual.shape[1]
    mine = (jnp.arange(4, dtype=jnp.int32) == 2 * yh + kc)[:, None]
    near = (jnp.arange(2, dtype=jnp.int32) == kc)[:, None]
    spots = jnp.where(near, scored[None, :], -1).reshape(2 * resp, 1)
    hot = (spots == jnp.arange(tok, dtype=jnp.int32)[None, :]).astype(jnp.bfloat16)
    res = jnp.where(mine[:, :, None], residual[None], 0).astype(jnp.bfloat16)
    res = jnp.transpose(res.reshape(4 * resp, 2, half // 2), (1, 0, 2))
    kvs, qs, hots, res = exchange(sizes, rotated_keys, value_matrix, queries, hot, res)
    o, l, co, cl = flash(sizes, doc_lengths, qs, kvs, hots)

    gain = norm_gain.reshape(2, 1, half // 2)
    vocab = lm_weight.shape[1]
    start = (((x * 2 + yh) * zs + z) * 2 + kc) * vocab
    ids = token_ids.reshape(xs, 2, 2, zs // 2, 2, resp).transpose(2, 0, 3, 1, 4, 5)
    ids = lax.dynamic_index_in_dim(ids.reshape(2, xs, -1, 1), hd, 0, keepdims=False) - start
    attended, found = tail(sizes, o, l, co, cl, res, gain, ids, out_weight, lm_weight.T)
    found = found[:, : xs // 2].reshape(2, xs, zs // 2, 2, 2, resp)
    log_probs = found.transpose(1, 3, 0, 2, 4, 5).reshape(-1)
    ratio = jnp.exp(jnp.clip(log_probs - old_logp, -4.0, 4.0))
    token_loss = -jnp.minimum(ratio * advantage, jnp.clip(ratio, 0.8, 1.2) * advantage)
    return (attended, log_probs, token_loss)


def solution(mesh, shape=(4, 2, 8, 2)):
    finer = Mesh(mesh.devices.reshape(*shape, mesh.shape["head"]), NAMES)
    placed = (
        P(CTX, "head"),
        P(CTX, "head"),
        P(CTX, "head"),
        P(),
        P(CTX),
        P(CTX, "head"),
        P("head"),
        P("head", None),
        P("head", CTX),
        P(),
        P(),
        P(),
    )
    return jax.shard_map(
        functools.partial(per_device, (shape[0], shape[2])),
        mesh=finer,
        in_specs=placed,
        out_specs=(P(CTX, "head"), P(), P()),
        check_vma=False,
    )
```

```python
import functools
import math

import jax
import jax.numpy as jnp
from jax import lax
from jax.experimental import pallas as pl
from jax.experimental.pallas import tpu as pltpu
from jax.sharding import Mesh
from jax.sharding import PartitionSpec as P

HEAD_SIZE = 128
CTX = ("x", "yh", "z", "core")
NAMES = ("x", "yh", "z", "core", "head")
NEG = -1e30
SCALE = HEAD_SIZE**-0.5 * math.log2(math.e)
MESH = pl.DeviceIdType.MESH
VMEM = pltpu.VMEM


def remote(src, dst, send_sem, recv_sem, **where):
    return pltpu.make_async_remote_copy(
        src_ref=src,
        dst_ref=dst,
        send_sem=send_sem,
        recv_sem=recv_sem,
        device_id=where,
        device_id_type=MESH,
    )


def greet(peers):
    barrier = pltpu.get_barrier_semaphore()
    for where in peers:
        pl.semaphore_signal(barrier, inc=1, device_id=where, device_id_type=MESH)
    pl.semaphore_wait(barrier, len(peers))


def exchange_kernel(
    sizes,
    k_ref,
    v_ref,
    q_ref,
    scored_ref,
    own_ref,
    kvbuf,
    qbuf,
    hotbuf,
    resbuf,
    hot_ref,
    res_ref,
    first_send,
    first_recv,
    up_send,
    up_recv,
    down_send,
    down_recv,
    q_send,
    q_recv,
    h_send,
    h_recv,
    r_send,
    r_recv,
    y_sem,
):
    xs, zs = sizes
    x, yh, z, kc = (lax.axis_index(n) for n in CTX)
    up, down = (lax.rem(z + 1, zs), lax.rem(z + zs - 1, zs))
    shift = lax.rem(z, xs)
    tx = lax.rem(x + z, xs)
    mine = 2 * yh + kc
    group = q_ref.shape[1] // 2
    peers = []
    for dx in range(xs):
        for dy in range(2):
            for dk in range(2):
                if dx or dy or dk:
                    peers.append(
                        {
                            "x": lax.rem(x + dx, xs),
                            "yh": lax.rem(yh + dy, 2),
                            "core": lax.rem(kc + dk, 2),
                        }
                    )
    peers.append({"z": up})
    peers.append({"z": down})
    picks = scored_ref.shape[0]
    row = lax.broadcasted_iota(jnp.int32, hot_ref.shape, 0)
    lane = lax.broadcasted_iota(jnp.int32, hot_ref.shape, 1)
    hot = jnp.zeros(hot_ref.shape, jnp.float32)
    for i in range(picks):
        hot = jnp.where((row == picks * kc + i) & (lane == scored_ref[i]), 1.0, hot)
    hot_ref[...] = hot.astype(jnp.bfloat16)
    wide = res_ref.shape[2]
    row = lax.broadcasted_iota(jnp.int32, res_ref.shape[1:], 0)
    for side in range(2):
        own = own_ref[:, side * wide : (side + 1) * wide].astype(jnp.float32)
        placed = jnp.zeros(res_ref.shape[1:], jnp.float32)
        for i in range(picks):
            placed = jnp.where(row == picks * mine + i, own[i : i + 1], placed)
        res_ref[side] = placed.astype(jnp.bfloat16)
    greet(peers)

    def columns(ref, head, width):
        return ref.at[:, pl.ds(pl.multiple_of(head * width, 128), width)]

    def first(dk):
        tk = lax.rem(kc + dk, 2)
        return [
            remote(
                columns(ref, tk, HEAD_SIZE),
                kvbuf.at[z, mine, i],
                first_send.at[dk, i],
                first_recv.at[kc, i],
                x=tx,
                core=tk,
            )
            for i, ref in enumerate((k_ref, v_ref))
        ]

    def first_here():
        return [
            pltpu.make_async_copy(
                columns(ref, kc, HEAD_SIZE), kvbuf.at[z, mine, i], first_recv.at[kc, i]
            )
            for i, ref in enumerate((k_ref, v_ref))
        ]

    for copy in first(1):
        copy.start()

    @pl.when(shift == 0)
    def _():
        for copy in first_here():
            copy.start()

    @pl.when(shift != 0)
    def _():
        for copy in first(0):
            copy.start()

    def q_copies(dx, dk):
        ox, tk = (lax.rem(x + dx, xs), lax.rem(kc + dk, 2))
        s, own = (2 * dx + dk, 2 * x + kc)
        where = {"x": ox, "core": tk}
        q_part = columns(q_ref, tk, group)
        return (
            remote(hot_ref, hotbuf.at[x, kc], h_send.at[s], h_recv.at[own], **where),
            remote(q_part, qbuf.at[x, kc], q_send.at[s], q_recv.at[own], **where),
        )

    pltpu.make_async_copy(
        columns(q_ref, kc, group), qbuf.at[x, kc], q_recv.at[2 * x + kc]
    ).start()
    pltpu.make_async_copy(hot_ref, hotbuf.at[x, kc], h_recv.at[2 * x + kc]).start()
    q_order = [
        (dx, dk)
        for dx in [0] + sorted(range(1, xs), key=lambda d: min(d, xs - d))
        for dk in (0, 1)
        if dx or dk
    ]
    for dx, dk in q_order:
        for copy in q_copies(dx, dk):
            copy.start()

    near = ((0, 1), (1, 0), (1, 1))

    def r_copy(dy, dk):
        ty, tk = (lax.rem(yh + dy, 2), lax.rem(kc + dk, 2))
        return remote(
            res_ref.at[tk],
            resbuf.at[mine],
            r_send.at[2 * dy + dk],
            r_recv.at[mine],
            yh=ty,
            core=tk,
        )

    for dy, dk in near:
        r_copy(dy, dk).start()
    pltpu.make_async_copy(res_ref.at[kc], resbuf.at[mine], r_recv.at[mine]).start()

    def first_wait(k):
        for i in range(2):
            part = kvbuf.at[z, 2 * yh + k, i]
            remote(part, part, first_send.at[0, i], first_recv.at[k, i], z=up).wait_recv()

    def across(side):
        part = kvbuf.at[z, pl.ds(2 * side, 2)]
        return remote(part, part, y_sem.at[0], y_sem.at[1], yh=lax.rem(yh + 1, 2))

    for k in range(2):
        first_wait(k)
    across(yh).start()

    def ring(going_up, slot, t, h):
        send, recv, to = (up_send, up_recv, up) if going_up else (down_send, down_recv, down)
        part = kvbuf.at[slot, pl.ds(2 * lax.rem(yh + h, 2), 2)]
        return remote(part, part, send.at[t, h], recv.at[t, h], z=to)

    def sent(going_up, t, h):
        slot = lax.rem(z - t + zs, zs) if going_up else lax.rem(z + t, zs)
        return ring(going_up, slot, t, h)

    def got(going_up, t, h):
        slot = lax.rem(z - 1 - t + zs, zs) if going_up else lax.rem(z + 1 + t, zs)
        return ring(going_up, slot, t, h)

    full = (zs - 2) // 2
    for t in range(full):
        for h in range(2):
            if t == 0 and h == 1:
                across(1 - yh).wait_recv()
            for going_up in (True, False):
                if t > 0:
                    got(going_up, t - 1, h).wait_recv()
                sent(going_up, t, h).start()
    if full == 0:
        across(1 - yh).wait_recv()
    for going_up, h in ((True, 0), (False, 1)):
        if full > 0:
            got(going_up, full - 1, h).wait_recv()
        sent(going_up, full, h).start()
    if full > 0:
        got(True, full - 1, 1).wait_recv()
        got(False, full - 1, 0).wait_recv()
    got(True, full, 0).wait_recv()
    got(False, full, 1).wait_recv()

    for t in range(full):
        for h in range(2):
            for going_up in (True, False):
                sent(going_up, t, h).wait_send()
    sent(True, full, 0).wait_send()
    sent(False, full, 1).wait_send()
    for copy in first(1):
        copy.wait_send()
    across(yh).wait_send()

    @pl.when(shift != 0)
    def _():
        for copy in first(0):
            copy.wait_send()

    for dy, dk in near:
        r_copy(dy, dk).wait_send()
    for s in range(4):
        part = resbuf.at[s]
        remote(part, part, r_send.at[0], r_recv.at[s], z=up).wait_recv()
    for dx, dk in q_order:
        for copy in q_copies(dx, dk):
            copy.wait_send()
    for s in range(2 * xs):
        part = qbuf.at[s // 2, s % 2]
        remote(part, part, q_send.at[0], q_recv.at[s], z=up).wait_recv()
        part = hotbuf.at[s // 2, s % 2]
        remote(part, part, h_send.at[0], h_recv.at[s], z=up).wait_recv()


def exchange(sizes, k, v, q, scored, residual):
    xs, zs = sizes
    tok = q.shape[0]
    picks, half = residual.shape
    hot, res = ((2 * picks, tok), (4 * picks, half // 2))
    full = (zs - 2) // 2
    dma = pltpu.SemaphoreType.DMA
    return pl.pallas_call(
        functools.partial(exchange_kernel, sizes),
        out_shape=(
            jax.ShapeDtypeStruct((zs, 4, 2, tok, HEAD_SIZE), k.dtype),
            jax.ShapeDtypeStruct((xs, 2, tok, q.shape[1] // 2), q.dtype),
            jax.ShapeDtypeStruct((xs, 2, *hot), jnp.bfloat16),
            jax.ShapeDtypeStruct((4, *res), jnp.bfloat16),
        ),
        in_specs=[
            pl.BlockSpec(memory_space=VMEM),
            pl.BlockSpec(memory_space=VMEM),
            pl.BlockSpec(memory_space=VMEM),
            pl.BlockSpec(memory_space=pltpu.SMEM),
            pl.BlockSpec(memory_space=VMEM),
        ],
        out_specs=(pl.BlockSpec(memory_space=VMEM),) * 4,
        scratch_shapes=[
            VMEM(hot, jnp.bfloat16),
            VMEM((2, *res), jnp.bfloat16),
            dma((2, 2)),
            dma((2, 2)),
            dma((full + 1, 2)),
            dma((full + 1, 2)),
            dma((full + 1, 2)),
            dma((full + 1, 2)),
            dma((2 * xs,)),
            dma((2 * xs,)),
            dma((2 * xs,)),
            dma((2 * xs,)),
            dma((4,)),
            dma((4,)),
            dma((2,)),
        ],
        compiler_params=pltpu.CompilerParams(
            collective_id=0, has_side_effects=True, vmem_limit_bytes=24 << 20
        ),
        name="exchange",
    )(k, v, q, scored, residual)


def flash_kernel(
    sizes,
    docs,
    lengths,
    q_ref,
    kv_ref,
    hot_ref,
    o_ref,
    l_ref,
    co_ref,
    cl_ref,
    acc,
    top,
    causal,
    start,
    order,
    where,
):
    xs, zs = sizes
    chunks = 2 * zs
    xq = pl.program_id(0)
    x, yh, z, _ = (lax.axis_index(n) for n in CTX)
    tok = q_ref.shape[2]
    rows = 2 * tok
    plane = chunks * rows
    heads = q_ref.shape[3] // HEAD_SIZE
    first = xq * plane + (yh * zs + z) * rows
    lanes = lax.broadcasted_iota(jnp.int32, (rows, 128), 1)
    positions = first + lax.broadcasted_iota(jnp.int32, (rows, 128), 0)
    begins = jnp.zeros((rows, 128), jnp.int32)
    low = jnp.int32(0)
    doc_start = jnp.int32(0)
    for d in range(docs):
        begins = jnp.where(positions >= doc_start, doc_start, begins)
        low = jnp.where(first >= doc_start, doc_start, low)
        doc_start = doc_start + lengths[d]
    causal[...] = positions - lanes
    start[...] = begins - lanes
    acc[...] = jnp.zeros_like(acc)
    top[...] = jnp.full_like(top, NEG)

    active = jnp.int32(0)
    for i in range(chunks):
        zz, yy = (i // 2, i % 2)
        base = lax.rem(x + 2 * xs * zs - zz, xs) * plane + (yy * zs + zz) * rows
        order[active] = i
        where[active] = base
        active = active + jnp.where((base < first + rows) & (base + rows > low), 1, 0)

    def attend(places):
        keys, values, biases = [], [], []
        for place in places:
            chunk, base = (order[place], where[place])
            zz, yy = (chunk // 2, lax.rem(chunk, 2))
            for k in range(2):
                keys.append(kv_ref[zz, 2 * yy + k, 0])
                values.append(kv_ref[zz, 2 * yy + k, 1])
                at = base + k * tok
                ok = (causal[...] >= at) & (start[...] <= at)
                biases.append(jnp.where(ok, 0.0, NEG))
        key = jnp.concatenate(keys, axis=0)
        value = jnp.concatenate(values, axis=0)
        value = jnp.concatenate([value, jnp.ones_like(value)], axis=1)
        bias = jnp.concatenate(biases, axis=1)
        for h in range(heads):
            cols = slice(h * HEAD_SIZE, (h + 1) * HEAD_SIZE)
            q = q_ref[0, :, :, cols].reshape(rows, HEAD_SIZE)
            s = lax.dot_general(
                q, key, (((1,), (1,)), ((), ())), preferred_element_type=jnp.float32
            )
            s = s * SCALE + bias
            old = top[h]
            new = jnp.maximum(old, jnp.max(s, axis=1, keepdims=True))
            w = jnp.exp2(s - new[:, :1]).astype(jnp.bfloat16)
            update = jnp.dot(w, value, preferred_element_type=jnp.float32)
            shrink = jnp.exp2(old - new)
            top[h] = new
            acc[h] = acc[h] * jnp.concatenate([shrink, shrink], axis=1) + update

    def step(pair, carry):
        attend((2 * pair, 2 * pair + 1))
        return carry

    lax.fori_loop(0, active // 2, step, 0)

    @pl.when(lax.rem(active, 2) == 1)
    def _():
        attend((active - 1,))


    packed = jnp.zeros((rows, 128), jnp.float32)
    for h in range(heads):
        total = jnp.maximum(acc[h, :, HEAD_SIZE:], 1e-30)
        out = acc[h, :, :HEAD_SIZE] / total
        o_ref[0, :, :, h * HEAD_SIZE : (h + 1) * HEAD_SIZE] = out.astype(jnp.bfloat16).reshape(
            2, tok, HEAD_SIZE
        )
        packed = jnp.where(lanes == h, top[h] + jnp.log2(total), packed)
    chosen, levels = 0.0, 0.0
    for k in range(2):
        level = packed[k * tok : (k + 1) * tok]
        l_ref[0, k] = jnp.transpose(level)[:8]
        hot = hot_ref[0, k]
        chosen = chosen + jnp.dot(hot, o_ref[0, k], preferred_element_type=jnp.float32)
        levels = levels + jnp.dot(
            hot.astype(jnp.float32),
            level,
            preferred_element_type=jnp.float32,
            precision=lax.Precision.HIGHEST,
        )
    co_ref[0] = chosen.astype(jnp.bfloat16)
    cl_ref[0] = levels


def flash(sizes, lengths, q, kv, hot):
    xs, _, tok, width = q.shape
    heads = width // HEAD_SIZE
    keys = kv.shape[0] * 4 * tok
    rows = 2 * tok
    picks = hot.shape[2]

    def whole(*shape):
        return pl.BlockSpec((1, *shape), lambda i: (i,) + (0,) * len(shape))

    return pl.pallas_call(
        functools.partial(flash_kernel, sizes, lengths.shape[0]),
        out_shape=(
            jax.ShapeDtypeStruct(q.shape, jnp.bfloat16),
            jax.ShapeDtypeStruct((xs, 2, 8, 128), jnp.float32),
            jax.ShapeDtypeStruct((xs, picks, width), jnp.bfloat16),
            jax.ShapeDtypeStruct((xs, picks, 128), jnp.float32),
        ),
        grid=(xs,),
        in_specs=[
            pl.BlockSpec(memory_space=pltpu.SMEM),
            whole(2, tok, width),
            pl.BlockSpec(memory_space=VMEM),
            whole(2, picks, 128),
        ],
        out_specs=(
            whole(2, tok, width),
            whole(2, 8, 128),
            whole(picks, width),
            whole(picks, 128),
        ),
        scratch_shapes=[
            VMEM((heads, rows, 2 * HEAD_SIZE), jnp.float32),
            VMEM((heads, rows, 128), jnp.float32),
            VMEM((rows, 128), jnp.int32),
            VMEM((rows, 128), jnp.int32),
            pltpu.SMEM((2 * sizes[1] + 2,), jnp.int32),
            pltpu.SMEM((2 * sizes[1] + 2,), jnp.int32),
        ],
        compiler_params=pltpu.CompilerParams(vmem_limit_bytes=32 << 20),
        cost_estimate=pl.CostEstimate(
            flops=4 * heads * xs * rows * keys * HEAD_SIZE // 3,
            bytes_accessed=4 << 20,
            transcendentals=heads * xs * rows * keys // 3,
        ),
        name="flash",
    )(lengths, q, kv, hot)


def shares_of(levels):
    highest = functools.reduce(jnp.maximum, levels)
    parts = [jnp.exp2(level - highest) for level in levels]
    total = functools.reduce(jnp.add, parts)
    return [part / total for part in parts]


def tail_kernel(
    sizes,
    width_full,
    o_ref,
    l_ref,
    co_ref,
    cl_ref,
    res_ref,
    gain_ref,
    ids_ref,
    ow_ref,
    lm_ref,
    att_ref,
    out_ref,
    obuf,
    lbuf,
    cobuf,
    clbuf,
    wbuf,
    lmbuf,
    psend,
    pbuf,
    sqbuf,
    ubuf,
    g_ref,
    logits,
    arrived,
    sbuf,
    fbuf,
    w_sem,
    o_send,
    o_recv,
    l_send,
    l_recv,
    c_send,
    c_recv,
    p_sem,
    s_send,
    s_recv,
    u_sem,
    z_send,
    z_recv,
    x_send,
    x_recv,
    k_send,
    k_recv,
    e_send,
    e_recv,
    m_send,
    m_recv,
    f_send,
    f_recv,
):
    xs, zs = sizes
    x, yh, z, kc = (lax.axis_index(n) for n in CTX)
    hd = lax.axis_index("head")
    ok, oh = (lax.rem(kc + 1, 2), lax.rem(hd + 1, 2))
    row_slot = 2 * yh + kc
    half = width_full // 2
    wide = half // 2
    heads = o_ref.shape[3] // HEAD_SIZE
    z_order = sorted(range(1, zs), key=lambda d: min(d, zs - d))
    x_order = sorted(range(1, xs), key=lambda d: min(d, xs - d))

    weights = []
    for j, side in enumerate((hd, oh)):
        col = pl.multiple_of(side * half + kc * wide, 128)
        weights.append(
            pltpu.make_async_copy(ow_ref.at[:, pl.ds(col, wide)], wbuf.at[j], w_sem.at[j])
        )
        weights[-1].start()
    embedding = pltpu.make_async_copy(lm_ref, lmbuf, w_sem.at[2])
    embedding.start()

    peers = []
    for dx in range(xs):
        for dy in range(2):
            for dk in range(2):
                if dx or dy or dk:
                    peers.append(
                        {
                            "x": lax.rem(x + dx, xs),
                            "yh": lax.rem(yh + dy, 2),
                            "core": lax.rem(kc + dk, 2),
                        }
                    )
    for where in ({}, {"core": ok}):
        peers.append({"head": oh, **where})
    for dz in range(1, zs):
        peers.append({"z": lax.rem(z + dz, zs)})
        peers.append({"z": lax.rem(z + dz, zs), "head": oh})
    greet(peers)

    def c_copies(dx, dy, dk):
        where = {
            "x": lax.rem(x + dx, xs),
            "yh": lax.rem(yh + dy, 2),
            "core": lax.rem(kc + dk, 2),
        }
        at = where["x"]
        own = (x, yh, kc)
        return (
            remote(
                cl_ref.at[at],
                clbuf.at[own],
                c_send.at[0, 4 * dx + 2 * dy + dk],
                c_recv.at[0, 4 * x + row_slot],
                **where,
            ),
            remote(
                co_ref.at[at],
                cobuf.at[own],
                c_send.at[1, 4 * dx + 2 * dy + dk],
                c_recv.at[1, 4 * x + row_slot],
                **where,
            ),
        )

    c_order = [
        (dx, dy, dk)
        for dx in list(reversed(x_order)) + [0]
        for dy in (1, 0)
        for dk in (0, 1)
        if dx or dy or dk
    ]
    for each in c_order:
        for copy in c_copies(*each):
            copy.start()
    pltpu.make_async_copy(
        cl_ref.at[x], clbuf.at[x, yh, kc], c_recv.at[0, 4 * x + row_slot]
    ).start()
    pltpu.make_async_copy(
        co_ref.at[x], cobuf.at[x, yh, kc], c_recv.at[1, 4 * x + row_slot]
    ).start()

    def o_copies(dx, dk):
        tx, tk = (lax.rem(x + dx, xs), lax.rem(kc + dk, 2))
        where = {"x": tx, "core": tk}
        s, mine = (2 * dx + dk, 2 * x + kc)
        return (
            remote(l_ref.at[tx, tk], lbuf.at[x, kc], l_send.at[s], l_recv.at[mine], **where),
            remote(o_ref.at[tx, tk], obuf.at[x, kc], o_send.at[s], o_recv.at[mine], **where),
        )

    o_order = [
        (dx, dk) for dx in list(reversed(x_order)) + [0] for dk in (0, 1) if dx or dk
    ]
    for dx, dk in o_order:
        for copy in o_copies(dx, dk):
            copy.start()
    pltpu.make_async_copy(o_ref.at[x, kc], obuf.at[x, kc], o_recv.at[2 * x + kc]).start()
    pltpu.make_async_copy(l_ref.at[x, kc], lbuf.at[x, kc], l_recv.at[2 * x + kc]).start()

    for s in range(4 * xs):
        at = (s // 4, s // 2 % 2, s % 2)
        for i, buf in enumerate((clbuf, cobuf)):
            part = buf.at[at]
            remote(part, part, c_send.at[i, 0], c_recv.at[i, s], head=oh).wait_recv()
    pieces = []
    for k in range(2):
        shares = shares_of(
            [jnp.concatenate([clbuf[j, 0, k], clbuf[j, 1, k]], axis=0) for j in range(xs)]
        )
        values = [
            jnp.concatenate([cobuf[j, yy, k].astype(jnp.float32) for yy in range(2)], axis=0)
            for j in range(xs)
        ]
        for h in range(heads):
            cols = slice(h * HEAD_SIZE, (h + 1) * HEAD_SIZE)
            merged = sum(shares[j][:, h : h + 1] * values[j][:, cols] for j in range(xs))
            pieces.append(merged.astype(jnp.bfloat16))
    chosen = jnp.concatenate(pieces, axis=1)

    for copy in weights:
        copy.wait()
    psend[...] = jnp.dot(chosen, wbuf[1], preferred_element_type=jnp.float32).astype(jnp.bfloat16)
    p_copy = remote(psend, pbuf, p_sem.at[0], p_sem.at[1], head=oh)
    p_copy.start()
    hidden = jnp.dot(chosen, wbuf[0], preferred_element_type=jnp.float32)
    residual = (res_ref[0] + res_ref[1]) + (res_ref[2] + res_ref[3])
    p_copy.wait_recv()
    hidden = residual.astype(jnp.float32) + (hidden + pbuf[...].astype(jnp.float32))

    own = 2 * hd + kc
    sqbuf[own] = jnp.broadcast_to(jnp.sum(hidden * hidden, axis=1, keepdims=True), (16, 128))

    def s_copy(d):
        return remote(
            sqbuf.at[own],
            sqbuf.at[own],
            s_send.at[d],
            s_recv.at[d],
            head=lax.rem(hd + d // 2, 2),
            core=lax.rem(kc + d % 2, 2),
        )

    for d in range(1, 4):
        s_copy(d).start()
    for d in range(1, 4):
        s_copy(d).wait_recv()
    squares = (sqbuf[0] + sqbuf[1]) + (sqbuf[2] + sqbuf[3])
    scale = lax.rsqrt(squares / width_full + 1e-05)[:, :1]
    ubuf[...] = (hidden * scale * gain_ref[kc]).astype(jnp.bfloat16)
    both = pl.ds(pl.multiple_of(kc * wide, 128), wide)

    def block(bx, bz):
        return g_ref.at[bx, bz, :, both]

    def z_copy(dz):
        to = lax.rem(z + dz, zs)
        return remote(ubuf, block(x, z), z_send.at[dz], z_recv.at[dz], z=to)

    def x_copy(dx, dz):
        bz = lax.rem(z + zs - dz, zs)
        to = lax.rem(x + dx, xs)
        return remote(block(x, bz), block(x, bz), x_send.at[dx, dz], x_recv.at[dx, dz], x=to)

    def relay(dz):
        bz = lax.rem(z + zs - dz, zs)
        step = 1 if 2 * dz < zs - 2 else xs - 1
        part = block(lax.rem(x + xs - step, xs), bz)
        to = lax.rem(x + step, xs)
        return remote(part, part, x_send.at[2, dz], x_recv.at[2, dz], x=to)

    def plane_of(dx):
        return lax.rem(x + xs - dx, xs)

    def k_copy(dx):
        plane = g_ref.at[plane_of(dx), :, :, both]
        return remote(plane, plane, k_send.at[dx], k_recv.at[dx], core=ok)

    def e_copy(dx):
        at = plane_of(dx)
        return remote(
            logits.at[at, oh], arrived.at[at], e_send.at[dx], e_recv.at[dx], head=oh
        )

    def project(dx):
        at = plane_of(dx)
        k_copy(dx).wait_recv()
        rows = g_ref[at].reshape(zs * 16, half)
        out = lax.dot_general(
            rows, lmbuf[...], (((1,), (1,)), ((), ())), preferred_element_type=jnp.float32
        )
        logits[at] = out.astype(jnp.bfloat16).reshape(logits.shape[1:])
        e_copy(dx).start()

    def reduce_plane(dx, packed):
        at = plane_of(dx)
        e_copy(dx).wait_recv()
        both_halves = logits[at, hd].astype(jnp.float32) + arrived[at].astype(jnp.float32)
        rows, width = both_halves.shape
        highest = jnp.max(both_halves, axis=1, keepdims=True)
        total = jnp.sum(jnp.exp(both_halves - highest), axis=1, keepdims=True)
        match = ids_ref[at] == lax.broadcasted_iota(jnp.int32, (rows, width), 1)
        target = jnp.sum(jnp.where(match, both_halves, 0.0), axis=1, keepdims=True)
        lane = lax.broadcasted_iota(jnp.int32, packed.shape, 1)
        row = lax.broadcasted_iota(jnp.int32, packed.shape, 0)
        low = lax.rem(at, 2) * rows
        here = (row >= low) & (row < low + rows)
        for i, column in enumerate((highest, total, target)):
            column = jnp.concatenate([column, column], axis=0)
            packed = jnp.where(here & (lane == at // 2 + 2 * i), column, packed)
        return packed

    for dz in reversed(z_order):
        z_copy(dz).start()
    here = pltpu.make_async_copy(ubuf, block(x, z), u_sem)
    here.start()
    here.wait()
    z_seq = [0] + z_order
    sides = [1, xs - 1] if xs > 2 else [1]
    for dz in z_seq:
        if dz:
            z_copy(dz).wait_recv()
        for dx in sides:
            x_copy(dx, dz).start()
    k_copy(0).start()
    embedding.wait()
    project(0)
    for s in range(2 * xs):
        at = (s // 2, s % 2)
        for buf, send, recv in ((lbuf, l_send, l_recv), (obuf, o_send, o_recv)):
            part = buf.at[at]
            remote(part, part, send.at[0], recv.at[s], head=oh).wait_recv()
    for k in range(2):
        parts = shares_of([lbuf[j, k] for j in range(xs)])
        parts.append(jnp.zeros((128 - 8 * xs, 128), jnp.float32))
        shares = jnp.transpose(jnp.concatenate(parts, axis=0))
        for h in range(heads):
            cols = slice(h * HEAD_SIZE, (h + 1) * HEAD_SIZE)
            merged = sum(
                shares[:, 8 * j + h : 8 * j + h + 1] * obuf[j, k, :, cols].astype(jnp.float32)
                for j in range(xs)
            )
            at = (k * heads + h) * HEAD_SIZE
            att_ref[:, at : at + HEAD_SIZE] = merged.astype(jnp.bfloat16)

    for dz in z_seq:
        for dx in sides:
            x_copy(dx, dz).wait_recv()
        if xs > 2:
            relay(dz).start()
    for dx in sides:
        k_copy(dx).start()
    for dx in sides:
        project(dx)

    packed = jnp.zeros((zs * 16, 128), jnp.float32)
    packed = reduce_plane(0, packed)
    if xs > 2:
        for dz in z_seq:
            relay(dz).wait_recv()
        k_copy(2).start()
        packed = reduce_plane(1, packed)
        project(2)
        packed = reduce_plane(xs - 1, packed)
        packed = reduce_plane(2, packed)
    else:
        packed = reduce_plane(1, packed)
    mine = 4 * x + row_slot
    sbuf[mine] = jnp.transpose(packed)[:8]

    def merged(parts):
        tops = [part[0:2] for part in parts]
        top = functools.reduce(jnp.maximum, tops)
        total = functools.reduce(
            jnp.add, [part[2:4] * jnp.exp(part[0:2] - top) for part in parts]
        )
        target = functools.reduce(jnp.add, [part[4:6] for part in parts])
        return (top, total, target)

    def m_copy(dx, dy, dk):
        s = 4 * dx + 2 * dy + dk
        return remote(
            sbuf.at[mine],
            sbuf.at[mine],
            m_send.at[s],
            m_recv.at[s],
            x=lax.rem(x + dx, xs),
            yh=lax.rem(yh + dy, 2),
            core=lax.rem(kc + dk, 2),
        )

    for each in c_order:
        m_copy(*each).start()
    for each in c_order:
        m_copy(*each).wait_recv()
    top, total, target = merged([sbuf[s] for s in range(4 * xs)])
    fbuf[hd, z] = jnp.concatenate([top, total, target, target], axis=0)

    def f_copy(dh, dz):
        part = fbuf.at[hd, z]
        s = zs * dh + dz
        where = {"head": lax.rem(hd + dh, 2), "z": lax.rem(z + dz, zs)}
        return remote(part, part, f_send.at[s], f_recv.at[s], **where)

    f_order = [(dh, dz) for dz in reversed([0] + z_order) for dh in (0, 1) if dh or dz]
    for each in f_order:
        f_copy(*each).start()
    for each in f_order:
        f_copy(*each).wait_recv()
    for h in range(2):
        top, total, target = merged([fbuf[h, zz] for zz in range(zs)])
        found = target - top - jnp.log(total)
        out_ref[h] = jnp.concatenate([found] * 4, axis=0)

    for each in c_order:
        for copy in c_copies(*each):
            copy.wait_send()
    for dx, dk in o_order:
        for copy in o_copies(dx, dk):
            copy.wait_send()
    p_copy.wait_send()
    for d in range(1, 4):
        s_copy(d).wait_send()
    for dz in z_order:
        z_copy(dz).wait_send()
    for dz in range(zs):
        for dx in sides:
            x_copy(dx, dz).wait_send()
        if xs > 2:
            relay(dz).wait_send()
    for dx in range(xs):
        k_copy(dx).wait_send()
        e_copy(dx).wait_send()
    for each in c_order:
        m_copy(*each).wait_send()
    for each in f_order:
        f_copy(*each).wait_send()


def tail(sizes, o, l, co, cl, res, gain, ids, out_weight, lm_weight):
    xs, zs = sizes
    tok = o.shape[2]
    depth, width_full = out_weight.shape
    vocab, half = lm_weight.shape
    wide = half // 2
    side = zs * 8
    dma = pltpu.SemaphoreType.DMA
    bf16, f32 = (jnp.bfloat16, jnp.float32)
    hbm = pl.BlockSpec(memory_space=pltpu.HBM)
    return pl.pallas_call(
        functools.partial(tail_kernel, sizes, width_full),
        out_shape=(
            jax.ShapeDtypeStruct((tok, depth), bf16),
            jax.ShapeDtypeStruct((2, 8, 2 * side), f32),
        ),
        in_specs=[pl.BlockSpec(memory_space=VMEM)] * 7 + [hbm] * 2,
        out_specs=(pl.BlockSpec(memory_space=VMEM),) * 2,
        scratch_shapes=[
            VMEM(o.shape, bf16),
            VMEM(l.shape, f32),
            VMEM((xs, 2, 2, *co.shape[1:]), bf16),
            VMEM((xs, 2, 2, *cl.shape[1:]), f32),
            VMEM((2, depth, wide), bf16),
            VMEM((vocab, half), bf16),
            VMEM((16, wide), bf16),
            VMEM((16, wide), bf16),
            VMEM((4, 16, 128), f32),
            VMEM((16, wide), bf16),
            VMEM((xs, zs, 16, half), bf16),
            VMEM((xs, 2, side, vocab), bf16),
            VMEM((xs, side, vocab), bf16),
            VMEM((4 * xs, 8, 2 * side), f32),
            VMEM((2, zs, 8, 2 * side), f32),
            dma((3,)),
            dma((2 * xs,)),
            dma((2 * xs,)),
            dma((2 * xs,)),
            dma((2 * xs,)),
            dma((2, 4 * xs)),
            dma((2, 4 * xs)),
            dma((2,)),
            dma((4,)),
            dma((4,)),
            dma,
            dma((zs,)),
            dma((zs,)),
            dma((xs, zs)),
            dma((xs, zs)),
            dma((xs,)),
            dma((xs,)),
            dma((xs,)),
            dma((xs,)),
            dma((4 * xs,)),
            dma((4 * xs,)),
            dma((2 * zs,)),
            dma((2 * zs,)),
        ],
        compiler_params=pltpu.CompilerParams(
            collective_id=1, has_side_effects=True, vmem_limit_bytes=50 << 20
        ),
        name="tail",
    )(o, l, co, cl, res, gain, ids, out_weight, lm_weight)


def per_device(
    sizes,
    queries,
    rotated_keys,
    value_matrix,
    doc_lengths,
    scored,
    residual,
    norm_gain,
    out_weight,
    lm_weight,
    token_ids,
    old_logp,
    advantage,
):
    xs, zs = sizes
    x, yh, z, kc = (lax.axis_index(n) for n in CTX)
    hd = lax.axis_index("head")
    resp = scored.shape[0]
    half = residual.shape[1]
    kvs, qs, hots, res = exchange(
        sizes, rotated_keys, value_matrix, queries, scored, residual
    )
    o, l, co, cl = flash(sizes, doc_lengths, qs, kvs, hots)

    gain = norm_gain.reshape(2, 1, half // 2)
    vocab = lm_weight.shape[1]
    start = (((x * 2 + yh) * zs + z) * 2 + kc) * vocab
    ids = token_ids.reshape(xs, 2, 2, zs // 2, 2, resp).transpose(2, 0, 3, 1, 4, 5)
    ids = lax.dynamic_index_in_dim(ids.reshape(2, xs, -1, 1), hd, 0, keepdims=False) - start
    attended, found = tail(sizes, o, l, co, cl, res, gain, ids, out_weight, lm_weight.T)
    found = found[:, : xs // 2].reshape(2, xs, zs // 2, 2, 2, resp)
    log_probs = found.transpose(1, 3, 0, 2, 4, 5).reshape(-1)
    ratio = jnp.exp(jnp.clip(log_probs - old_logp, -4.0, 4.0))
    token_loss = -jnp.minimum(ratio * advantage, jnp.clip(ratio, 0.8, 1.2) * advantage)
    return (attended, log_probs, token_loss)


def solution(mesh, shape=(4, 2, 8, 2)):
    finer = Mesh(mesh.devices.reshape(*shape, mesh.shape["head"]), NAMES)
    placed = (
        P(CTX, "head"),
        P(CTX, "head"),
        P(CTX, "head"),
        P(),
        P(CTX),
        P(CTX, "head"),
        P("head"),
        P("head", None),
        P("head", CTX),
        P(),
        P(),
        P(),
    )
    return jax.shard_map(
        functools.partial(per_device, (shape[0], shape[2])),
        mesh=finer,
        in_specs=placed,
        out_specs=(P(CTX, "head"), P(), P()),
        check_vma=False,
    )
```

```python
import functools
import math

import jax
import jax.numpy as jnp
from jax import lax
from jax.experimental import pallas as pl
from jax.experimental.pallas import tpu as pltpu
from jax.sharding import Mesh
from jax.sharding import PartitionSpec as P

HEAD_SIZE = 128
CTX = ("x", "yh", "z", "core")
NAMES = ("x", "yh", "z", "core", "head")
NEG = -1e30
SCALE = HEAD_SIZE**-0.5 * math.log2(math.e)
MESH = pl.DeviceIdType.MESH
VMEM = pltpu.VMEM


def remote(src, dst, send_sem, recv_sem, **where):
    return pltpu.make_async_remote_copy(
        src_ref=src,
        dst_ref=dst,
        send_sem=send_sem,
        recv_sem=recv_sem,
        device_id=where,
        device_id_type=MESH,
    )


def greet(peers):
    barrier = pltpu.get_barrier_semaphore()
    for where in peers:
        pl.semaphore_signal(barrier, inc=1, device_id=where, device_id_type=MESH)
    pl.semaphore_wait(barrier, len(peers))


def exchange_kernel(
    sizes,
    k_ref,
    v_ref,
    q_ref,
    scored_ref,
    own_ref,
    kvbuf,
    qbuf,
    hotbuf,
    resbuf,
    hot_ref,
    res_ref,
    first_send,
    first_recv,
    up_send,
    up_recv,
    down_send,
    down_recv,
    q_send,
    q_recv,
    h_send,
    h_recv,
    r_send,
    r_recv,
    y_sem,
):
    xs, zs = sizes
    x, yh, z, kc = (lax.axis_index(n) for n in CTX)
    up, down = (lax.rem(z + 1, zs), lax.rem(z + zs - 1, zs))
    shift = lax.rem(z, xs)
    tx = lax.rem(x + z, xs)
    mine = 2 * yh + kc
    group = q_ref.shape[1] // 2
    peers = []
    for dx in range(xs):
        for dy in range(2):
            for dk in range(2):
                if dx or dy or dk:
                    peers.append(
                        {
                            "x": lax.rem(x + dx, xs),
                            "yh": lax.rem(yh + dy, 2),
                            "core": lax.rem(kc + dk, 2),
                        }
                    )
    peers.append({"z": up})
    peers.append({"z": down})
    picks = scored_ref.shape[0]
    row = lax.broadcasted_iota(jnp.int32, hot_ref.shape, 0)
    lane = lax.broadcasted_iota(jnp.int32, hot_ref.shape, 1)
    hot = jnp.zeros(hot_ref.shape, jnp.float32)
    for i in range(picks):
        hot = jnp.where((row == picks * kc + i) & (lane == scored_ref[i]), 1.0, hot)
    hot_ref[...] = hot.astype(jnp.bfloat16)
    wide = res_ref.shape[2]
    row = lax.broadcasted_iota(jnp.int32, res_ref.shape[1:], 0)
    for side in range(2):
        own = own_ref[:, side * wide : (side + 1) * wide].astype(jnp.float32)
        placed = jnp.zeros(res_ref.shape[1:], jnp.float32)
        for i in range(picks):
            placed = jnp.where(row == picks * mine + i, own[i : i + 1], placed)
        res_ref[side] = placed.astype(jnp.bfloat16)
    greet(peers)

    def columns(ref, head, width):
        return ref.at[:, pl.ds(pl.multiple_of(head * width, 128), width)]

    def first(dk):
        tk = lax.rem(kc + dk, 2)
        return [
            remote(
                columns(ref, tk, HEAD_SIZE),
                kvbuf.at[z, mine, i],
                first_send.at[dk, i],
                first_recv.at[kc, i],
                x=tx,
                core=tk,
            )
            for i, ref in enumerate((k_ref, v_ref))
        ]

    def first_here():
        return [
            pltpu.make_async_copy(
                columns(ref, kc, HEAD_SIZE), kvbuf.at[z, mine, i], first_recv.at[kc, i]
            )
            for i, ref in enumerate((k_ref, v_ref))
        ]

    for copy in first(1):
        copy.start()

    @pl.when(shift == 0)
    def _():
        for copy in first_here():
            copy.start()

    @pl.when(shift != 0)
    def _():
        for copy in first(0):
            copy.start()

    def q_copies(dx, dk):
        ox, tk = (lax.rem(x + dx, xs), lax.rem(kc + dk, 2))
        s, own = (2 * dx + dk, 2 * x + kc)
        where = {"x": ox, "core": tk}
        q_part = columns(q_ref, tk, group)
        return (
            remote(hot_ref, hotbuf.at[x, kc], h_send.at[s], h_recv.at[own], **where),
            remote(q_part, qbuf.at[x, kc], q_send.at[s], q_recv.at[own], **where),
        )

    pltpu.make_async_copy(
        columns(q_ref, kc, group), qbuf.at[x, kc], q_recv.at[2 * x + kc]
    ).start()
    pltpu.make_async_copy(hot_ref, hotbuf.at[x, kc], h_recv.at[2 * x + kc]).start()
    q_order = [
        (dx, dk)
        for dx in [0] + sorted(range(1, xs), key=lambda d: min(d, xs - d))
        for dk in (0, 1)
        if dx or dk
    ]
    for dx, dk in q_order:
        for copy in q_copies(dx, dk):
            copy.start()

    near = ((0, 1), (1, 0), (1, 1))

    def r_copy(dy, dk):
        ty, tk = (lax.rem(yh + dy, 2), lax.rem(kc + dk, 2))
        return remote(
            res_ref.at[tk],
            resbuf.at[mine],
            r_send.at[2 * dy + dk],
            r_recv.at[mine],
            yh=ty,
            core=tk,
        )

    for dy, dk in near:
        r_copy(dy, dk).start()
    pltpu.make_async_copy(res_ref.at[kc], resbuf.at[mine], r_recv.at[mine]).start()

    def first_wait(k):
        for i in range(2):
            part = kvbuf.at[z, 2 * yh + k, i]
            remote(part, part, first_send.at[0, i], first_recv.at[k, i], z=up).wait_recv()

    def across(side):
        part = kvbuf.at[z, pl.ds(2 * side, 2)]
        return remote(part, part, y_sem.at[0], y_sem.at[1], yh=lax.rem(yh + 1, 2))

    for k in range(2):
        first_wait(k)
    across(yh).start()

    def ring(going_up, slot, t, h):
        send, recv, to = (up_send, up_recv, up) if going_up else (down_send, down_recv, down)
        part = kvbuf.at[slot, pl.ds(2 * lax.rem(yh + h, 2), 2)]
        return remote(part, part, send.at[t, h], recv.at[t, h], z=to)

    def sent(going_up, t, h):
        slot = lax.rem(z - t + zs, zs) if going_up else lax.rem(z + t, zs)
        return ring(going_up, slot, t, h)

    def got(going_up, t, h):
        slot = lax.rem(z - 1 - t + zs, zs) if going_up else lax.rem(z + 1 + t, zs)
        return ring(going_up, slot, t, h)

    full = (zs - 2) // 2
    for t in range(full):
        for h in range(2):
            if t == 0 and h == 1:
                across(1 - yh).wait_recv()
            for going_up in (True, False):
                if t > 0:
                    got(going_up, t - 1, h).wait_recv()
                sent(going_up, t, h).start()
    if full == 0:
        across(1 - yh).wait_recv()
    for going_up, h in ((True, 0), (False, 1)):
        if full > 0:
            got(going_up, full - 1, h).wait_recv()
        sent(going_up, full, h).start()
    if full > 0:
        got(True, full - 1, 1).wait_recv()
        got(False, full - 1, 0).wait_recv()
    got(True, full, 0).wait_recv()
    got(False, full, 1).wait_recv()

    for t in range(full):
        for h in range(2):
            for going_up in (True, False):
                sent(going_up, t, h).wait_send()
    sent(True, full, 0).wait_send()
    sent(False, full, 1).wait_send()
    for copy in first(1):
        copy.wait_send()
    across(yh).wait_send()

    @pl.when(shift != 0)
    def _():
        for copy in first(0):
            copy.wait_send()

    for dy, dk in near:
        r_copy(dy, dk).wait_send()
    for s in range(4):
        part = resbuf.at[s]
        remote(part, part, r_send.at[0], r_recv.at[s], z=up).wait_recv()
    for dx, dk in q_order:
        for copy in q_copies(dx, dk):
            copy.wait_send()
    for s in range(2 * xs):
        part = qbuf.at[s // 2, s % 2]
        remote(part, part, q_send.at[0], q_recv.at[s], z=up).wait_recv()
        part = hotbuf.at[s // 2, s % 2]
        remote(part, part, h_send.at[0], h_recv.at[s], z=up).wait_recv()


def exchange(sizes, k, v, q, scored, residual):
    xs, zs = sizes
    tok = q.shape[0]
    picks, half = residual.shape
    hot, res = ((2 * picks, tok), (4 * picks, half // 2))
    full = (zs - 2) // 2
    dma = pltpu.SemaphoreType.DMA
    return pl.pallas_call(
        functools.partial(exchange_kernel, sizes),
        out_shape=(
            jax.ShapeDtypeStruct((zs, 4, 2, tok, HEAD_SIZE), k.dtype),
            jax.ShapeDtypeStruct((xs, 2, tok, q.shape[1] // 2), q.dtype),
            jax.ShapeDtypeStruct((xs, 2, *hot), jnp.bfloat16),
            jax.ShapeDtypeStruct((4, *res), jnp.bfloat16),
        ),
        in_specs=[
            pl.BlockSpec(memory_space=VMEM),
            pl.BlockSpec(memory_space=VMEM),
            pl.BlockSpec(memory_space=VMEM),
            pl.BlockSpec(memory_space=pltpu.SMEM),
            pl.BlockSpec(memory_space=VMEM),
        ],
        out_specs=(pl.BlockSpec(memory_space=VMEM),) * 4,
        scratch_shapes=[
            VMEM(hot, jnp.bfloat16),
            VMEM((2, *res), jnp.bfloat16),
            dma((2, 2)),
            dma((2, 2)),
            dma((full + 1, 2)),
            dma((full + 1, 2)),
            dma((full + 1, 2)),
            dma((full + 1, 2)),
            dma((2 * xs,)),
            dma((2 * xs,)),
            dma((2 * xs,)),
            dma((2 * xs,)),
            dma((4,)),
            dma((4,)),
            dma((2,)),
        ],
        compiler_params=pltpu.CompilerParams(
            collective_id=0, has_side_effects=True, vmem_limit_bytes=24 << 20
        ),
        name="exchange",
    )(k, v, q, scored, residual)


def flash_kernel(
    sizes,
    docs,
    lengths,
    q_ref,
    kv_ref,
    hot_ref,
    o_ref,
    l_ref,
    co_ref,
    cl_ref,
    acc,
    top,
    causal,
    start,
    order,
    where,
):
    xs, zs = sizes
    chunks = 2 * zs
    xq = pl.program_id(0)
    x, yh, z, _ = (lax.axis_index(n) for n in CTX)
    tok = q_ref.shape[2]
    rows = 2 * tok
    plane = chunks * rows
    heads = q_ref.shape[3] // HEAD_SIZE
    first = xq * plane + (yh * zs + z) * rows
    lanes = lax.broadcasted_iota(jnp.int32, (rows, 128), 1)
    positions = first + lax.broadcasted_iota(jnp.int32, (rows, 128), 0)
    begins = jnp.zeros((rows, 128), jnp.int32)
    low = jnp.int32(0)
    doc_start = jnp.int32(0)
    for d in range(docs):
        begins = jnp.where(positions >= doc_start, doc_start, begins)
        low = jnp.where(first >= doc_start, doc_start, low)
        doc_start = doc_start + lengths[d]
    causal[...] = positions - lanes
    start[...] = begins - lanes
    acc[...] = jnp.zeros_like(acc)
    top[...] = jnp.full_like(top, NEG)

    active = jnp.int32(0)
    for i in range(chunks):
        zz, yy = (i // 2, i % 2)
        base = lax.rem(x + 2 * xs * zs - zz, xs) * plane + (yy * zs + zz) * rows
        order[active] = i
        where[active] = base
        active = active + jnp.where((base < first + rows) & (base + rows > low), 1, 0)

    def attend(places):
        keys, values, biases = [], [], []
        for place in places:
            chunk, base = (order[place], where[place])
            zz, yy = (chunk // 2, lax.rem(chunk, 2))
            for k in range(2):
                keys.append(kv_ref[zz, 2 * yy + k, 0])
                values.append(kv_ref[zz, 2 * yy + k, 1])
                at = base + k * tok
                ok = (causal[...] >= at) & (start[...] <= at)
                biases.append(jnp.where(ok, 0.0, NEG))
        key = jnp.concatenate(keys, axis=0)
        value = jnp.concatenate(values, axis=0)
        value = jnp.concatenate([value, jnp.ones_like(value)], axis=1)
        bias = jnp.concatenate(biases, axis=1)
        for h in range(heads):
            cols = slice(h * HEAD_SIZE, (h + 1) * HEAD_SIZE)
            q = q_ref[0, :, :, cols].reshape(rows, HEAD_SIZE)
            s = lax.dot_general(
                q, key, (((1,), (1,)), ((), ())), preferred_element_type=jnp.float32
            )
            s = s * SCALE + bias
            old = top[h]
            new = jnp.maximum(old, jnp.max(s, axis=1, keepdims=True))
            w = jnp.exp2(s - new[:, :1]).astype(jnp.bfloat16)
            update = jnp.dot(w, value, preferred_element_type=jnp.float32)
            shrink = jnp.exp2(old - new)
            top[h] = new
            acc[h] = acc[h] * jnp.concatenate([shrink, shrink], axis=1) + update

    def step(pair, carry):
        attend((2 * pair, 2 * pair + 1))
        return carry

    lax.fori_loop(0, active // 2, step, 0)

    @pl.when(lax.rem(active, 2) == 1)
    def _():
        attend((active - 1,))


    packed = jnp.zeros((rows, 128), jnp.float32)
    for h in range(heads):
        total = jnp.maximum(acc[h, :, HEAD_SIZE:], 1e-30)
        out = acc[h, :, :HEAD_SIZE] / total
        o_ref[0, :, :, h * HEAD_SIZE : (h + 1) * HEAD_SIZE] = out.astype(jnp.bfloat16).reshape(
            2, tok, HEAD_SIZE
        )
        packed = jnp.where(lanes == h, top[h] + jnp.log2(total), packed)
    chosen, levels = 0.0, 0.0
    for k in range(2):
        level = packed[k * tok : (k + 1) * tok]
        l_ref[0, k] = jnp.transpose(level)[:8]
        hot = hot_ref[0, k]
        chosen = chosen + jnp.dot(hot, o_ref[0, k], preferred_element_type=jnp.float32)
        levels = levels + jnp.dot(
            hot.astype(jnp.float32),
            level,
            preferred_element_type=jnp.float32,
            precision=lax.Precision.HIGHEST,
        )
    co_ref[0] = chosen.astype(jnp.bfloat16)
    cl_ref[0] = levels


def flash(sizes, lengths, q, kv, hot):
    xs, _, tok, width = q.shape
    heads = width // HEAD_SIZE
    keys = kv.shape[0] * 4 * tok
    rows = 2 * tok
    picks = hot.shape[2]

    def whole(*shape):
        return pl.BlockSpec((1, *shape), lambda i: (i,) + (0,) * len(shape))

    return pl.pallas_call(
        functools.partial(flash_kernel, sizes, lengths.shape[0]),
        out_shape=(
            jax.ShapeDtypeStruct(q.shape, jnp.bfloat16),
            jax.ShapeDtypeStruct((xs, 2, 8, 128), jnp.float32),
            jax.ShapeDtypeStruct((xs, picks, width), jnp.bfloat16),
            jax.ShapeDtypeStruct((xs, picks, 128), jnp.float32),
        ),
        grid=(xs,),
        in_specs=[
            pl.BlockSpec(memory_space=pltpu.SMEM),
            whole(2, tok, width),
            pl.BlockSpec(memory_space=VMEM),
            whole(2, picks, 128),
        ],
        out_specs=(
            whole(2, tok, width),
            whole(2, 8, 128),
            whole(picks, width),
            whole(picks, 128),
        ),
        scratch_shapes=[
            VMEM((heads, rows, 2 * HEAD_SIZE), jnp.float32),
            VMEM((heads, rows, 128), jnp.float32),
            VMEM((rows, 128), jnp.int32),
            VMEM((rows, 128), jnp.int32),
            pltpu.SMEM((2 * sizes[1] + 2,), jnp.int32),
            pltpu.SMEM((2 * sizes[1] + 2,), jnp.int32),
        ],
        compiler_params=pltpu.CompilerParams(vmem_limit_bytes=32 << 20),
        cost_estimate=pl.CostEstimate(
            flops=4 * heads * xs * rows * keys * HEAD_SIZE // 3,
            bytes_accessed=4 << 20,
            transcendentals=heads * xs * rows * keys // 3,
        ),
        name="flash",
    )(lengths, q, kv, hot)


def shares_of(levels):
    highest = functools.reduce(jnp.maximum, levels)
    parts = [jnp.exp2(level - highest) for level in levels]
    total = functools.reduce(jnp.add, parts)
    return [part / total for part in parts]


def tail_kernel(
    sizes,
    width_full,
    o_ref,
    l_ref,
    co_ref,
    cl_ref,
    res_ref,
    gain_ref,
    ids_ref,
    ow_ref,
    lm_ref,
    att_ref,
    out_ref,
    obuf,
    lbuf,
    cobuf,
    clbuf,
    wbuf,
    lmbuf,
    psend,
    pbuf,
    sqbuf,
    ubuf,
    g_ref,
    logits,
    arrived,
    sbuf,
    fbuf,
    w_sem,
    o_send,
    o_recv,
    l_send,
    l_recv,
    c_send,
    c_recv,
    p_sem,
    s_send,
    s_recv,
    u_sem,
    z_send,
    z_recv,
    x_send,
    x_recv,
    k_send,
    k_recv,
    e_send,
    e_recv,
    m_send,
    m_recv,
    f_send,
    f_recv,
):
    xs, zs = sizes
    x, yh, z, kc = (lax.axis_index(n) for n in CTX)
    hd = lax.axis_index("head")
    ok, oh = (lax.rem(kc + 1, 2), lax.rem(hd + 1, 2))
    row_slot = 2 * yh + kc
    half = width_full // 2
    wide = half // 2
    heads = o_ref.shape[3] // HEAD_SIZE
    z_order = sorted(range(1, zs), key=lambda d: min(d, zs - d))
    x_order = sorted(range(1, xs), key=lambda d: min(d, xs - d))

    weights = []
    for j, side in enumerate((hd, oh)):
        col = pl.multiple_of(side * half + kc * wide, 128)
        weights.append(
            pltpu.make_async_copy(ow_ref.at[:, pl.ds(col, wide)], wbuf.at[j], w_sem.at[j])
        )
        weights[-1].start()
    embedding = pltpu.make_async_copy(lm_ref, lmbuf, w_sem.at[2])
    embedding.start()

    peers = []
    for dx in range(xs):
        for dy in range(2):
            for dk in range(2):
                if dx or dy or dk:
                    peers.append(
                        {
                            "x": lax.rem(x + dx, xs),
                            "yh": lax.rem(yh + dy, 2),
                            "core": lax.rem(kc + dk, 2),
                        }
                    )
    for where in ({}, {"core": ok}):
        peers.append({"head": oh, **where})
    for dz in range(1, zs):
        peers.append({"z": lax.rem(z + dz, zs)})
        peers.append({"z": lax.rem(z + dz, zs), "head": oh})
    greet(peers)

    def c_copies(dx, dy, dk):
        where = {
            "x": lax.rem(x + dx, xs),
            "yh": lax.rem(yh + dy, 2),
            "core": lax.rem(kc + dk, 2),
        }
        at = where["x"]
        own = (x, yh, kc)
        return (
            remote(
                cl_ref.at[at],
                clbuf.at[own],
                c_send.at[0, 4 * dx + 2 * dy + dk],
                c_recv.at[0, 4 * x + row_slot],
                **where,
            ),
            remote(
                co_ref.at[at],
                cobuf.at[own],
                c_send.at[1, 4 * dx + 2 * dy + dk],
                c_recv.at[1, 4 * x + row_slot],
                **where,
            ),
        )

    c_order = [
        (dx, dy, dk)
        for dx in list(reversed(x_order)) + [0]
        for dy in (1, 0)
        for dk in (0, 1)
        if dx or dy or dk
    ]
    for each in c_order:
        for copy in c_copies(*each):
            copy.start()
    pltpu.make_async_copy(
        cl_ref.at[x], clbuf.at[x, yh, kc], c_recv.at[0, 4 * x + row_slot]
    ).start()
    pltpu.make_async_copy(
        co_ref.at[x], cobuf.at[x, yh, kc], c_recv.at[1, 4 * x + row_slot]
    ).start()

    def o_copies(dx, dk):
        tx, tk = (lax.rem(x + dx, xs), lax.rem(kc + dk, 2))
        where = {"x": tx, "core": tk}
        s, mine = (2 * dx + dk, 2 * x + kc)
        return (
            remote(l_ref.at[tx, tk], lbuf.at[x, kc], l_send.at[s], l_recv.at[mine], **where),
            remote(o_ref.at[tx, tk], obuf.at[x, kc], o_send.at[s], o_recv.at[mine], **where),
        )

    o_order = [
        (dx, dk) for dx in list(reversed(x_order)) + [0] for dk in (0, 1) if dx or dk
    ]
    for dx, dk in o_order:
        for copy in o_copies(dx, dk):
            copy.start()
    pltpu.make_async_copy(o_ref.at[x, kc], obuf.at[x, kc], o_recv.at[2 * x + kc]).start()
    pltpu.make_async_copy(l_ref.at[x, kc], lbuf.at[x, kc], l_recv.at[2 * x + kc]).start()

    for s in range(4 * xs):
        at = (s // 4, s // 2 % 2, s % 2)
        for i, buf in enumerate((clbuf, cobuf)):
            part = buf.at[at]
            remote(part, part, c_send.at[i, 0], c_recv.at[i, s], head=oh).wait_recv()
    pieces = []
    for k in range(2):
        shares = shares_of(
            [jnp.concatenate([clbuf[j, 0, k], clbuf[j, 1, k]], axis=0) for j in range(xs)]
        )
        values = [
            jnp.concatenate([cobuf[j, yy, k].astype(jnp.float32) for yy in range(2)], axis=0)
            for j in range(xs)
        ]
        for h in range(heads):
            cols = slice(h * HEAD_SIZE, (h + 1) * HEAD_SIZE)
            merged = sum(shares[j][:, h : h + 1] * values[j][:, cols] for j in range(xs))
            pieces.append(merged.astype(jnp.bfloat16))
    chosen = jnp.concatenate(pieces, axis=1)

    for copy in weights:
        copy.wait()
    psend[...] = jnp.dot(chosen, wbuf[1], preferred_element_type=jnp.float32).astype(jnp.bfloat16)
    p_copy = remote(psend, pbuf, p_sem.at[0], p_sem.at[1], head=oh)
    p_copy.start()
    hidden = jnp.dot(chosen, wbuf[0], preferred_element_type=jnp.float32)
    residual = (res_ref[0] + res_ref[1]) + (res_ref[2] + res_ref[3])
    p_copy.wait_recv()
    hidden = residual.astype(jnp.float32) + (hidden + pbuf[...].astype(jnp.float32))

    own = 2 * hd + kc
    sqbuf[own] = jnp.broadcast_to(jnp.sum(hidden * hidden, axis=1, keepdims=True), (16, 128))

    def s_copy(d):
        return remote(
            sqbuf.at[own],
            sqbuf.at[own],
            s_send.at[d],
            s_recv.at[d],
            head=lax.rem(hd + d // 2, 2),
            core=lax.rem(kc + d % 2, 2),
        )

    for d in range(1, 4):
        s_copy(d).start()
    for d in range(1, 4):
        s_copy(d).wait_recv()
    squares = (sqbuf[0] + sqbuf[1]) + (sqbuf[2] + sqbuf[3])
    scale = lax.rsqrt(squares / width_full + 1e-05)[:, :1]
    ubuf[...] = (hidden * scale * gain_ref[kc]).astype(jnp.bfloat16)
    both = pl.ds(pl.multiple_of(kc * wide, 128), wide)

    def block(bx, bz):
        return g_ref.at[bx, bz, :, both]

    def z_copy(dz):
        to = lax.rem(z + dz, zs)
        return remote(ubuf, block(x, z), z_send.at[dz], z_recv.at[dz], z=to)

    def x_copy(dx, dz):
        bz = lax.rem(z + zs - dz, zs)
        to = lax.rem(x + dx, xs)
        return remote(block(x, bz), block(x, bz), x_send.at[dx, dz], x_recv.at[dx, dz], x=to)

    def relay(dz):
        bz = lax.rem(z + zs - dz, zs)
        step = 1 if ([0] + z_order).index(dz) % 2 == 0 else xs - 1
        part = block(lax.rem(x + xs - step, xs), bz)
        to = lax.rem(x + step, xs)
        return remote(part, part, x_send.at[2, dz], x_recv.at[2, dz], x=to)

    def plane_of(dx):
        return lax.rem(x + xs - dx, xs)

    def k_copy(dx):
        plane = g_ref.at[plane_of(dx), :, :, both]
        return remote(plane, plane, k_send.at[dx], k_recv.at[dx], core=ok)

    def e_copy(dx):
        at = plane_of(dx)
        return remote(
            logits.at[at, oh], arrived.at[at], e_send.at[dx], e_recv.at[dx], head=oh
        )

    def project(dx):
        at = plane_of(dx)
        k_copy(dx).wait_recv()
        rows = g_ref[at].reshape(zs * 16, half)
        out = lax.dot_general(
            rows, lmbuf[...], (((1,), (1,)), ((), ())), preferred_element_type=jnp.float32
        )
        logits[at] = out.astype(jnp.bfloat16).reshape(logits.shape[1:])
        e_copy(dx).start()

    def reduce_plane(dx, packed):
        at = plane_of(dx)
        e_copy(dx).wait_recv()
        both_halves = logits[at, hd].astype(jnp.float32) + arrived[at].astype(jnp.float32)
        rows, width = both_halves.shape
        highest = jnp.max(both_halves, axis=1, keepdims=True)
        total = jnp.sum(jnp.exp(both_halves - highest), axis=1, keepdims=True)
        match = ids_ref[at] == lax.broadcasted_iota(jnp.int32, (rows, width), 1)
        target = jnp.sum(jnp.where(match, both_halves, 0.0), axis=1, keepdims=True)
        lane = lax.broadcasted_iota(jnp.int32, packed.shape, 1)
        row = lax.broadcasted_iota(jnp.int32, packed.shape, 0)
        low = lax.rem(at, 2) * rows
        here = (row >= low) & (row < low + rows)
        for i, column in enumerate((highest, total, target)):
            column = jnp.concatenate([column, column], axis=0)
            packed = jnp.where(here & (lane == at // 2 + 2 * i), column, packed)
        return packed

    for dz in reversed(z_order):
        z_copy(dz).start()
    here = pltpu.make_async_copy(ubuf, block(x, z), u_sem)
    here.start()
    here.wait()
    z_seq = [0] + z_order
    sides = [1, xs - 1] if xs > 2 else [1]
    for dz in z_seq:
        if dz:
            z_copy(dz).wait_recv()
        for dx in sides:
            x_copy(dx, dz).start()
    k_copy(0).start()
    embedding.wait()
    project(0)
    for s in range(2 * xs):
        at = (s // 2, s % 2)
        for buf, send, recv in ((lbuf, l_send, l_recv), (obuf, o_send, o_recv)):
            part = buf.at[at]
            remote(part, part, send.at[0], recv.at[s], head=oh).wait_recv()
    for k in range(2):
        parts = shares_of([lbuf[j, k] for j in range(xs)])
        parts.append(jnp.zeros((128 - 8 * xs, 128), jnp.float32))
        shares = jnp.transpose(jnp.concatenate(parts, axis=0))
        for h in range(heads):
            cols = slice(h * HEAD_SIZE, (h + 1) * HEAD_SIZE)
            merged = sum(
                shares[:, 8 * j + h : 8 * j + h + 1] * obuf[j, k, :, cols].astype(jnp.float32)
                for j in range(xs)
            )
            at = (k * heads + h) * HEAD_SIZE
            att_ref[:, at : at + HEAD_SIZE] = merged.astype(jnp.bfloat16)

    for dz in z_seq:
        for dx in sides:
            x_copy(dx, dz).wait_recv()
        if xs > 2:
            relay(dz).start()
    for dx in sides:
        k_copy(dx).start()
    for dx in sides:
        project(dx)

    packed = jnp.zeros((zs * 16, 128), jnp.float32)
    packed = reduce_plane(0, packed)
    if xs > 2:
        for dz in z_seq:
            relay(dz).wait_recv()
        k_copy(2).start()
        packed = reduce_plane(1, packed)
        project(2)
        packed = reduce_plane(xs - 1, packed)
        packed = reduce_plane(2, packed)
    else:
        packed = reduce_plane(1, packed)
    mine = 4 * x + row_slot
    sbuf[mine] = jnp.transpose(packed)[:8]

    def merged(parts):
        tops = [part[0:2] for part in parts]
        top = functools.reduce(jnp.maximum, tops)
        total = functools.reduce(
            jnp.add, [part[2:4] * jnp.exp(part[0:2] - top) for part in parts]
        )
        target = functools.reduce(jnp.add, [part[4:6] for part in parts])
        return (top, total, target)

    def m_copy(dx, dy, dk):
        s = 4 * dx + 2 * dy + dk
        return remote(
            sbuf.at[mine],
            sbuf.at[mine],
            m_send.at[s],
            m_recv.at[s],
            x=lax.rem(x + dx, xs),
            yh=lax.rem(yh + dy, 2),
            core=lax.rem(kc + dk, 2),
        )

    for each in c_order:
        m_copy(*each).start()
    for each in c_order:
        m_copy(*each).wait_recv()
    top, total, target = merged([sbuf[s] for s in range(4 * xs)])
    fbuf[hd, z] = jnp.concatenate([top, total, target, target], axis=0)

    def f_copy(dh, dz):
        part = fbuf.at[hd, z]
        s = zs * dh + dz
        where = {"head": lax.rem(hd + dh, 2), "z": lax.rem(z + dz, zs)}
        return remote(part, part, f_send.at[s], f_recv.at[s], **where)

    f_order = [(dh, dz) for dz in reversed([0] + z_order) for dh in (0, 1) if dh or dz]
    for each in f_order:
        f_copy(*each).start()
    for each in f_order:
        f_copy(*each).wait_recv()
    for h in range(2):
        top, total, target = merged([fbuf[h, zz] for zz in range(zs)])
        found = target - top - jnp.log(total)
        out_ref[h] = jnp.concatenate([found] * 4, axis=0)

    for each in c_order:
        for copy in c_copies(*each):
            copy.wait_send()
    for dx, dk in o_order:
        for copy in o_copies(dx, dk):
            copy.wait_send()
    p_copy.wait_send()
    for d in range(1, 4):
        s_copy(d).wait_send()
    for dz in z_order:
        z_copy(dz).wait_send()
    for dz in range(zs):
        for dx in sides:
            x_copy(dx, dz).wait_send()
        if xs > 2:
            relay(dz).wait_send()
    for dx in range(xs):
        k_copy(dx).wait_send()
        e_copy(dx).wait_send()
    for each in c_order:
        m_copy(*each).wait_send()
    for each in f_order:
        f_copy(*each).wait_send()


def tail(sizes, o, l, co, cl, res, gain, ids, out_weight, lm_weight):
    xs, zs = sizes
    tok = o.shape[2]
    depth, width_full = out_weight.shape
    vocab, half = lm_weight.shape
    wide = half // 2
    side = zs * 8
    dma = pltpu.SemaphoreType.DMA
    bf16, f32 = (jnp.bfloat16, jnp.float32)
    hbm = pl.BlockSpec(memory_space=pltpu.HBM)
    return pl.pallas_call(
        functools.partial(tail_kernel, sizes, width_full),
        out_shape=(
            jax.ShapeDtypeStruct((tok, depth), bf16),
            jax.ShapeDtypeStruct((2, 8, 2 * side), f32),
        ),
        in_specs=[pl.BlockSpec(memory_space=VMEM)] * 7 + [hbm] * 2,
        out_specs=(pl.BlockSpec(memory_space=VMEM),) * 2,
        scratch_shapes=[
            VMEM(o.shape, bf16),
            VMEM(l.shape, f32),
            VMEM((xs, 2, 2, *co.shape[1:]), bf16),
            VMEM((xs, 2, 2, *cl.shape[1:]), f32),
            VMEM((2, depth, wide), bf16),
            VMEM((vocab, half), bf16),
            VMEM((16, wide), bf16),
            VMEM((16, wide), bf16),
            VMEM((4, 16, 128), f32),
            VMEM((16, wide), bf16),
            VMEM((xs, zs, 16, half), bf16),
            VMEM((xs, 2, side, vocab), bf16),
            VMEM((xs, side, vocab), bf16),
            VMEM((4 * xs, 8, 2 * side), f32),
            VMEM((2, zs, 8, 2 * side), f32),
            dma((3,)),
            dma((2 * xs,)),
            dma((2 * xs,)),
            dma((2 * xs,)),
            dma((2 * xs,)),
            dma((2, 4 * xs)),
            dma((2, 4 * xs)),
            dma((2,)),
            dma((4,)),
            dma((4,)),
            dma,
            dma((zs,)),
            dma((zs,)),
            dma((xs, zs)),
            dma((xs, zs)),
            dma((xs,)),
            dma((xs,)),
            dma((xs,)),
            dma((xs,)),
            dma((4 * xs,)),
            dma((4 * xs,)),
            dma((2 * zs,)),
            dma((2 * zs,)),
        ],
        compiler_params=pltpu.CompilerParams(
            collective_id=1, has_side_effects=True, vmem_limit_bytes=50 << 20
        ),
        name="tail",
    )(o, l, co, cl, res, gain, ids, out_weight, lm_weight)


def per_device(
    sizes,
    queries,
    rotated_keys,
    value_matrix,
    doc_lengths,
    scored,
    residual,
    norm_gain,
    out_weight,
    lm_weight,
    token_ids,
    old_logp,
    advantage,
):
    xs, zs = sizes
    x, yh, z, kc = (lax.axis_index(n) for n in CTX)
    hd = lax.axis_index("head")
    resp = scored.shape[0]
    half = residual.shape[1]
    kvs, qs, hots, res = exchange(
        sizes, rotated_keys, value_matrix, queries, scored, residual
    )
    o, l, co, cl = flash(sizes, doc_lengths, qs, kvs, hots)

    gain = norm_gain.reshape(2, 1, half // 2)
    vocab = lm_weight.shape[1]
    start = (((x * 2 + yh) * zs + z) * 2 + kc) * vocab
    ids = token_ids.reshape(xs, 2, 2, zs // 2, 2, resp).transpose(2, 0, 3, 1, 4, 5)
    ids = lax.dynamic_index_in_dim(ids.reshape(2, xs, -1, 1), hd, 0, keepdims=False) - start
    attended, found = tail(sizes, o, l, co, cl, res, gain, ids, out_weight, lm_weight.T)
    found = found[:, : xs // 2].reshape(2, xs, zs // 2, 2, 2, resp)
    log_probs = found.transpose(1, 3, 0, 2, 4, 5).reshape(-1)
    ratio = jnp.exp(jnp.clip(log_probs - old_logp, -4.0, 4.0))
    token_loss = -jnp.minimum(ratio * advantage, jnp.clip(ratio, 0.8, 1.2) * advantage)
    return (attended, log_probs, token_loss)


def solution(mesh, shape=(4, 2, 8, 2)):
    finer = Mesh(mesh.devices.reshape(*shape, mesh.shape["head"]), NAMES)
    placed = (
        P(CTX, "head"),
        P(CTX, "head"),
        P(CTX, "head"),
        P(),
        P(CTX),
        P(CTX, "head"),
        P("head"),
        P("head", None),
        P("head", CTX),
        P(),
        P(),
        P(),
    )
    return jax.shard_map(
        functools.partial(per_device, (shape[0], shape[2])),
        mesh=finer,
        in_specs=placed,
        out_specs=(P(CTX, "head"), P(), P()),
        check_vma=False,
    )
```
